32 devices in a mesh: groups: 2 (over y), ctx: 4 (over z), heads: 4 (over x, core).
Axes of the slice: x: 2, y: 2, z: 4, core: 2. Of those that a mesh axis runs over, the one named last changes fastest.
Arguments:
- ssm_input: bfloat16 [2048, 8192], P(('groups', 'ctx'), 'heads'), parts along dimension 0, may hold values from -6 to 6
- decay_log: float32 [2048, 128], P(('groups', 'ctx'), 'heads'), parts along dimension 0
- state_write: bfloat16 [2048, 128], P(('groups', 'ctx')), parts along dimension 0, may hold values from -2 to 2
- state_read: bfloat16 [2048, 128], P(('groups', 'ctx')), parts along dimension 0, may hold values from -2 to 2
- skip_scale: float32 [128], P('heads'), may hold values from 0.5 to 3
- gate_input: bfloat16 [2048, 8192], P(('groups', 'ctx'), 'heads'), parts along dimension 0, may hold values from -6 to 6
- ssm_gain: float32 [8192], P('heads'), may hold values from 0.1 to 1.9
- out_weight: bfloat16 [8192, 4096], P('heads', 'ctx'), may hold values from -0.0625 to 0.0625
- residual_in: bfloat16 [2048, 4096], P(('groups', 'ctx'), 'heads'), parts along dimension 0, may hold values from -24 to 24
- moe_gain: float32 [4096], P('heads'), may hold values from 0.1 to 1.9
- down_latent: bfloat16 [4096, 1024], P('heads'), may hold values from -0.09375 to 0.09375
- expert_up: bfloat16 [8, 1024, 2688], P('ctx', None, 'heads'), may hold values from -0.1875 to 0.1875
- expert_down: bfloat16 [8, 2688, 1024], P('ctx', 'heads'), may hold values from -0.125 to 0.125
- up_latent: bfloat16 [1024, 4096], P(None, 'heads'), may hold values from -0.1875 to 0.1875
- expert_ids: int32 [2048, 22], P(('groups', 'ctx')), parts along dimension 0, may hold values from 0 to 511, as said below
- combine_fixed: int32 [2048, 22], P(('groups', 'ctx')), parts along dimension 0, may hold values from 1 to 65535
Outputs:
- layer_out: bfloat16 [2048, 4096], P(('groups', 'ctx'), 'heads'), parts along dimension 0
The draws below stay inside these ranges and needn't reach their ends.
There are 2 independent parts, one for each index of `groups`. The reference program is written for one: setup_inputs(seed, part) draws one part's arguments, and reference() takes and returns one part's arrays. A program takes and returns all parts, laid end to end along the dimension named above; an argument that names none is the same for every part. Nothing has to cross between parts.
Inputs may be any that keep to these rules, and one draw needn't show every extreme that they name: `expert_ids`: each row names 22 different experts. No expert below 8 is named by more than 16 of the 256 tokens of one block, and in every block some expert below 8 is named by exactly 16 of them.
All inputs are finite; a program needn't handle non-finite values.
Results may differ from the reference program's by a relative error of at most 0.014.
Values may be sent and summed in bfloat16 or wider, within the bound.
A program may use at most 128 MiB of HBM per device.

```python
import jax
import jax.numpy as jnp
from jax import lax

D = 4096
SCAN_HEADS = 128
P_SIZE = 64
N = 128
GRP = 1024
LAT = 1024
FFN = 2688
E = 512
TOPK = 22
TOK_CTX = 256
INNER = 8192
CAP = 16
WAVE = 8
WINDOW_TOKENS = 1024
N_HEADS = 4


def draw_decay_log(key, part):
    key_kind = jax.random.fold_in(key, 21)
    key_fast = jax.random.fold_in(key, 22)
    key_slow = jax.random.fold_in(key, 23)
    key_block = jax.random.fold_in(key, 24)
    key_rough = jax.random.fold_in(key, 25)
    position_key = jax.random.fold_in(key, 26)
    spike_key = jax.random.fold_in(key, 27)
    slow_share = 0.5
    is_slow = jax.random.uniform(key_kind, (SCAN_HEADS,)) < slow_share
    fast_rate = jnp.exp(jax.random.uniform(key_fast, (SCAN_HEADS,), jnp.float32, jnp.log(1.0 / 50.0), jnp.log(1.0 / 30.0)))
    slow_rate = jnp.exp(jax.random.uniform(key_slow, (SCAN_HEADS,), jnp.float32, jnp.log(0.2), jnp.log(0.5))) / WINDOW_TOKENS
    head_rate = jnp.where(is_slow, slow_rate, fast_rate)
    block_factor = jnp.exp(jax.random.uniform(key_block, (WINDOW_TOKENS // TOK_CTX, 1), jnp.float32, jnp.log(0.5), jnp.log(2.0)))
    block_factor = jnp.repeat(block_factor, TOK_CTX, axis=0)
    roughness = jnp.exp(jax.random.uniform(key_rough, (WINDOW_TOKENS, SCAN_HEADS), jnp.float32, jnp.log(0.5), jnp.log(2.0)))
    baseline_rate = head_rate[None, :] * block_factor * roughness
    spike_positions = jax.random.randint(position_key, (2,), 0, WINDOW_TOKENS)
    spike_length = jax.random.uniform(spike_key, (SCAN_HEADS,), jnp.float32, 0.22, 0.69)
    spike_mask = jnp.any(jnp.arange(WINDOW_TOKENS)[:, None] == spike_positions[None, :], axis=1)
    return (baseline_rate + jnp.where(spike_mask[:, None], spike_length[None, :], 0.0)).astype(jnp.float32)


def draw_residual_in(key, part):
    key_row = jax.random.fold_in(key, 31)
    key_col = jax.random.fold_in(key, 32)
    key_base = jax.random.fold_in(key, 33)
    row_scale = jnp.exp(jax.random.uniform(key_row, (WINDOW_TOKENS, 1), jnp.float32, jnp.log(0.3), jnp.log(3.0)))
    position = jnp.arange(D, dtype=jnp.float32)[None, :] / D
    col_scale = 0.5 * 4.0 ** position * jnp.exp(jax.random.uniform(key_col, (1, D), jnp.float32, jnp.log(0.7), jnp.log(1.4)))
    base_value = jax.random.normal(key_base, (WINDOW_TOKENS, D), jnp.float32)
    return jnp.clip(base_value * row_scale * col_scale, -24.0, 24.0).astype(jnp.bfloat16)


def draw_expert_ids(key, part):
    block_count = WINDOW_TOKENS // TOK_CTX
    hot_order = jax.random.permutation(jax.random.fold_in(key, 11), WAVE)
    is_hot = hot_order < max(1, WAVE // 8)
    entries = jnp.arange(WAVE * CAP)
    owner_of = entries // CAP
    copy_index = entries % CAP
    expert_range = jnp.arange(E)

    def one_block(block_key):
        key_load = jax.random.fold_in(block_key, 1)
        key_rows = jax.random.fold_in(block_key, 2)
        key_other = jax.random.fold_in(block_key, 3)
        key_shuffle = jax.random.fold_in(block_key, 4)
        load_count = jax.random.randint(key_load, (WAVE,), CAP // 8, CAP // 2 + 1)
        load_count = jnp.where(is_hot, CAP, load_count)
        is_valid = (copy_index < load_count[owner_of]).astype(jnp.int32)
        ranking = jnp.cumsum(is_valid) - 1
        row_order = jax.random.permutation(key_rows, TOK_CTX)
        target = row_order[jnp.mod(ranking, TOK_CTX)]
        member = jnp.zeros((TOK_CTX, E), jnp.int32).at[target, owner_of].add(is_valid)
        random_part = jax.random.randint(key_other, (TOK_CTX, E), 0, 2 ** 20) * E + expert_range[None, :]
        in_wave = expert_range[None, :] < WAVE
        scores = jnp.where(in_wave, jnp.where(member > 0, 2 ** 30 + expert_range[None, :], -1 - expert_range[None, :]), random_part)
        ignored, chosen = lax.top_k(scores, TOPK)
        shuffle_keys = jax.random.randint(key_shuffle, (TOK_CTX, TOPK), 0, 2 ** 20) * TOPK + jnp.arange(TOPK)[None, :]
        new_order = jnp.argsort(shuffle_keys, axis=1)
        return jnp.take_along_axis(chosen, new_order, axis=1)
    block_keys = jax.random.split(key, block_count)
    return jax.vmap(one_block)(block_keys).reshape(WINDOW_TOKENS, TOPK).astype(jnp.int32)


def place_ends(result, own_key, low, high):
    dims = result.shape
    index_at = [jax.random.randint(jax.random.fold_in(own_key, axis), (), 0, dims[axis]) for axis in range(len(dims))]
    result = result.at[tuple(index_at)].set(low)
    longest = dims.index(max(dims))
    index_at[longest] = (index_at[longest] + 1) % dims[longest]
    return result.at[tuple(index_at)].set(high)


def shard_levels(own_key, dims, cuts, smallest, largest):
    loudness = 1.0
    for dim, blocks in cuts:
        heights = jax.random.uniform(jax.random.fold_in(jax.random.fold_in(own_key, 6), dim), (blocks,), jnp.float32, smallest / len(cuts), largest / len(cuts))
        loudness = loudness * jnp.repeat(jnp.exp(heights), dims[dim] // blocks).reshape((-1,) + (1,) * (len(dims) - 1 - dim))
    return loudness


def gaussian(own_key, dims, scale, limit, cuts=(), kind=jnp.bfloat16):
    factor_of = shard_levels(own_key, dims, cuts, -0.22, 0.18) if cuts else 1.0
    values = jax.random.normal(own_key, dims, jnp.float32) * scale * factor_of
    return jnp.minimum(jnp.maximum(values, -limit), limit).astype(kind)


def setup_inputs(seed: int = 0, part: int = 0) -> dict:
    key_of = jax.random.split(jax.random.key(seed), 17)
    part_splits = jax.random.split(jax.random.fold_in(key_of[16], part), 17)
    return {
        "ssm_input": gaussian(part_splits[0], (WINDOW_TOKENS, INNER), 1.0, 6.0, ((0, 4), (1, 4))),
        "decay_log": draw_decay_log(jax.random.fold_in(jax.random.fold_in(key_of[16], part), 71), part),
        "state_write": gaussian(part_splits[2], (WINDOW_TOKENS, N), 0.3, 2.0, ((0, 4),)),
        "state_read": gaussian(part_splits[3], (WINDOW_TOKENS, N), 0.3, 2.0, ((0, 4),)),
        "skip_scale": jnp.clip(0.5 + 2.5 * jax.random.uniform(key_of[4], (SCAN_HEADS,), jnp.float32) ** shard_levels(key_of[4], (SCAN_HEADS,), ((0, 4),), -0.2, 0.2), 0.5, 3.0),
        "gate_input": gaussian(part_splits[5], (WINDOW_TOKENS, INNER), 1.0, 6.0, ((0, 4), (1, 4))),
        "ssm_gain": jnp.clip(1.0 + 0.18 * jax.random.normal(key_of[6], (INNER,), jnp.float32), 0.1, 1.9),
        "out_weight": gaussian(key_of[7], (INNER, D), INNER ** -0.5, 0.0625, ((0, 4), (1, 4))),
        "residual_in": draw_residual_in(jax.random.fold_in(jax.random.fold_in(key_of[16], part), 71), part),
        "moe_gain": jnp.clip(1.0 + 0.18 * jax.random.normal(key_of[9], (D,), jnp.float32), 0.1, 1.9),
        "down_latent": gaussian(key_of[10], (D, LAT), D ** -0.5, 0.09375, ((0, 4),)),
        "expert_up": gaussian(key_of[11], (WAVE, LAT, FFN), LAT ** -0.5, 0.1875, ((0, 4), (2, 4))),
        "expert_down": gaussian(key_of[12], (WAVE, FFN, LAT), FFN ** -0.5, 0.125, ((0, 4), (1, 4))),
        "up_latent": gaussian(key_of[13], (LAT, D), LAT ** -0.5, 0.1875, ((1, 4),)),
        "expert_ids": draw_expert_ids(jax.random.fold_in(jax.random.fold_in(key_of[16], part), 71), part),
        "combine_fixed": place_ends(jax.random.randint(part_splits[15], (WINDOW_TOKENS, TOPK), 1, 65536), jax.random.fold_in(part_splits[15], 1), 1, 65535).astype(jnp.int32),
    }


epsilon = 1e-05

def ssd_block(carry_state, block_data):
    inputs, decays, writes, reads, writes_low, reads_low = block_data
    cumulative = jnp.cumsum(decays, axis=0)
    length_tok = inputs.shape[0]
    causal = jnp.arange(length_tok)[:, None] >= jnp.arange(length_tok)[None, :]
    spread = jnp.where(causal[:, :, None], cumulative[:, None, :] - cumulative[None, :, :], 0.0)
    intersection = jnp.dot(reads_low, writes_low.T, preferred_element_type=jnp.float32)
    mixing = jnp.where(causal[:, :, None], jnp.exp(-spread), 0.0) * intersection[:, :, None]
    within = jnp.einsum('tsh,shp->thp', mixing, inputs, precision=lax.Precision.HIGHEST)
    carried = jnp.einsum('tn,hnp->thp', reads, carry_state, precision=lax.Precision.HIGHEST) * jnp.exp(-cumulative)[:, :, None]
    tail_decay = jnp.exp(cumulative - cumulative[-1][None, :])
    fresh = jnp.einsum('sn,sh,shp->hnp', writes, tail_decay, inputs, precision=lax.Precision.HIGHEST)
    new_state = carry_state * jnp.exp(-cumulative[-1])[:, None, None] + fresh
    return (new_state, within + carried)

def rms_groups(gated, gain):
    grouped = gated.reshape(gated.shape[0], -1, GRP)
    inv_rms = lax.rsqrt(lax.optimization_barrier(jnp.mean(grouped * grouped, axis=2, keepdims=True)) + epsilon)
    return (grouped * inv_rms).reshape(gated.shape) * gain

def route_tables(ids_block, fixed_block):
    matches = ids_block[:, :, None] == jnp.arange(WAVE)[None, None, :]
    chosen = jnp.any(matches, axis=1).astype(jnp.int32)
    weight_fixed = lax.optimization_barrier(jnp.sum(jnp.where(matches, fixed_block[:, :, None], 0), axis=1))
    slot_index = jnp.cumsum(chosen, axis=0) - 1
    placed = (chosen[:, :, None] == 1) & (slot_index[:, :, None] == jnp.arange(CAP)[None, None, :])
    route_weight = (weight_fixed.astype(jnp.float32) / 65536.0).astype(jnp.bfloat16)
    table = jnp.where(placed, route_weight[:, :, None], jnp.zeros((), jnp.bfloat16)).astype(jnp.bfloat16)
    return (placed.astype(jnp.bfloat16).reshape(TOK_CTX, WAVE * CAP), table.reshape(TOK_CTX, WAVE * CAP))

def expert_apply(operands):
    rows_in, first_mat, second_mat = operands
    hidden = jnp.dot(rows_in, first_mat, preferred_element_type=jnp.float32)
    hidden = (jnp.maximum(hidden, 0.0) ** 2).astype(jnp.bfloat16)
    return jnp.dot(hidden, second_mat, preferred_element_type=jnp.float32).astype(jnp.bfloat16)

def reference(ssm_input, decay_log, state_write, state_read, skip_scale, gate_input, ssm_gain, out_weight, residual_in, moe_gain, down_latent, expert_up, expert_down, up_latent, expert_ids, combine_fixed):
    block_count = WINDOW_TOKENS // TOK_CTX
    inputs = ssm_input.astype(jnp.float32).reshape(block_count, TOK_CTX, SCAN_HEADS, P_SIZE)
    decays = decay_log.astype(jnp.float32).reshape(block_count, TOK_CTX, SCAN_HEADS)
    writes = state_write.astype(jnp.float32).reshape(block_count, TOK_CTX, N)
    reads = state_read.astype(jnp.float32).reshape(block_count, TOK_CTX, N)
    writes_low = state_write.reshape(block_count, TOK_CTX, N)
    reads_low = state_read.reshape(block_count, TOK_CTX, N)
    start_state = jnp.zeros((SCAN_HEADS, N, P_SIZE), jnp.float32)
    ignored, mixed = lax.scan(ssd_block, start_state, (inputs, decays, writes, reads, writes_low, reads_low))
    mixed = mixed.reshape(WINDOW_TOKENS, SCAN_HEADS, P_SIZE) + skip_scale[None, :, None] * inputs.reshape(WINDOW_TOKENS, SCAN_HEADS, P_SIZE)
    gated = mixed.reshape(WINDOW_TOKENS, INNER) * jax.nn.silu(gate_input.astype(jnp.float32))
    normed = rms_groups(gated, ssm_gain).astype(jnp.bfloat16)
    slice_width = INNER // N_HEADS
    mamba_out = jnp.zeros((WINDOW_TOKENS, D), jnp.float32)
    for head_slice in range(N_HEADS):
        lower = head_slice * slice_width
        partial_value = jnp.dot(normed[:, lower:lower + slice_width], out_weight[lower:lower + slice_width], preferred_element_type=jnp.float32)
        partial_value = lax.optimization_barrier(partial_value.astype(jnp.bfloat16))
        mamba_out = mamba_out + partial_value.astype(jnp.float32)
    residual = residual_in.astype(jnp.float32) + mamba_out
    inv_rms = lax.rsqrt(lax.optimization_barrier(jnp.mean(residual * residual, axis=1, keepdims=True)) + epsilon)
    scaled = (residual * moe_gain).astype(jnp.bfloat16)
    latent = (jnp.dot(scaled, down_latent, preferred_element_type=jnp.float32) * inv_rms).astype(jnp.bfloat16)
    placed, tables = jax.vmap(route_tables)(expert_ids.reshape(block_count, TOK_CTX, TOPK), combine_fixed.reshape(block_count, TOK_CTX, TOPK))
    latent_blocks = latent.reshape(block_count, TOK_CTX, LAT)
    dispatched = jax.vmap(lambda place_block, latent_block: jnp.dot(place_block.T, latent_block, preferred_element_type=jnp.float32))(placed, latent_blocks)
    dispatched = dispatched.astype(jnp.bfloat16).reshape(block_count, WAVE, CAP, LAT)
    expert_rows = dispatched.transpose(1, 0, 2, 3).reshape(WAVE, block_count * CAP, LAT)
    expert_out = lax.map(expert_apply, (expert_rows, expert_up, expert_down))
    returned = expert_out.reshape(WAVE, block_count, CAP, LAT).transpose(1, 0, 2, 3).reshape(block_count, WAVE * CAP, LAT)
    combined = jax.vmap(lambda table_block, back_block: jnp.dot(table_block, back_block, preferred_element_type=jnp.float32))(tables, returned)
    combined_low = combined.reshape(WINDOW_TOKENS, LAT).astype(jnp.bfloat16)
    moe_out = jnp.dot(combined_low, up_latent, preferred_element_type=jnp.float32)
    return (residual + moe_out).astype(jnp.bfloat16)
```

```python
import functools

import jax
import jax.numpy as jnp
from jax import lax
from jax.experimental import pallas as pl
from jax.experimental.pallas import tpu as pltpu
from jax.sharding import PartitionSpec as P

D = 4096
GRP = 1024
LAT = 1024
CAP = 16


epsilon = 1e-05


MESH = pl.DeviceIdType.MESH
BF = jnp.bfloat16
F32 = jnp.float32


def vmem(count=1):
    return [pl.BlockSpec(memory_space=pltpu.VMEM)] * count


def greet(device):
    pl.semaphore_signal(
        pltpu.get_barrier_semaphore(), inc=1, device_id=device, device_id_type=MESH
    )


def greeted(count):
    pl.semaphore_wait(pltpu.get_barrier_semaphore(), count)


def one_if(condition):
    return jnp.where(condition, 1, 0)


def remote(src, dst, send, recv, device):
    return pltpu.make_async_remote_copy(
        src_ref=src, dst_ref=dst, send_sem=send, recv_sem=recv, device_id=device, device_id_type=MESH
    )


def pair_wide(first, second, width):
    lane = lax.broadcasted_iota(jnp.int32, (first.shape[0], 2 * width), 1)
    return jnp.where(lane < width, first, second)


def mixer_kernel(
    n, heads, width, piece, lag,
    x_hbm, gate_hbm, weight_hbm, resid_hbm, decay_ref, write_ref, read_ref, skip_ref, gain_ref,
    out_ref,
    x_ref, gate_ref, weight_ref, resid_ref, cum, cum_rows, skips, inter,
    mixed, state, ends, prior, outgoing, gated,
    blocks, acc, parts, core_in, chip_out, x_in, fin_out, final,
    load_sem, chain_send, chain_recv, up_send, up_recv, down_send, down_recv,
    core_send, core_recv, x_send, x_recv, fin_send, fin_recv,
):
    me, head = lax.axis_index("ctx"), lax.axis_index("heads")
    rows, columns = x_ref.shape
    span = 2 * width
    pairs = columns // span
    head_count = decay_ref.shape[1]
    out_width = weight_ref.shape[1]
    count = columns // piece
    share = n // heads
    cores = 2
    chips = heads // cores
    core, chip = head % cores, head // cores
    half, strip = out_width // cores, rows // chips
    has_prev, has_next = me > 0, me < n - 1
    prev, after = jnp.maximum(me - 1, 0), jnp.minimum(me + 1, n - 1)

    loads = [
        pltpu.make_async_copy(src, dst, load_sem.at[i])
        for i, (src, dst) in enumerate(
            [(x_hbm, x_ref), (gate_hbm, gate_ref), (weight_hbm, weight_ref), (resid_hbm, resid_ref)]
        )
    ]
    for load in loads:
        load.start()
    for i in range(n):
        for j in range(heads):
            if i or j:
                greet({"ctx": (me + i) % n, "heads": (head + j) % heads})

    t = lax.broadcasted_iota(jnp.int32, (rows, rows), 0)
    s = lax.broadcasted_iota(jnp.int32, (rows, rows), 1)
    lower = jnp.where(t >= s, 1.0, 0.0)
    cum[...] = jnp.zeros(cum.shape, F32)
    cum[:, :head_count] = jnp.dot(
        lower, decay_ref[...], precision=lax.Precision.HIGHEST, preferred_element_type=F32
    )
    cum_rows[...] = lax.dot_general(
        decay_ref[...], lower, (((0,), (1,)), ((), ())),
        precision=lax.Precision.HIGHEST, preferred_element_type=F32,
    )
    skips[...] = jnp.zeros(skips.shape, F32)
    skips[0:1, :head_count] = skip_ref[...]
    product = lax.dot_general(
        read_ref[...], write_ref[...], (((1,), (1,)), ((), ())), preferred_element_type=F32
    )
    inter[...] = jnp.where(t >= s, product, 0.0)
    greeted(n * heads - 1)
    loads[0].wait()

    def lanes(p):
        return pl.ds(pl.multiple_of(p * span, span), span)

    def shifted(ref, p):
        lane_count = ref.shape[1]
        return pltpu.roll(ref[...], (lane_count - 2 * p) % lane_count, 1)

    band = rows // 2
    causal = lax.broadcasted_iota(jnp.int32, (band, band), 0) >= lax.broadcasted_iota(
        jnp.int32, (band, band), 1
    )

    def scan(p):
        x = x_ref[:, lanes(p)]
        cols = shifted(cum, p)
        skip = shifted(skips, p)
        outs, tails, lasts = [], [], []
        for j in range(2):
            col = cols[:, j : j + 1]
            row = cum_rows[pl.ds(2 * p + j, 1), :]
            last = col[rows - 1 : rows, :]
            lane = x[:, j * width : (j + 1) * width]
            bands = []
            for lo in range(0, rows, band):
                hi = lo + band
                spread = jnp.where(causal, col[lo:hi] - row[:, lo:hi], 0.0)
                if lo:
                    spread = jnp.concatenate([col[lo:hi] - row[:, :lo], spread], axis=1)
                mixing = (jnp.exp(-spread) * inter[lo:hi, :hi]).astype(BF)
                bands.append(jnp.dot(mixing, lane[:hi], preferred_element_type=F32))
            outs.append(jnp.concatenate(bands, axis=0))
            tails.append(jnp.exp(col - last))
            lasts.append(jnp.exp(-last))
        wide = x.astype(F32)
        direct = pair_wide(skip[0:1, 0:1], skip[0:1, 1:2], width) * wide
        mixed[p] = jnp.concatenate(outs, axis=1) + direct
        scaled = (wide * pair_wide(tails[0], tails[1], width)).astype(BF)
        state[p] = lax.dot_general(
            write_ref[...], scaled, (((0,), (0,)), ((), ())), preferred_element_type=F32
        )
        ends[p] = pair_wide(lasts[0], lasts[1], width)

    def chain_copy(q):
        return remote(
            outgoing.at[q], prior.at[q], chain_send.at[q], chain_recv.at[q], {"ctx": after}
        )

    def chain(q):
        @pl.when(me == 0)
        def _():
            prior[q] = jnp.zeros(prior.shape[1:], BF)
            outgoing[q] = state[q].astype(BF)

        @pl.when(has_prev)
        def _():
            chain_copy(q).wait_recv()
            outgoing[q] = (prior[q].astype(F32) * ends[q] + state[q]).astype(BF)

        pl.when(has_next)(lambda: chain_copy(q).start())

    def advance(i, carry):
        pl.when(i < pairs)(lambda: scan(i))
        q = i - lag * me
        pl.when(jnp.logical_and(q >= 0, q < pairs))(lambda: chain(q))
        return carry

    lax.fori_loop(0, pairs + lag * (n - 1), advance, 0)

    def upward(b, p):
        spot = blocks.at[b, p]
        return remote(spot, spot, up_send.at[b, p], up_recv.at[b, p], {"ctx": after})

    def downward(b, p):
        spot = blocks.at[b, p]
        return remote(spot, spot, down_send.at[b, p], down_recv.at[b, p], {"ctx": prev})

    group_pairs = GRP // span
    group_pieces = GRP // piece
    piece_pairs = piece // span
    loads[1].wait()

    def gate(g, carry):
        squares = jnp.zeros((rows, span), F32)
        for i in range(group_pairs):
            p = g * group_pairs + i
            cols = shifted(cum, p)
            reach = jnp.exp(-pair_wide(cols[:, 0:1], cols[:, 1:2], width))
            carried = jnp.dot(read_ref[...], prior[p], preferred_element_type=F32) * reach
            gating = gate_ref[:, lanes(p)].astype(F32)
            value = (mixed[p] + carried) * (gating / (1.0 + jnp.exp(-gating)))
            gated[i] = value
            squares = squares + value * value
        scale = lax.rsqrt(jnp.sum(squares, axis=1, keepdims=True) / GRP + epsilon)
        for i in range(group_pairs):
            p = g * group_pairs + i
            value = (gated[i] * scale * gain_ref[:, lanes(p)]).astype(BF)
            lo = (i % piece_pairs) * span
            blocks[me, g * group_pieces + i // piece_pairs, :, lo : lo + span] = value
        for k in range(group_pieces):
            p = g * group_pieces + k
            pl.when(has_next)(lambda: upward(me, p).start())
            pl.when(has_prev)(lambda: downward(me, p).start())
        return carry

    lax.fori_loop(0, columns // GRP, gate, 0)
    loads[2].wait()

    def multiply(slot, b, p):
        step = min(out_width, 256)
        fed = blocks[b, p]
        for lo in range(0, out_width, step):
            held = acc[slot, :, lo : lo + step]
            part = weight_ref[pl.ds(pl.multiple_of(p * piece, piece), piece), lo : lo + step]
            acc[slot, :, lo : lo + step] = jnp.where(p == 0, 0.0, held) + jnp.dot(
                fed, part, preferred_element_type=F32
            )

    def core_copy(b):
        return remote(
            parts.at[b, 1 - core], core_in.at[b], core_send.at[b], core_recv.at[b],
            {"heads": head + 1 - 2 * core},
        )

    def round_partial(b, slot):
        for k in range(cores):
            parts[b, k] = acc[slot, :, k * half : (k + 1) * half].astype(BF)
        core_copy(b).start()

    def chip_copy(b, k):
        to = (chip + k) % chips
        return remote(
            chip_out.at[b, to], x_in.at[b, k], x_send.at[b, k], x_recv.at[b, k],
            {"heads": to * cores + core},
        )

    def sum_cores(b):
        core_copy(b).wait_recv()
        for k in range(chips):
            part = slice(k * strip, (k + 1) * strip)
            both = parts[b, core, part].astype(F32) + core_in[b, part].astype(F32)
            chip_out[b, k] = both.astype(BF)
        for k in range(1, chips):
            chip_copy(b, k).start()

    def local_final(b):
        return jnp.logical_and(b == me, head == me // share)

    def final_copy(b):
        return remote(
            fin_out.at[b], final.at[me % share, head], fin_send.at[b],
            fin_recv.at[me % share, head], {"ctx": b, "heads": me // share},
        )

    def sum_chips(b):
        part = pl.ds(pl.multiple_of(chip * strip, strip), strip)
        total = parts[b, core, part].astype(F32) + core_in[b, part].astype(F32)
        for k in range(1, chips):
            chip_copy(b, k).wait_recv()
            total = total + x_in[b, k].astype(F32)
        fin_out[b] = total.astype(BF)

        @pl.when(local_final(b))
        def _():
            final[me % share, head] = total.astype(BF)

        pl.when(jnp.logical_not(local_final(b)))(lambda: final_copy(b).start())

    def own(p, carry):
        multiply(0, me, p)
        return carry

    lax.fori_loop(0, count, own, 0)
    round_partial(me, 0)

    def around(s, act):
        low, high = me - s, me + s
        pl.when(low >= 0)(lambda: act(jnp.maximum(low, 0), 0))

        @pl.when(jnp.logical_and(high < n, s > 0))
        def _():
            act(jnp.minimum(high, n - 1), 1)

    def step(i, carry):
        s, p = 1 + i // count, i % count
        low, high = me - s, me + s
        low_spot, high_spot = jnp.maximum(low, 0), jnp.minimum(high, n - 1)

        @pl.when(low >= 0)
        def _():
            upward(low_spot, p).wait_recv()
            pl.when(has_next)(lambda: upward(low_spot, p).start())

        @pl.when(high < n)
        def _():
            downward(high_spot, p).wait_recv()
            pl.when(has_prev)(lambda: downward(high_spot, p).start())

        around(s, lambda b, slot: multiply(slot, b, p))
        pl.when(p == count - 1)(lambda: around(s, round_partial))
        pl.when(p == 0)(lambda: around(s - 1, lambda b, slot: sum_cores(b)))
        pl.when(p == min(1, count - 1))(lambda: around(s - 1, lambda b, slot: sum_chips(b)))
        return carry

    lax.fori_loop(0, (n - 1) * count, step, 0)
    around(n - 1, lambda b, slot: sum_cores(b))
    around(n - 1, lambda b, slot: sum_chips(b))
    loads[3].wait()

    for j in range(share):
        source = head * share + j
        for k in range(heads):
            here = jnp.logical_and(source == me, k == head)

            @pl.when(jnp.logical_not(here))
            def _():
                remote(
                    fin_out.at[0], final.at[j, k], fin_send.at[0], fin_recv.at[j, k],
                    {"ctx": source, "heads": k},
                ).wait_recv()

            part = slice((k // cores) * strip, (k // cores + 1) * strip)
            lo = j * out_width + (k % cores) * half
            out_ref[part, lo : lo + half] = (
                resid_ref[part, lo : lo + half].astype(F32) + final[j, k].astype(F32)
            )

    for q in range(pairs):
        pl.when(has_next)(lambda: chain_copy(q).wait_send())
    for b in range(n):
        for p in range(count):
            pl.when(jnp.logical_and(has_next, b <= me))(lambda: upward(b, p).wait_send())
            pl.when(jnp.logical_and(has_prev, b >= me))(lambda: downward(b, p).wait_send())
        core_copy(b).wait_send()
        for k in range(1, chips):
            chip_copy(b, k).wait_send()
        pl.when(jnp.logical_not(local_final(b)))(lambda: final_copy(b).wait_send())


def slots_kernel(
    n, heads, width, features, src_ref, out_ref,
    first, middle, second, third,
    first_send, first_recv, second_send, second_recv, third_send, third_recv,
):
    me, head = lax.axis_index("ctx"), lax.axis_index("heads")

    for k in range(1, heads):
        greet({"heads": (head + k) % heads})
    for k in range(1, n):
        greet({"ctx": (me + k) % n})
    greeted(heads + n - 2)

    def first_copy(k):
        to = (head + k) % heads
        return remote(
            src_ref.at[to], first.at[k], first_send.at[k], first_recv.at[k], {"heads": to}
        )

    def second_copy(k):
        to = (me + k) % n
        return remote(
            middle.at[to], second.at[me], second_send.at[k], second_recv.at[k], {"ctx": to}
        )

    def third_copy(k):
        to = (head + k) % heads
        return remote(second, third.at[k], third_send.at[k], third_recv.at[k], {"heads": to})

    for k in range(1, heads):
        first_copy(k).start()
    total = src_ref[head].astype(F32)
    for k in range(1, heads):
        first_copy(k).wait_recv()
        total = total + first[k].astype(F32)
    if src_ref.shape[-1] > width:
        power = total[:, :, width : width + 1]
        total = total[:, :, :width] * lax.rsqrt(power / features + epsilon)
    middle[...] = total.astype(BF)
    for k in range(1, n):
        second_copy(k).start()
    second[me] = middle[me]
    for k in range(1, n):
        second_copy(k).wait_recv()
    for k in range(1, heads):
        third_copy(k).start()
    out_ref[head] = second[...]
    for k in range(1, heads):
        third_copy(k).wait_recv()
        out_ref[(head + heads - k) % heads] = third[k]
    for k in range(1, heads):
        first_copy(k).wait_send()
        third_copy(k).wait_send()
    for k in range(1, n):
        second_copy(k).wait_send()


def reaching(collective_id):
    return pltpu.CompilerParams(
        collective_id=collective_id, has_side_effects=True, vmem_limit_bytes=48 * 1024 * 1024
    )


def dma(*shape):
    return pltpu.SemaphoreType.DMA(shape)


def through_slots(pieces, width, features, collective_id):
    heads, n, rows, wide = pieces.shape
    return pl.pallas_call(
        functools.partial(slots_kernel, n, heads, width, features),
        out_shape=jax.ShapeDtypeStruct((heads, n, rows, width), BF),
        in_specs=vmem(),
        out_specs=vmem()[0],
        scratch_shapes=[
            pltpu.VMEM((heads, n, rows, wide), BF),
            pltpu.VMEM((n, rows, width), BF),
            pltpu.VMEM((n, rows, width), BF),
            pltpu.VMEM((heads, n, rows, width), BF),
            dma(heads), dma(heads), dma(n), dma(n), dma(heads), dma(heads),
        ],
        compiler_params=reaching(collective_id),
    )(pieces)


def mixer(
    ssm_input, decay_log, state_write, state_read, skip_scale, gate_input, ssm_gain, weight, residual_in
):
    n, heads = lax.axis_size("ctx"), lax.axis_size("heads")
    rows, columns = ssm_input.shape
    head_count = decay_log.shape[1]
    width = columns // head_count
    states = state_write.shape[1]
    span = 2 * width
    pairs = columns // span
    piece = GRP // 2
    count = columns // piece
    out_width = weight.shape[1]
    share = n // heads
    chips = heads // 2
    half, strip = out_width // 2, rows // chips
    lane_count = -(-head_count // 128) * 128
    block = (rows, out_width)
    anywhere = pl.BlockSpec(memory_space=pl.ANY)
    return pl.pallas_call(
        functools.partial(mixer_kernel, n, heads, width, piece, 3),
        out_shape=jax.ShapeDtypeStruct((rows, share * out_width), F32),
        in_specs=[anywhere] * 4 + vmem(5),
        out_specs=vmem()[0],
        scratch_shapes=[
            pltpu.VMEM((rows, columns), BF),
            pltpu.VMEM((rows, columns), BF),
            pltpu.VMEM(weight.shape, BF),
            pltpu.VMEM(residual_in.shape, BF),
            pltpu.VMEM((rows, lane_count), F32),
            pltpu.VMEM((head_count, rows), F32),
            pltpu.VMEM((8, lane_count), F32),
            pltpu.VMEM((rows, rows), F32),
            pltpu.VMEM((pairs, rows, span), F32),
            pltpu.VMEM((pairs, states, span), F32),
            pltpu.VMEM((pairs, 1, span), F32),
            pltpu.VMEM((pairs, states, span), BF),
            pltpu.VMEM((pairs, states, span), BF),
            pltpu.VMEM((GRP // span, rows, span), F32),
            pltpu.VMEM((n, count, rows, piece), BF),
            pltpu.VMEM((2,) + block, F32),
            pltpu.VMEM((n, 2, rows, half), BF),
            pltpu.VMEM((n, rows, half), BF),
            pltpu.VMEM((n, chips, strip, half), BF),
            pltpu.VMEM((n, chips, strip, half), BF),
            pltpu.VMEM((n, strip, half), BF),
            pltpu.VMEM((share, heads, strip, half), BF),
            dma(4), dma(pairs), dma(pairs),
            dma(n, count), dma(n, count), dma(n, count), dma(n, count),
            dma(n), dma(n), dma(n, chips), dma(n, chips), dma(n), dma(share, heads),
        ],
        compiler_params=reaching(1),
    )(
        ssm_input, gate_input, weight, residual_in, decay_log, state_write, state_read,
        skip_scale.reshape(1, head_count), ssm_gain.reshape(1, columns),
    )


def local(
    ssm_input,
    decay_log,
    state_write,
    state_read,
    skip_scale,
    gate_input,
    ssm_gain,
    out_weight,
    residual_in,
    moe_gain,
    down_latent,
    expert_up,
    expert_down,
    up_latent,
    expert_ids,
    combine_fixed,
):
    row_count = ssm_input.shape[0]
    n, heads = lax.axis_size("ctx"), lax.axis_size("heads")
    features = residual_in.shape[1] * heads
    latent_width = down_latent.shape[1]
    piece = latent_width // heads
    experts_here = expert_up.shape[0]
    wave_size = experts_here * n
    slot_rows = experts_here * CAP

    matches = expert_ids[:, :, None] == jnp.arange(wave_size)[None, None, :]
    chosen = jnp.any(matches, axis=1).astype(jnp.int32)
    weight_fixed = jnp.sum(jnp.where(matches, combine_fixed[:, :, None], 0), axis=1)
    slot_index = jnp.cumsum(chosen, axis=0) - 1
    placed = (chosen[:, :, None] == 1) & (slot_index[:, :, None] == jnp.arange(CAP)[None, None, :])
    route_weight = (weight_fixed.astype(F32) / 65536.0).astype(BF)
    combine_table = jnp.where(placed, route_weight[:, :, None], jnp.zeros((), BF)).reshape(
        row_count, wave_size * CAP
    )
    placed = placed.astype(BF).reshape(row_count, wave_size * CAP)

    residual = mixer(
        ssm_input, decay_log, state_write, state_read, skip_scale, gate_input, ssm_gain,
        out_weight, residual_in,
    )
    scaled = (residual * moe_gain).astype(BF)
    latent_part = jnp.dot(scaled, down_latent, preferred_element_type=F32).astype(BF)
    squares = jnp.sum(residual * residual, axis=1).astype(BF)
    side = jnp.concatenate(
        [latent_part, jnp.broadcast_to(squares[:, None], (row_count, 128))], axis=1
    )
    slots = lax.dot_general(
        placed, side, (((0,), (0,)), ((), ())), preferred_element_type=F32
    ).astype(BF)
    slots = slots.reshape(n, slot_rows, latent_width + 128)
    pieces = jnp.stack(
        [
            jnp.concatenate(
                [slots[:, :, h * piece : (h + 1) * piece], slots[:, :, latent_width:]], axis=2
            )
            for h in range(heads)
        ]
    )
    incoming = through_slots(pieces, piece, features, 3)
    incoming = incoming.reshape(heads, n, experts_here, CAP, piece).transpose(2, 1, 3, 0, 4)
    incoming = incoming.reshape(experts_here, n * CAP, latent_width)
    hidden = jnp.einsum("esl,elf->esf", incoming, expert_up, preferred_element_type=F32)
    hidden = (jnp.maximum(hidden, 0.0) ** 2).astype(BF)
    expert_out = jnp.einsum("esf,efl->esl", hidden, expert_down, preferred_element_type=F32)
    expert_out = expert_out.astype(BF).reshape(experts_here, n, CAP, heads, piece)
    expert_out = expert_out.transpose(3, 1, 0, 2, 4).reshape(heads, n, slot_rows, piece)
    returned = through_slots(expert_out, piece, features, 4)
    returned = returned.transpose(1, 2, 0, 3).reshape(wave_size * CAP, latent_width)
    combined = jnp.dot(combine_table, returned, preferred_element_type=F32)
    moe_out = jnp.dot(combined.astype(BF), up_latent, preferred_element_type=F32)
    return (residual + moe_out).astype(BF)


def solution(mesh):
    placed = (
        P(("groups", "ctx"), "heads"),
        P(("groups", "ctx"), "heads"),
        P(("groups", "ctx"), None),
        P(("groups", "ctx"), None),
        P("heads"),
        P(("groups", "ctx"), "heads"),
        P("heads"),
        P("heads", "ctx"),
        P(("groups", "ctx"), "heads"),
        P("heads"),
        P("heads", None),
        P("ctx", None, "heads"),
        P("ctx", "heads", None),
        P(None, "heads"),
        P(("groups", "ctx"), None),
        P(("groups", "ctx"), None),
    )
    return jax.shard_map(
        local, mesh=mesh, in_specs=placed, out_specs=P(("groups", "ctx"), "heads"), check_vma=False
    )
```

```python
import functools

import jax
import jax.numpy as jnp
from jax import lax
from jax.experimental import pallas as pl
from jax.experimental.pallas import tpu as pltpu
from jax.sharding import PartitionSpec as P

D = 4096
GRP = 1024
LAT = 1024
CAP = 16
LENT_NUM, LENT_DEN = 3, 8


epsilon = 1e-05


MESH = pl.DeviceIdType.MESH
BF = jnp.bfloat16
F32 = jnp.float32


def vmem(count=1):
    return [pl.BlockSpec(memory_space=pltpu.VMEM)] * count


def greet(device):
    pl.semaphore_signal(
        pltpu.get_barrier_semaphore(), inc=1, device_id=device, device_id_type=MESH
    )


def greeted(count):
    pl.semaphore_wait(pltpu.get_barrier_semaphore(), count)


def one_if(condition):
    return jnp.where(condition, 1, 0)


def remote(src, dst, send, recv, device):
    return pltpu.make_async_remote_copy(
        src_ref=src, dst_ref=dst, send_sem=send, recv_sem=recv, device_id=device, device_id_type=MESH
    )


def pair_wide(first, second, width):
    lane = lax.broadcasted_iota(jnp.int32, (first.shape[0], 2 * width), 1)
    return jnp.where(lane < width, first, second)


def mixer_kernel(
    n, heads, width, piece, lag, lent,
    x_hbm, write_hbm, read_hbm, decay_hbm, skip_hbm, weight_hbm, gate_hbm, gain_hbm, resid_hbm,
    out_ref,
    x_ref, write_ref, read_ref, decay_ref, skip_ref, weight_ref, gate_ref, gain_ref, resid_ref,
    cum, cum_rows, skips, inter,
    mixed, state, ends, prior, outgoing, gated,
    blocks, acc, parts, core_in, chip_out, x_in, fin_out, final, borrowed, strips,
    load_sem, chain_send, chain_recv, up_send, up_recv, down_send, down_recv,
    core_send, core_recv, x_send, x_recv, fin_send, fin_recv, lend_send, lend_recv, strip_recv,
):
    me, head = lax.axis_index("ctx"), lax.axis_index("heads")
    rows, columns = x_ref.shape
    span = 2 * width
    pairs = columns // span
    head_count = decay_ref.shape[0]
    out_width = weight_ref.shape[1]
    count = columns // piece
    share = n // heads
    cores = 2
    chips = heads // cores
    core, chip = head % cores, head // cores
    half, strip = out_width // cores, rows // chips
    has_prev, has_next = me > 0, me < n - 1
    prev, after = jnp.maximum(me - 1, 0), jnp.minimum(me + 1, n - 1)
    keep = count - lent
    at_end = jnp.logical_or(me == 0, me == n - 1)
    beside = jnp.logical_or(me == 1, me == n - 2)
    end_here = jnp.where(me == 1, 0, n - 1)
    beside_here = jnp.where(me == 0, 1, n - 2)

    loads = [
        pltpu.make_async_copy(src, dst, load_sem.at[i])
        for i, (src, dst) in enumerate(
            [
                (x_hbm, x_ref), (write_hbm, write_ref), (read_hbm, read_ref), (decay_hbm, decay_ref),
                (skip_hbm, skip_ref), (weight_hbm, weight_ref), (gate_hbm, gate_ref),
                (gain_hbm, gain_ref), (resid_hbm, resid_ref),
            ]
        )
    ]
    for load in loads:
        load.start()
    for i in range(n):
        for j in range(heads):
            if i or j:
                greet({"ctx": (me + i) % n, "heads": (head + j) % heads})

    t = lax.broadcasted_iota(jnp.int32, (rows, rows), 0)
    s = lax.broadcasted_iota(jnp.int32, (rows, rows), 1)
    lower = jnp.where(t >= s, 1.0, 0.0)
    cum[...] = jnp.zeros(cum.shape, F32)
    for load in loads[:5]:
        load.wait()
    cum[:, :head_count] = lax.dot_general(
        lower, decay_ref[...], (((1,), (1,)), ((), ())),
        precision=lax.Precision.HIGHEST, preferred_element_type=F32,
    )
    cum_rows[...] = lax.dot_general(
        decay_ref[...], lower, (((1,), (1,)), ((), ())),
        precision=lax.Precision.HIGHEST, preferred_element_type=F32,
    )
    skips[...] = jnp.zeros(skips.shape, F32)
    skips[0:1, :head_count] = skip_ref[...]
    product = lax.dot_general(
        read_ref[...], write_ref[...], (((1,), (1,)), ((), ())), preferred_element_type=F32
    )
    inter[...] = jnp.where(t >= s, product, 0.0)
    greeted(n * heads - 1)

    def lend():
        return remote(
            weight_ref.at[pl.ds(keep * piece, lent * piece)], borrowed, lend_send.at[0],
            lend_recv.at[0], {"ctx": beside_here},
        )

    @pl.when(me == n - 1)
    def _():
        loads[5].wait()
        if lent:
            lend().start()

    def lanes(p):
        return pl.ds(pl.multiple_of(p * span, span), span)

    def shifted(ref, p):
        lane_count = ref.shape[1]
        return pltpu.roll(ref[...], (lane_count - 2 * p) % lane_count, 1)

    band = rows // 2
    causal = lax.broadcasted_iota(jnp.int32, (band, band), 0) >= lax.broadcasted_iota(
        jnp.int32, (band, band), 1
    )

    def scan(p):
        x = x_ref[:, lanes(p)]
        cols = shifted(cum, p)
        skip = shifted(skips, p)
        outs, tails, lasts = [], [], []
        for j in range(2):
            col = cols[:, j : j + 1]
            row = cum_rows[pl.ds(2 * p + j, 1), :]
            last = col[rows - 1 : rows, :]
            lane = x[:, j * width : (j + 1) * width]
            bands = []
            for lo in range(0, rows, band):
                hi = lo + band
                spread = jnp.where(causal, col[lo:hi] - row[:, lo:hi], 0.0)
                if lo:
                    spread = jnp.concatenate([col[lo:hi] - row[:, :lo], spread], axis=1)
                mixing = (jnp.exp(-spread) * inter[lo:hi, :hi]).astype(BF)
                bands.append(jnp.dot(mixing, lane[:hi], preferred_element_type=F32))
            outs.append(jnp.concatenate(bands, axis=0))
            tails.append(jnp.exp(col - last))
            lasts.append(jnp.exp(-last))
        wide = x.astype(F32)
        direct = pair_wide(skip[0:1, 0:1], skip[0:1, 1:2], width) * wide
        mixed[p] = jnp.concatenate(outs, axis=1) + direct
        scaled = (wide * pair_wide(tails[0], tails[1], width)).astype(BF)
        state[p] = lax.dot_general(
            write_ref[...], scaled, (((0,), (0,)), ((), ())), preferred_element_type=F32
        )
        ends[p] = pair_wide(lasts[0], lasts[1], width)

    def chain_copy(q):
        return remote(
            outgoing.at[q], prior.at[q], chain_send.at[q], chain_recv.at[q], {"ctx": after}
        )

    def chain(q):
        @pl.when(me == 0)
        def _():
            prior[q] = jnp.zeros(prior.shape[1:], BF)
            outgoing[q] = state[q].astype(BF)

        @pl.when(has_prev)
        def _():
            chain_copy(q).wait_recv()
            outgoing[q] = (prior[q].astype(F32) * ends[q] + state[q]).astype(BF)

        pl.when(has_next)(lambda: chain_copy(q).start())

    def advance(i, carry):
        pl.when(i < pairs)(lambda: scan(i))
        q = i - lag * me
        pl.when(jnp.logical_and(q >= 0, q < pairs))(lambda: chain(q))
        return carry

    lax.fori_loop(0, pairs + lag * (n - 1), advance, 0)

    def upward(b, p):
        spot = blocks.at[b, p]
        return remote(spot, spot, up_send.at[b, p], up_recv.at[b, p], {"ctx": after})

    def downward(b, p):
        spot = blocks.at[b, p]
        return remote(spot, spot, down_send.at[b, p], down_recv.at[b, p], {"ctx": prev})

    @pl.when(me < n - 1)
    def _():
        loads[5].wait()
        if lent:
            pl.when(me == 0)(lambda: lend().start())

    def goes_up(p):
        return jnp.logical_and(has_next, jnp.logical_or(p < keep, me + 1 < n - 1))

    def goes_down(p):
        return jnp.logical_and(has_prev, jnp.logical_or(p < keep, me > 1))

    def needed(p):
        return jnp.logical_or(p < keep, jnp.logical_not(at_end))

    group_pairs = GRP // span
    group_pieces = GRP // piece
    piece_pairs = piece // span
    loads[6].wait()
    loads[7].wait()

    def gate(g, carry):
        squares = jnp.zeros((rows, span), F32)
        for i in range(group_pairs):
            p = g * group_pairs + i
            cols = shifted(cum, p)
            reach = jnp.exp(-pair_wide(cols[:, 0:1], cols[:, 1:2], width))
            carried = jnp.dot(read_ref[...], prior[p], preferred_element_type=F32) * reach
            gating = gate_ref[:, lanes(p)].astype(F32)
            value = (mixed[p] + carried) * (gating / (1.0 + jnp.exp(-gating)))
            gated[i] = value
            squares = squares + value * value
        scale = lax.rsqrt(jnp.sum(squares, axis=1, keepdims=True) / GRP + epsilon)
        for i in range(group_pairs):
            p = g * group_pairs + i
            value = (gated[i] * scale * gain_ref[:, lanes(p)]).astype(BF)
            lo = (i % piece_pairs) * span
            blocks[me, g * group_pieces + i // piece_pairs, :, lo : lo + span] = value
        for k in range(group_pieces):
            p = g * group_pieces + k
            pl.when(goes_up(p))(lambda: upward(me, p).start())
            pl.when(goes_down(p))(lambda: downward(me, p).start())
        return carry

    lax.fori_loop(0, columns // GRP, gate, 0)

    def multiply(slot, b, p):
        step = min(out_width, 256)
        fed = blocks[b, p]
        for lo in range(0, out_width, step):
            held = acc[slot, :, lo : lo + step]
            part = weight_ref[pl.ds(pl.multiple_of(p * piece, piece), piece), lo : lo + step]
            acc[slot, :, lo : lo + step] = jnp.where(p == 0, 0.0, held) + jnp.dot(
                fed, part, preferred_element_type=F32
            )

    def core_copy(b, kind):
        return remote(
            parts.at[kind, b, 1 - core], core_in.at[kind, b], core_send.at[kind, b],
            core_recv.at[kind, b], {"heads": head + 1 - 2 * core},
        )

    def round_partial(b, slot, kind=0):
        for k in range(cores):
            parts[kind, b, k] = acc[slot, :, k * half : (k + 1) * half].astype(BF)
        core_copy(b, kind).start()

    def chip_copy(b, k, kind):
        to = (chip + k) % chips
        return remote(
            chip_out.at[kind, b, to], x_in.at[kind, b, k], x_send.at[kind, b, k],
            x_recv.at[kind, b, k], {"heads": to * cores + core},
        )

    def sum_cores(b, kind=0):
        core_copy(b, kind).wait_recv()
        for k in range(chips):
            part = slice(k * strip, (k + 1) * strip)
            both = parts[kind, b, core, part].astype(F32) + core_in[kind, b, part].astype(F32)
            chip_out[kind, b, k] = both.astype(BF)
        for k in range(1, chips):
            chip_copy(b, k, kind).start()

    def local_final(b, column):
        return jnp.logical_and(b == me, head == column // share)

    def final_copy(b, column, kind):
        return remote(
            fin_out.at[kind, b], final.at[column % share, head], fin_send.at[kind, b],
            fin_recv.at[column % share, head], {"ctx": b, "heads": column // share},
        )

    def strip_copy(b):
        return remote(
            fin_out.at[0, b], strips.at[b], fin_send.at[0, b], strip_recv.at[b],
            {"ctx": beside_here},
        )

    def to_beside(b):
        if not lent:
            return False
        return jnp.logical_and(at_end, b != me)

    def strip_total(b, kind):
        part = pl.ds(pl.multiple_of(chip * strip, strip), strip)
        total = parts[kind, b, core, part].astype(F32) + core_in[kind, b, part].astype(F32)
        for k in range(1, chips):
            chip_copy(b, k, kind).wait_recv()
            total = total + x_in[kind, b, k].astype(F32)
        return total

    def deliver(b, column, kind, total):
        @pl.when(local_final(b, column))
        def _():
            final[column % share, head] = total.astype(BF)

        pl.when(jnp.logical_not(local_final(b, column)))(
            lambda: final_copy(b, column, kind).start()
        )

    def sum_chips(b):
        total = strip_total(b, 0)
        fin_out[0, b] = total.astype(BF)
        if lent:
            pl.when(to_beside(b))(lambda: strip_copy(b).start())
            pl.when(jnp.logical_not(to_beside(b)))(lambda: deliver(b, me, 0, total))
        else:
            deliver(b, me, 0, total)

    def helps(b):
        return jnp.logical_and(beside, b != end_here)

    def helping(b):
        @pl.when(helps(b))
        def _():
            step = min(out_width, 256)
            for lo in range(0, out_width, step):
                total = jnp.zeros((rows, step), F32)
                for k in range(lent):
                    part = borrowed[k * piece : (k + 1) * piece, lo : lo + step]
                    total = total + jnp.dot(
                        blocks[b, keep + k], part, preferred_element_type=F32
                    )
                acc[2, :, lo : lo + step] = total
            round_partial(b, 2, 1)

    def combine(b):
        @pl.when(helps(b))
        def _():
            strip_copy(b).wait_recv()
            total = strip_total(b, 1) + strips[b].astype(F32)
            fin_out[1, b] = total.astype(BF)
            deliver(b, end_here, 1, total)

    def own(p, carry):
        multiply(0, me, p)
        return carry

    lax.fori_loop(0, count, own, 0)
    round_partial(me, 0)

    def around(s, act):
        low, high = me - s, me + s
        pl.when(low >= 0)(lambda: act(jnp.maximum(low, 0), 0))

        @pl.when(jnp.logical_and(high < n, s > 0))
        def _():
            act(jnp.minimum(high, n - 1), 1)

    def both_sides(s, act):
        around(s, lambda b, slot: act(b))

    def step(i, carry):
        s, p = 1 + i // count, i % count
        low, high = me - s, me + s
        low_spot, high_spot = jnp.maximum(low, 0), jnp.minimum(high, n - 1)
        wanted = needed(p)

        @pl.when(jnp.logical_and(low >= 0, wanted))
        def _():
            upward(low_spot, p).wait_recv()
            pl.when(goes_up(p))(lambda: upward(low_spot, p).start())

        @pl.when(jnp.logical_and(high < n, wanted))
        def _():
            downward(high_spot, p).wait_recv()
            pl.when(goes_down(p))(lambda: downward(high_spot, p).start())

        pl.when(wanted)(lambda: around(s, lambda b, slot: multiply(slot, b, p)))
        last = jnp.where(at_end, keep - 1, count - 1)
        pl.when(p == last)(lambda: around(s, round_partial))

        def at(spot, act):
            pl.when(p == min(spot, count - 1))(lambda: both_sides(s - 1, act))

        at(0, sum_cores)
        at(1, sum_chips)
        if lent:
            @pl.when(jnp.logical_and(i == 0, beside))
            def _():
                lend().wait_recv()

            at(2, helping)
            at(3, lambda b: pl.when(helps(b))(lambda: sum_cores(b, 1)))
        return carry

    lax.fori_loop(0, (n - 1) * count, step, 0)
    both_sides(n - 1, sum_cores)
    both_sides(n - 1, sum_chips)
    if lent:
        for s in range(n - 1):
            both_sides(s, combine)
    loads[8].wait()

    for j in range(share):
        source = head * share + j
        if lent:
            outer = jnp.logical_and(source != me, jnp.logical_or(source == 0, source == n - 1))
            source = jnp.where(outer, jnp.where(source == 0, 1, n - 2), source)
        for k in range(heads):
            here = jnp.logical_and(source == me, k == head)

            @pl.when(jnp.logical_not(here))
            def _():
                remote(
                    fin_out.at[0, 0], final.at[j, k], fin_send.at[0, 0], fin_recv.at[j, k],
                    {"ctx": source, "heads": k},
                ).wait_recv()

            part = slice((k // cores) * strip, (k // cores + 1) * strip)
            lo = j * out_width + (k % cores) * half
            out_ref[part, lo : lo + half] = (
                resid_ref[part, lo : lo + half].astype(F32) + final[j, k].astype(F32)
            )

    for q in range(pairs):
        pl.when(has_next)(lambda: chain_copy(q).wait_send())
    for b in range(n):
        for p in range(count):
            pl.when(jnp.logical_and(goes_up(p), b <= me))(lambda: upward(b, p).wait_send())
            pl.when(jnp.logical_and(goes_down(p), b >= me))(lambda: downward(b, p).wait_send())
        core_copy(b, 0).wait_send()
        for k in range(1, chips):
            chip_copy(b, k, 0).wait_send()
        sent = jnp.logical_or(to_beside(b), jnp.logical_not(local_final(b, me)))
        pl.when(sent)(lambda: final_copy(b, me, 0).wait_send())

        if lent:
            @pl.when(helps(b))
            def _():
                core_copy(b, 1).wait_send()
                for k in range(1, chips):
                    chip_copy(b, k, 1).wait_send()
                pl.when(jnp.logical_not(local_final(b, end_here)))(
                    lambda: final_copy(b, end_here, 1).wait_send()
                )

    if lent:
        pl.when(at_end)(lambda: lend().wait_send())


def slots_kernel(
    n, heads, width, features, src_ref, out_ref,
    first, middle, second, third,
    first_send, first_recv, second_send, second_recv, third_send, third_recv,
):
    me, head = lax.axis_index("ctx"), lax.axis_index("heads")

    for k in range(1, heads):
        greet({"heads": (head + k) % heads})
    for k in range(1, n):
        greet({"ctx": (me + k) % n})
    greeted(heads + n - 2)

    def first_copy(k):
        to = (head + k) % heads
        return remote(
            src_ref.at[to], first.at[k], first_send.at[k], first_recv.at[k], {"heads": to}
        )

    def second_copy(k):
        to = (me + k) % n
        return remote(
            middle.at[to], second.at[me], second_send.at[k], second_recv.at[k], {"ctx": to}
        )

    def third_copy(k):
        to = (head + k) % heads
        return remote(second, third.at[k], third_send.at[k], third_recv.at[k], {"heads": to})

    for k in range(1, heads):
        first_copy(k).start()
    total = src_ref[head].astype(F32)
    for k in range(1, heads):
        first_copy(k).wait_recv()
        total = total + first[k].astype(F32)
    if src_ref.shape[-1] > width:
        power = total[:, :, width : width + 1]
        total = total[:, :, :width] * lax.rsqrt(power / features + epsilon)
    middle[...] = total.astype(BF)
    for k in range(1, n):
        second_copy(k).start()
    second[me] = middle[me]
    for k in range(1, n):
        second_copy(k).wait_recv()
    for k in range(1, heads):
        third_copy(k).start()
    out_ref[head] = second[...]
    for k in range(1, heads):
        third_copy(k).wait_recv()
        out_ref[(head + heads - k) % heads] = third[k]
    for k in range(1, heads):
        first_copy(k).wait_send()
        third_copy(k).wait_send()
    for k in range(1, n):
        second_copy(k).wait_send()


def reaching(collective_id):
    return pltpu.CompilerParams(
        collective_id=collective_id, has_side_effects=True, vmem_limit_bytes=48 * 1024 * 1024
    )


def dma(*shape):
    return pltpu.SemaphoreType.DMA(shape)


def through_slots(pieces, width, features, collective_id):
    heads, n, rows, wide = pieces.shape
    return pl.pallas_call(
        functools.partial(slots_kernel, n, heads, width, features),
        out_shape=jax.ShapeDtypeStruct((heads, n, rows, width), BF),
        in_specs=vmem(),
        out_specs=vmem()[0],
        scratch_shapes=[
            pltpu.VMEM((heads, n, rows, wide), BF),
            pltpu.VMEM((n, rows, width), BF),
            pltpu.VMEM((n, rows, width), BF),
            pltpu.VMEM((heads, n, rows, width), BF),
            dma(heads), dma(heads), dma(n), dma(n), dma(heads), dma(heads),
        ],
        compiler_params=reaching(collective_id),
    )(pieces)


def mixer(
    ssm_input, decay_log, state_write, state_read, skip_scale, gate_input, ssm_gain, weight, residual_in
):
    n, heads = lax.axis_size("ctx"), lax.axis_size("heads")
    rows, columns = ssm_input.shape
    head_count = decay_log.shape[1]
    width = columns // head_count
    states = state_write.shape[1]
    span = 2 * width
    pairs = columns // span
    piece = GRP // 4
    count = columns // piece
    lent = LENT_NUM * count // LENT_DEN if n > 3 else 0
    out_width = weight.shape[1]
    share = n // heads
    chips = heads // 2
    half, strip = out_width // 2, rows // chips
    lane_count = -(-head_count // 128) * 128
    block = (rows, out_width)
    anywhere = pl.BlockSpec(memory_space=pl.ANY)
    return pl.pallas_call(
        functools.partial(mixer_kernel, n, heads, width, piece, 3, lent),
        out_shape=jax.ShapeDtypeStruct((rows, share * out_width), F32),
        in_specs=[anywhere] * 9,
        out_specs=vmem()[0],
        scratch_shapes=[
            pltpu.VMEM((rows, columns), BF),
            pltpu.VMEM((rows, states), BF),
            pltpu.VMEM((rows, states), BF),
            pltpu.VMEM((head_count, rows), F32),
            pltpu.VMEM((1, head_count), F32),
            pltpu.VMEM(weight.shape, BF),
            pltpu.VMEM((rows, columns), BF),
            pltpu.VMEM((1, columns), F32),
            pltpu.VMEM(residual_in.shape, BF),
            pltpu.VMEM((rows, lane_count), F32),
            pltpu.VMEM((head_count, rows), F32),
            pltpu.VMEM((8, lane_count), F32),
            pltpu.VMEM((rows, rows), F32),
            pltpu.VMEM((pairs, rows, span), F32),
            pltpu.VMEM((pairs, states, span), F32),
            pltpu.VMEM((pairs, 1, span), F32),
            pltpu.VMEM((pairs, states, span), BF),
            pltpu.VMEM((pairs, states, span), BF),
            pltpu.VMEM((GRP // span, rows, span), F32),
            pltpu.VMEM((n, count, rows, piece), BF),
            pltpu.VMEM((3,) + block, F32),
            pltpu.VMEM((2, n, 2, rows, half), BF),
            pltpu.VMEM((2, n, rows, half), BF),
            pltpu.VMEM((2, n, chips, strip, half), BF),
            pltpu.VMEM((2, n, chips, strip, half), BF),
            pltpu.VMEM((2, n, strip, half), BF),
            pltpu.VMEM((share, heads, strip, half), BF),
            pltpu.VMEM((max(lent, 1) * piece, out_width), BF),
            pltpu.VMEM((n, strip, half), BF),
            dma(9), dma(pairs), dma(pairs),
            dma(n, count), dma(n, count), dma(n, count), dma(n, count),
            dma(2, n), dma(2, n), dma(2, n, chips), dma(2, n, chips), dma(2, n), dma(share, heads),
            dma(1), dma(1), dma(n),
        ],
        compiler_params=reaching(1),
    )(
        ssm_input, state_write, state_read, decay_log.T, skip_scale.reshape(1, head_count), weight,
        gate_input, ssm_gain.reshape(1, columns), residual_in,
    )


def local(
    ssm_input,
    decay_log,
    state_write,
    state_read,
    skip_scale,
    gate_input,
    ssm_gain,
    out_weight,
    residual_in,
    moe_gain,
    down_latent,
    expert_up,
    expert_down,
    up_latent,
    expert_ids,
    combine_fixed,
):
    row_count = ssm_input.shape[0]
    n, heads = lax.axis_size("ctx"), lax.axis_size("heads")
    features = residual_in.shape[1] * heads
    latent_width = down_latent.shape[1]
    piece = latent_width // heads
    experts_here = expert_up.shape[0]
    wave_size = experts_here * n
    slot_rows = experts_here * CAP

    matches = expert_ids[:, :, None] == jnp.arange(wave_size)[None, None, :]
    chosen = jnp.any(matches, axis=1).astype(jnp.int32)
    weight_fixed = jnp.sum(jnp.where(matches, combine_fixed[:, :, None], 0), axis=1)
    slot_index = jnp.cumsum(chosen, axis=0) - 1
    placed = (chosen[:, :, None] == 1) & (slot_index[:, :, None] == jnp.arange(CAP)[None, None, :])
    route_weight = (weight_fixed.astype(F32) / 65536.0).astype(BF)
    combine_table = jnp.where(placed, route_weight[:, :, None], jnp.zeros((), BF)).reshape(
        row_count, wave_size * CAP
    )
    placed = placed.astype(BF).reshape(row_count, wave_size * CAP)

    residual = mixer(
        ssm_input, decay_log, state_write, state_read, skip_scale, gate_input, ssm_gain,
        out_weight, residual_in,
    )
    scaled = (residual * moe_gain).astype(BF)
    latent_part = jnp.dot(scaled, down_latent, preferred_element_type=F32).astype(BF)
    squares = jnp.sum(residual * residual, axis=1).astype(BF)
    side = jnp.concatenate(
        [latent_part, jnp.broadcast_to(squares[:, None], (row_count, 128))], axis=1
    )
    slots = lax.dot_general(
        placed, side, (((0,), (0,)), ((), ())), preferred_element_type=F32
    ).astype(BF)
    slots = slots.reshape(n, slot_rows, latent_width + 128)
    pieces = jnp.stack(
        [
            jnp.concatenate(
                [slots[:, :, h * piece : (h + 1) * piece], slots[:, :, latent_width:]], axis=2
            )
            for h in range(heads)
        ]
    )
    incoming = through_slots(pieces, piece, features, 3)
    incoming = incoming.reshape(heads, n, experts_here, CAP, piece).transpose(2, 1, 3, 0, 4)
    incoming = incoming.reshape(experts_here, n * CAP, latent_width)
    hidden = jnp.einsum("esl,elf->esf", incoming, expert_up, preferred_element_type=F32)
    hidden = (jnp.maximum(hidden, 0.0) ** 2).astype(BF)
    expert_out = jnp.einsum("esf,efl->esl", hidden, expert_down, preferred_element_type=F32)
    expert_out = expert_out.astype(BF).reshape(experts_here, n, CAP, heads, piece)
    expert_out = expert_out.transpose(3, 1, 0, 2, 4).reshape(heads, n, slot_rows, piece)
    returned = through_slots(expert_out, piece, features, 4)
    returned = returned.transpose(1, 2, 0, 3).reshape(wave_size * CAP, latent_width)
    combined = jnp.dot(combine_table, returned, preferred_element_type=F32)
    moe_out = jnp.dot(combined.astype(BF), up_latent, preferred_element_type=F32)
    return (residual + moe_out).astype(BF)


def solution(mesh):
    placed = (
        P(("groups", "ctx"), "heads"),
        P(("groups", "ctx"), "heads"),
        P(("groups", "ctx"), None),
        P(("groups", "ctx"), None),
        P("heads"),
        P(("groups", "ctx"), "heads"),
        P("heads"),
        P("heads", "ctx"),
        P(("groups", "ctx"), "heads"),
        P("heads"),
        P("heads", None),
        P("ctx", None, "heads"),
        P("ctx", "heads", None),
        P(None, "heads"),
        P(("groups", "ctx"), None),
        P(("groups", "ctx"), None),
    )
    return jax.shard_map(
        local, mesh=mesh, in_specs=placed, out_specs=P(("groups", "ctx"), "heads"), check_vma=False
    )
```

```python
import functools

import jax
import jax.numpy as jnp
from jax import lax
from jax.experimental import pallas as pl
from jax.experimental.pallas import tpu as pltpu
from jax.sharding import PartitionSpec as P

D = 4096
GRP = 1024
LAT = 1024
CAP = 16
LENT_NUM, LENT_DEN = 3, 8


epsilon = 1e-05


MESH = pl.DeviceIdType.MESH
BF = jnp.bfloat16
F32 = jnp.float32


def vmem(count=1):
    return [pl.BlockSpec(memory_space=pltpu.VMEM)] * count


def greet(device):
    pl.semaphore_signal(
        pltpu.get_barrier_semaphore(), inc=1, device_id=device, device_id_type=MESH
    )


def greeted(count):
    pl.semaphore_wait(pltpu.get_barrier_semaphore(), count)


def one_if(condition):
    return jnp.where(condition, 1, 0)


def remote(src, dst, send, recv, device):
    return pltpu.make_async_remote_copy(
        src_ref=src, dst_ref=dst, send_sem=send, recv_sem=recv, device_id=device, device_id_type=MESH
    )


def pair_wide(first, second, width):
    lane = lax.broadcasted_iota(jnp.int32, (first.shape[0], 2 * width), 1)
    return jnp.where(lane < width, first, second)


def mixer_kernel(
    n, heads, groups, width, piece, lag, lent,
    x_hbm, write_hbm, read_hbm, decay_hbm, skip_hbm, weight_hbm, gate_hbm, gain_hbm, resid_hbm,
    out_ref,
    x_ref, write_ref, read_ref, decay_ref, skip_ref, weight_ref, gate_ref, gain_ref, resid_ref,
    cum, cum_rows, skips, inter,
    mixed, state, ends, prior, outgoing, gated,
    blocks, acc, parts, core_in, chip_out, x_in, fin_out, final, borrowed, strips,
    load_sem, chain_send, chain_recv, up_send, up_recv, down_send, down_recv,
    core_send, core_recv, x_send, x_recv, fin_send, fin_recv, lend_send, lend_recv, spread_send, spread_recv, strip_recv,
):
    me, head, group = lax.axis_index("ctx"), lax.axis_index("heads"), lax.axis_index("groups")
    rows, columns = x_ref.shape
    span = 2 * width
    pairs = columns // span
    head_count = decay_ref.shape[0]
    out_width = weight_ref.shape[1]
    count = columns // piece
    share = n // heads
    cores = 2
    chips = heads // cores
    core, chip = head % cores, head // cores
    half, strip = out_width // cores, rows // chips
    has_prev, has_next = me > 0, me < n - 1
    prev, after = jnp.maximum(me - 1, 0), jnp.minimum(me + 1, n - 1)
    keep = count - lent
    at_end = jnp.logical_or(me == 0, me == n - 1)
    beside = jnp.logical_or(me == 1, me == n - 2)
    end_here = jnp.where(me == 1, 0, n - 1)
    beside_here = jnp.where(me == 0, 1, n - 2)

    loads = [
        pltpu.make_async_copy(src, dst, load_sem.at[i])
        for i, (src, dst) in enumerate(
            [
                (x_hbm, x_ref), (write_hbm, write_ref), (read_hbm, read_ref), (decay_hbm, decay_ref),
                (skip_hbm, skip_ref), (weight_hbm, weight_ref), (gate_hbm, gate_ref),
                (gain_hbm, gain_ref), (resid_hbm, resid_ref),
            ]
        )
    ]
    for load in loads:
        load.start()
    for i in range(n):
        for j in range(heads):
            if i or j:
                greet({"ctx": (me + i) % n, "heads": (head + j) % heads})
    for i in range(1, groups):
        greet({"groups": (group + i) % groups})

    t = lax.broadcasted_iota(jnp.int32, (rows, rows), 0)
    s = lax.broadcasted_iota(jnp.int32, (rows, rows), 1)
    lower = jnp.where(t >= s, 1.0, 0.0)
    cum[...] = jnp.zeros(cum.shape, F32)
    for load in loads[:5]:
        load.wait()
    cum[:, :head_count] = lax.dot_general(
        lower, decay_ref[...], (((1,), (1,)), ((), ())),
        precision=lax.Precision.HIGHEST, preferred_element_type=F32,
    )
    cum_rows[...] = lax.dot_general(
        decay_ref[...], lower, (((1,), (1,)), ((), ())),
        precision=lax.Precision.HIGHEST, preferred_element_type=F32,
    )
    skips[...] = jnp.zeros(skips.shape, F32)
    skips[0:1, :head_count] = skip_ref[...]
    product = lax.dot_general(
        read_ref[...], write_ref[...], (((1,), (1,)), ((), ())), preferred_element_type=F32
    )
    inter[...] = jnp.where(t >= s, product, 0.0)
    greeted(n * heads + groups - 2)

    share_rows = piece // groups

    def lend(k):
        return remote(
            weight_ref.at[pl.ds((keep + k) * piece + group * share_rows, share_rows)],
            borrowed.at[pl.ds(k * piece + group * share_rows, share_rows)],
            lend_send.at[k], lend_recv.at[k], {"ctx": beside_here},
        )

    def spread(k, i, back=False):
        owner = (group + groups - i) % groups if back else group
        part = borrowed.at[pl.ds(k * piece + owner * share_rows, share_rows)]
        return remote(
            part, part, spread_send.at[k, i], spread_recv.at[k, i],
            {"groups": (group + i) % groups},
        )

    @pl.when(me == n - 1)
    def _():
        loads[5].wait()
        for k in range(lent):
            lend(k).start()

    def lanes(p):
        return pl.ds(pl.multiple_of(p * span, span), span)

    def shifted(ref, p):
        lane_count = ref.shape[1]
        return pltpu.roll(ref[...], (lane_count - 2 * p) % lane_count, 1)

    band = rows // 2
    causal = lax.broadcasted_iota(jnp.int32, (band, band), 0) >= lax.broadcasted_iota(
        jnp.int32, (band, band), 1
    )

    def scan(p):
        x = x_ref[:, lanes(p)]
        cols = shifted(cum, p)
        skip = shifted(skips, p)
        outs, tails, lasts = [], [], []
        for j in range(2):
            col = cols[:, j : j + 1]
            row = cum_rows[pl.ds(2 * p + j, 1), :]
            last = col[rows - 1 : rows, :]
            lane = x[:, j * width : (j + 1) * width]
            bands = []
            for lo in range(0, rows, band):
                hi = lo + band
                spread = jnp.where(causal, col[lo:hi] - row[:, lo:hi], 0.0)
                if lo:
                    spread = jnp.concatenate([col[lo:hi] - row[:, :lo], spread], axis=1)
                mixing = (jnp.exp(-spread) * inter[lo:hi, :hi]).astype(BF)
                bands.append(jnp.dot(mixing, lane[:hi], preferred_element_type=F32))
            outs.append(jnp.concatenate(bands, axis=0))
            tails.append(jnp.exp(col - last))
            lasts.append(jnp.exp(-last))
        wide = x.astype(F32)
        direct = pair_wide(skip[0:1, 0:1], skip[0:1, 1:2], width) * wide
        mixed[p] = jnp.concatenate(outs, axis=1) + direct
        scaled = (wide * pair_wide(tails[0], tails[1], width)).astype(BF)
        state[p] = lax.dot_general(
            write_ref[...], scaled, (((0,), (0,)), ((), ())), preferred_element_type=F32
        )
        ends[p] = pair_wide(lasts[0], lasts[1], width)

    def chain_copy(q):
        return remote(
            outgoing.at[q], prior.at[q], chain_send.at[q], chain_recv.at[q], {"ctx": after}
        )

    def chain(q):
        @pl.when(me == 0)
        def _():
            prior[q] = jnp.zeros(prior.shape[1:], BF)
            outgoing[q] = state[q].astype(BF)

        @pl.when(has_prev)
        def _():
            chain_copy(q).wait_recv()
            outgoing[q] = (prior[q].astype(F32) * ends[q] + state[q]).astype(BF)

        pl.when(has_next)(lambda: chain_copy(q).start())

    def advance(i, carry):
        pl.when(i < pairs)(lambda: scan(i))
        q = i - lag * me
        pl.when(jnp.logical_and(q >= 0, q < pairs))(lambda: chain(q))
        return carry

    lax.fori_loop(0, pairs + lag * (n - 1), advance, 0)

    def upward(b, p):
        spot = blocks.at[b, p]
        return remote(spot, spot, up_send.at[b, p], up_recv.at[b, p], {"ctx": after})

    def downward(b, p):
        spot = blocks.at[b, p]
        return remote(spot, spot, down_send.at[b, p], down_recv.at[b, p], {"ctx": prev})

    pl.when(me < n - 1)(lambda: loads[5].wait())

    def goes_up(p):
        return jnp.logical_and(has_next, jnp.logical_or(p < keep, me + 1 < n - 1))

    def goes_down(p):
        return jnp.logical_and(has_prev, jnp.logical_or(p < keep, me > 1))

    def needed(p):
        return jnp.logical_or(p < keep, jnp.logical_not(at_end))

    group_pairs = GRP // span
    group_pieces = GRP // piece
    piece_pairs = piece // span
    loads[6].wait()
    loads[7].wait()

    def gate(g, carry):
        squares = jnp.zeros((rows, span), F32)
        for i in range(group_pairs):
            p = g * group_pairs + i
            cols = shifted(cum, p)
            reach = jnp.exp(-pair_wide(cols[:, 0:1], cols[:, 1:2], width))
            carried = jnp.dot(read_ref[...], prior[p], preferred_element_type=F32) * reach
            gating = gate_ref[:, lanes(p)].astype(F32)
            value = (mixed[p] + carried) * (gating / (1.0 + jnp.exp(-gating)))
            gated[i] = value
            squares = squares + value * value
        scale = lax.rsqrt(jnp.sum(squares, axis=1, keepdims=True) / GRP + epsilon)
        for i in range(group_pairs):
            p = g * group_pairs + i
            value = (gated[i] * scale * gain_ref[:, lanes(p)]).astype(BF)
            lo = (i % piece_pairs) * span
            blocks[me, g * group_pieces + i // piece_pairs, :, lo : lo + span] = value
        for k in range(group_pieces):
            p = g * group_pieces + k
            pl.when(goes_up(p))(lambda: upward(me, p).start())
            pl.when(goes_down(p))(lambda: downward(me, p).start())
        return carry

    lax.fori_loop(0, columns // GRP, gate, 0)
    for k in range(lent):
        pl.when(me == 0)(lambda: lend(k).start())

    def multiply(slot, b, p):
        step = min(out_width, 256)
        fed = blocks[b, p]
        for lo in range(0, out_width, step):
            held = acc[slot, :, lo : lo + step]
            part = weight_ref[pl.ds(pl.multiple_of(p * piece, piece), piece), lo : lo + step]
            acc[slot, :, lo : lo + step] = jnp.where(p == 0, 0.0, held) + jnp.dot(
                fed, part, preferred_element_type=F32
            )

    def core_copy(b, kind):
        return remote(
            parts.at[kind, b, 1 - core], core_in.at[kind, b], core_send.at[kind, b],
            core_recv.at[kind, b], {"heads": head + 1 - 2 * core},
        )

    def round_partial(b, slot, kind=0):
        for k in range(cores):
            parts[kind, b, k] = acc[slot, :, k * half : (k + 1) * half].astype(BF)
        core_copy(b, kind).start()

    def chip_copy(b, k, kind):
        to = (chip + k) % chips
        return remote(
            chip_out.at[kind, b, to], x_in.at[kind, b, k], x_send.at[kind, b, k],
            x_recv.at[kind, b, k], {"heads": to * cores + core},
        )

    def sum_cores(b, kind=0):
        core_copy(b, kind).wait_recv()
        for k in range(chips):
            part = slice(k * strip, (k + 1) * strip)
            both = parts[kind, b, core, part].astype(F32) + core_in[kind, b, part].astype(F32)
            chip_out[kind, b, k] = both.astype(BF)
        for k in range(1, chips):
            chip_copy(b, k, kind).start()

    def local_final(b, column):
        return jnp.logical_and(b == me, head == column // share)

    def final_copy(b, column, kind):
        return remote(
            fin_out.at[kind, b], final.at[column % share, head], fin_send.at[kind, b],
            fin_recv.at[column % share, head], {"ctx": b, "heads": column // share},
        )

    def strip_copy(b):
        return remote(
            fin_out.at[0, b], strips.at[b], fin_send.at[0, b], strip_recv.at[b],
            {"ctx": beside_here},
        )

    def to_beside(b):
        if not lent:
            return False
        return jnp.logical_and(at_end, b != me)

    def strip_total(b, kind):
        part = pl.ds(pl.multiple_of(chip * strip, strip), strip)
        total = parts[kind, b, core, part].astype(F32) + core_in[kind, b, part].astype(F32)
        for k in range(1, chips):
            chip_copy(b, k, kind).wait_recv()
            total = total + x_in[kind, b, k].astype(F32)
        return total

    def deliver(b, column, kind, total):
        @pl.when(local_final(b, column))
        def _():
            final[column % share, head] = total.astype(BF)

        pl.when(jnp.logical_not(local_final(b, column)))(
            lambda: final_copy(b, column, kind).start()
        )

    def sum_chips(b):
        total = strip_total(b, 0)
        fin_out[0, b] = total.astype(BF)
        if lent:
            pl.when(to_beside(b))(lambda: strip_copy(b).start())
            pl.when(jnp.logical_not(to_beside(b)))(lambda: deliver(b, me, 0, total))
        else:
            deliver(b, me, 0, total)

    def helps(b):
        return jnp.logical_and(beside, b != end_here)

    def helping(b):
        @pl.when(helps(b))
        def _():
            step = min(out_width, 256)
            for lo in range(0, out_width, step):
                total = jnp.zeros((rows, step), F32)
                for k in range(lent):
                    part = borrowed[k * piece : (k + 1) * piece, lo : lo + step]
                    total = total + jnp.dot(
                        blocks[b, keep + k], part, preferred_element_type=F32
                    )
                acc[2, :, lo : lo + step] = total
            round_partial(b, 2, 1)

    def combine(b):
        @pl.when(helps(b))
        def _():
            strip_copy(b).wait_recv()
            total = strip_total(b, 1) + strips[b].astype(F32)
            fin_out[1, b] = total.astype(BF)
            deliver(b, end_here, 1, total)

    def own(p, carry):
        multiply(0, me, p)
        return carry

    lax.fori_loop(0, count, own, 0)
    round_partial(me, 0)

    def around(s, act):
        low, high = me - s, me + s
        pl.when(low >= 0)(lambda: act(jnp.maximum(low, 0), 0))

        @pl.when(jnp.logical_and(high < n, s > 0))
        def _():
            act(jnp.minimum(high, n - 1), 1)

    def both_sides(s, act):
        around(s, lambda b, slot: act(b))

    def step(i, carry):
        s, p = 1 + i // count, i % count
        low, high = me - s, me + s
        low_spot, high_spot = jnp.maximum(low, 0), jnp.minimum(high, n - 1)
        wanted = needed(p)

        @pl.when(jnp.logical_and(low >= 0, wanted))
        def _():
            upward(low_spot, p).wait_recv()
            pl.when(goes_up(p))(lambda: upward(low_spot, p).start())

        @pl.when(jnp.logical_and(high < n, wanted))
        def _():
            downward(high_spot, p).wait_recv()
            pl.when(goes_down(p))(lambda: downward(high_spot, p).start())

        pl.when(wanted)(lambda: around(s, lambda b, slot: multiply(slot, b, p)))
        last = jnp.where(at_end, keep - 1, count - 1)
        pl.when(p == last)(lambda: around(s, round_partial))

        def at(spot, act):
            pl.when(p == min(spot, count - 1))(lambda: both_sides(s - 1, act))

        at(0, sum_cores)
        at(1, sum_chips)
        def reduce_help(b):
            pl.when(helps(b))(lambda: sum_cores(b, 1))

        for k in range(lent):
            @pl.when(jnp.logical_and(beside, i == (n - 3) * count + min(2 * (k + 1), count - 1)))
            def _():
                lend(k).wait_recv()
                for g in range(1, groups):
                    spread(k, g).start()

        if lent:
            @pl.when(i == (n - 2) * count - 1)
            def _():
                @pl.when(beside)
                def _():
                    for k in range(lent):
                        for g in range(1, groups):
                            spread(k, g, True).wait_recv()

                for r in range(n - 2):
                    both_sides(r, helping)

            @pl.when(i == (n - 2) * count)
            def _():
                both_sides(n - 2, helping)
                for r in range(n - 2):
                    both_sides(r, reduce_help)

            pl.when(i == (n - 2) * count + 1)(lambda: both_sides(n - 2, reduce_help))
        return carry

    lax.fori_loop(0, (n - 1) * count, step, 0)
    both_sides(n - 1, sum_cores)
    both_sides(n - 1, sum_chips)
    if lent:
        for s in range(n - 1):
            both_sides(s, combine)
    loads[8].wait()

    for j in range(share):
        source = head * share + j
        if lent:
            outer = jnp.logical_and(source != me, jnp.logical_or(source == 0, source == n - 1))
            source = jnp.where(outer, jnp.where(source == 0, 1, n - 2), source)
        for k in range(heads):
            here = jnp.logical_and(source == me, k == head)

            @pl.when(jnp.logical_not(here))
            def _():
                remote(
                    fin_out.at[0, 0], final.at[j, k], fin_send.at[0, 0], fin_recv.at[j, k],
                    {"ctx": source, "heads": k},
                ).wait_recv()

            part = slice((k // cores) * strip, (k // cores + 1) * strip)
            lo = j * out_width + (k % cores) * half
            out_ref[part, lo : lo + half] = (
                resid_ref[part, lo : lo + half].astype(F32) + final[j, k].astype(F32)
            )

    for q in range(pairs):
        pl.when(has_next)(lambda: chain_copy(q).wait_send())
    for b in range(n):
        for p in range(count):
            pl.when(jnp.logical_and(goes_up(p), b <= me))(lambda: upward(b, p).wait_send())
            pl.when(jnp.logical_and(goes_down(p), b >= me))(lambda: downward(b, p).wait_send())
        core_copy(b, 0).wait_send()
        for k in range(1, chips):
            chip_copy(b, k, 0).wait_send()
        sent = jnp.logical_or(to_beside(b), jnp.logical_not(local_final(b, me)))
        pl.when(sent)(lambda: final_copy(b, me, 0).wait_send())

        if lent:
            @pl.when(helps(b))
            def _():
                core_copy(b, 1).wait_send()
                for k in range(1, chips):
                    chip_copy(b, k, 1).wait_send()
                pl.when(jnp.logical_not(local_final(b, end_here)))(
                    lambda: final_copy(b, end_here, 1).wait_send()
                )

    for k in range(lent):
        pl.when(at_end)(lambda: lend(k).wait_send())
        for g in range(1, groups):
            pl.when(beside)(lambda: spread(k, g).wait_send())


def slots_kernel(
    n, heads, width, features, src_ref, out_ref,
    first, middle, second, third,
    first_send, first_recv, second_send, second_recv, third_send, third_recv,
):
    me, head = lax.axis_index("ctx"), lax.axis_index("heads")

    for k in range(1, heads):
        greet({"heads": (head + k) % heads})
    for k in range(1, n):
        greet({"ctx": (me + k) % n})
    greeted(heads + n - 2)

    def first_copy(k):
        to = (head + k) % heads
        return remote(
            src_ref.at[to], first.at[k], first_send.at[k], first_recv.at[k], {"heads": to}
        )

    def second_copy(k):
        to = (me + k) % n
        return remote(
            middle.at[to], second.at[me], second_send.at[k], second_recv.at[k], {"ctx": to}
        )

    def third_copy(k):
        to = (head + k) % heads
        return remote(second, third.at[k], third_send.at[k], third_recv.at[k], {"heads": to})

    for k in range(1, heads):
        first_copy(k).start()
    total = src_ref[head].astype(F32)
    for k in range(1, heads):
        first_copy(k).wait_recv()
        total = total + first[k].astype(F32)
    if src_ref.shape[-1] > width:
        power = total[:, :, width : width + 1]
        total = total[:, :, :width] * lax.rsqrt(power / features + epsilon)
    middle[...] = total.astype(BF)
    for k in range(1, n):
        second_copy(k).start()
    second[me] = middle[me]
    for k in range(1, n):
        second_copy(k).wait_recv()
    for k in range(1, heads):
        third_copy(k).start()
    out_ref[head] = second[...]
    for k in range(1, heads):
        third_copy(k).wait_recv()
        out_ref[(head + heads - k) % heads] = third[k]
    for k in range(1, heads):
        first_copy(k).wait_send()
        third_copy(k).wait_send()
    for k in range(1, n):
        second_copy(k).wait_send()


def reaching(collective_id, grant=48 * 1024 * 1024):
    return pltpu.CompilerParams(
        collective_id=collective_id, has_side_effects=True, vmem_limit_bytes=grant
    )


def dma(*shape):
    return pltpu.SemaphoreType.DMA(shape)


def through_slots(pieces, width, features, collective_id):
    heads, n, rows, wide = pieces.shape
    return pl.pallas_call(
        functools.partial(slots_kernel, n, heads, width, features),
        out_shape=jax.ShapeDtypeStruct((heads, n, rows, width), BF),
        in_specs=vmem(),
        out_specs=vmem()[0],
        scratch_shapes=[
            pltpu.VMEM((heads, n, rows, wide), BF),
            pltpu.VMEM((n, rows, width), BF),
            pltpu.VMEM((n, rows, width), BF),
            pltpu.VMEM((heads, n, rows, width), BF),
            dma(heads), dma(heads), dma(n), dma(n), dma(heads), dma(heads),
        ],
        compiler_params=reaching(collective_id),
    )(pieces)


def mixer(
    ssm_input, decay_log, state_write, state_read, skip_scale, gate_input, ssm_gain, weight, residual_in
):
    n, heads, groups = lax.axis_size("ctx"), lax.axis_size("heads"), lax.axis_size("groups")
    rows, columns = ssm_input.shape
    head_count = decay_log.shape[1]
    width = columns // head_count
    states = state_write.shape[1]
    span = 2 * width
    pairs = columns // span
    piece = GRP // 4
    count = columns // piece
    lent = LENT_NUM * count // LENT_DEN if n > 3 else 0
    out_width = weight.shape[1]
    share = n // heads
    chips = heads // 2
    half, strip = out_width // 2, rows // chips
    lane_count = -(-head_count // 128) * 128
    block = (rows, out_width)
    anywhere = pl.BlockSpec(memory_space=pltpu.HBM)
    return pl.pallas_call(
        functools.partial(mixer_kernel, n, heads, groups, width, piece, 3, lent),
        out_shape=jax.ShapeDtypeStruct((rows, share * out_width), F32),
        in_specs=[anywhere] * 9,
        out_specs=vmem()[0],
        scratch_shapes=[
            pltpu.VMEM((rows, columns), BF),
            pltpu.VMEM((rows, states), BF),
            pltpu.VMEM((rows, states), BF),
            pltpu.VMEM((head_count, rows), F32),
            pltpu.VMEM((1, head_count), F32),
            pltpu.VMEM(weight.shape, BF),
            pltpu.VMEM((rows, columns), BF),
            pltpu.VMEM((1, columns), F32),
            pltpu.VMEM(residual_in.shape, BF),
            pltpu.VMEM((rows, lane_count), F32),
            pltpu.VMEM((head_count, rows), F32),
            pltpu.VMEM((8, lane_count), F32),
            pltpu.VMEM((rows, rows), F32),
            pltpu.VMEM((pairs, rows, span), F32),
            pltpu.VMEM((pairs, states, span), F32),
            pltpu.VMEM((pairs, 1, span), F32),
            pltpu.VMEM((pairs, states, span), BF),
            pltpu.VMEM((pairs, states, span), BF),
            pltpu.VMEM((GRP // span, rows, span), F32),
            pltpu.VMEM((n, count, rows, piece), BF),
            pltpu.VMEM((3,) + block, F32),
            pltpu.VMEM((2, n, 2, rows, half), BF),
            pltpu.VMEM((2, n, rows, half), BF),
            pltpu.VMEM((2, n, chips, strip, half), BF),
            pltpu.VMEM((2, n, chips, strip, half), BF),
            pltpu.VMEM((2, n, strip, half), BF),
            pltpu.VMEM((share, heads, strip, half), BF),
            pltpu.VMEM((max(lent, 1) * piece, out_width), BF),
            pltpu.VMEM((n, strip, half), BF),
            dma(9), dma(pairs), dma(pairs),
            dma(n, count), dma(n, count), dma(n, count), dma(n, count),
            dma(2, n), dma(2, n), dma(2, n, chips), dma(2, n, chips), dma(2, n), dma(share, heads),
            dma(max(lent, 1)), dma(max(lent, 1)), dma(max(lent, 1), groups), dma(max(lent, 1), groups), dma(n),
        ],
        compiler_params=reaching(1, 67043328),
    )(
        ssm_input, state_write, state_read, decay_log.T, skip_scale.reshape(1, head_count), weight,
        gate_input, ssm_gain.reshape(1, columns), residual_in,
    )


def local(
    ssm_input,
    decay_log,
    state_write,
    state_read,
    skip_scale,
    gate_input,
    ssm_gain,
    out_weight,
    residual_in,
    moe_gain,
    down_latent,
    expert_up,
    expert_down,
    up_latent,
    expert_ids,
    combine_fixed,
):
    row_count = ssm_input.shape[0]
    n, heads = lax.axis_size("ctx"), lax.axis_size("heads")
    features = residual_in.shape[1] * heads
    latent_width = down_latent.shape[1]
    piece = latent_width // heads
    experts_here = expert_up.shape[0]
    wave_size = experts_here * n
    slot_rows = experts_here * CAP

    matches = expert_ids[:, :, None] == jnp.arange(wave_size)[None, None, :]
    chosen = jnp.any(matches, axis=1).astype(jnp.int32)
    weight_fixed = jnp.sum(jnp.where(matches, combine_fixed[:, :, None], 0), axis=1)
    slot_index = jnp.cumsum(chosen, axis=0) - 1
    placed = (chosen[:, :, None] == 1) & (slot_index[:, :, None] == jnp.arange(CAP)[None, None, :])
    route_weight = (weight_fixed.astype(F32) / 65536.0).astype(BF)
    combine_table = jnp.where(placed, route_weight[:, :, None], jnp.zeros((), BF)).reshape(
        row_count, wave_size * CAP
    )
    placed = placed.astype(BF).reshape(row_count, wave_size * CAP)

    residual = mixer(
        ssm_input, decay_log, state_write, state_read, skip_scale, gate_input, ssm_gain,
        out_weight, residual_in,
    )
    scaled = (residual * moe_gain).astype(BF)
    latent_part = jnp.dot(scaled, down_latent, preferred_element_type=F32).astype(BF)
    squares = jnp.sum(residual * residual, axis=1).astype(BF)
    side = jnp.concatenate(
        [latent_part, jnp.broadcast_to(squares[:, None], (row_count, 128))], axis=1
    )
    slots = lax.dot_general(
        placed, side, (((0,), (0,)), ((), ())), preferred_element_type=F32
    ).astype(BF)
    slots = slots.reshape(n, slot_rows, latent_width + 128)
    pieces = jnp.stack(
        [
            jnp.concatenate(
                [slots[:, :, h * piece : (h + 1) * piece], slots[:, :, latent_width:]], axis=2
            )
            for h in range(heads)
        ]
    )
    incoming = through_slots(pieces, piece, features, 3)
    incoming = incoming.reshape(heads, n, experts_here, CAP, piece).transpose(2, 1, 3, 0, 4)
    incoming = incoming.reshape(experts_here, n * CAP, latent_width)
    hidden = jnp.einsum("esl,elf->esf", incoming, expert_up, preferred_element_type=F32)
    hidden = (jnp.maximum(hidden, 0.0) ** 2).astype(BF)
    expert_out = jnp.einsum("esf,efl->esl", hidden, expert_down, preferred_element_type=F32)
    expert_out = expert_out.astype(BF).reshape(experts_here, n, CAP, heads, piece)
    expert_out = expert_out.transpose(3, 1, 0, 2, 4).reshape(heads, n, slot_rows, piece)
    returned = through_slots(expert_out, piece, features, 4)
    returned = returned.transpose(1, 2, 0, 3).reshape(wave_size * CAP, latent_width)
    combined = jnp.dot(combine_table, returned, preferred_element_type=F32)
    moe_out = jnp.dot(combined.astype(BF), up_latent, preferred_element_type=F32)
    return (residual + moe_out).astype(BF)


def solution(mesh):
    placed = (
        P(("groups", "ctx"), "heads"),
        P(("groups", "ctx"), "heads"),
        P(("groups", "ctx"), None),
        P(("groups", "ctx"), None),
        P("heads"),
        P(("groups", "ctx"), "heads"),
        P("heads"),
        P("heads", "ctx"),
        P(("groups", "ctx"), "heads"),
        P("heads"),
        P("heads", None),
        P("ctx", None, "heads"),
        P("ctx", "heads", None),
        P(None, "heads"),
        P(("groups", "ctx"), None),
        P(("groups", "ctx"), None),
    )
    return jax.shard_map(
        local, mesh=mesh, in_specs=placed, out_specs=P(("groups", "ctx"), "heads"), check_vma=False
    )
```

```python
import functools

import jax
import jax.numpy as jnp
from jax import lax
from jax.experimental import pallas as pl
from jax.experimental.pallas import tpu as pltpu
from jax.sharding import PartitionSpec as P

D = 4096
GRP = 1024
LAT = 1024
CAP = 16
LENT_NUM, LENT_DEN = 3, 8


epsilon = 1e-05


MESH = pl.DeviceIdType.MESH
BF = jnp.bfloat16
F32 = jnp.float32


def vmem(count=1):
    return [pl.BlockSpec(memory_space=pltpu.VMEM)] * count


def greet(device):
    pl.semaphore_signal(
        pltpu.get_barrier_semaphore(), inc=1, device_id=device, device_id_type=MESH
    )


def greeted(count):
    pl.semaphore_wait(pltpu.get_barrier_semaphore(), count)


def one_if(condition):
    return jnp.where(condition, 1, 0)


def remote(src, dst, send, recv, device):
    return pltpu.make_async_remote_copy(
        src_ref=src, dst_ref=dst, send_sem=send, recv_sem=recv, device_id=device, device_id_type=MESH
    )


def pair_wide(first, second, width):
    lane = lax.broadcasted_iota(jnp.int32, (first.shape[0], 2 * width), 1)
    return jnp.where(lane < width, first, second)


def mixer_kernel(
    n, heads, groups, width, piece, lag, lent,
    x_hbm, write_hbm, read_hbm, decay_hbm, skip_hbm, weight_hbm, gate_hbm, gain_hbm, resid_hbm,
    out_ref,
    x_ref, write_ref, read_ref, decay_ref, skip_ref, weight_ref, gate_ref, gain_ref, resid_ref,
    cum, cum_rows, skips, inter,
    mixed, state, ends, prior, outgoing, gated,
    blocks, acc, parts, core_in, chip_out, x_in, fin_out, final, borrowed, strips,
    load_sem, chain_send, chain_recv, up_send, up_recv, down_send, down_recv,
    core_send, core_recv, x_send, x_recv, fin_send, fin_recv, lend_send, lend_recv, spread_send, spread_recv, strip_recv,
):
    me, head, group = lax.axis_index("ctx"), lax.axis_index("heads"), lax.axis_index("groups")
    rows, columns = x_ref.shape
    span = 2 * width
    pairs = columns // span
    head_count = decay_ref.shape[0]
    out_width = weight_ref.shape[1]
    count = columns // piece
    share = n // heads
    cores = 2
    chips = heads // cores
    core, chip = head % cores, head // cores
    half, strip = out_width // cores, rows // chips
    has_prev, has_next = me > 0, me < n - 1
    prev, after = jnp.maximum(me - 1, 0), jnp.minimum(me + 1, n - 1)
    keep = count - lent
    at_end = jnp.logical_or(me == 0, me == n - 1)
    beside = jnp.logical_or(me == 1, me == n - 2)
    end_here = jnp.where(me == 1, 0, n - 1)
    beside_here = jnp.where(me == 0, 1, n - 2)

    loads = [
        pltpu.make_async_copy(src, dst, load_sem.at[i])
        for i, (src, dst) in enumerate(
            [
                (x_hbm, x_ref), (write_hbm, write_ref), (read_hbm, read_ref), (decay_hbm, decay_ref),
                (skip_hbm, skip_ref), (weight_hbm, weight_ref), (gate_hbm, gate_ref),
                (gain_hbm, gain_ref), (resid_hbm, resid_ref),
            ]
        )
    ]
    for load in loads:
        load.start()
    for i in range(n):
        for j in range(heads):
            if i or j:
                greet({"ctx": (me + i) % n, "heads": (head + j) % heads})
    for i in range(1, groups):
        greet({"groups": (group + i) % groups})

    t = lax.broadcasted_iota(jnp.int32, (rows, rows), 0)
    s = lax.broadcasted_iota(jnp.int32, (rows, rows), 1)
    lower = jnp.where(t >= s, 1.0, 0.0)
    cum[...] = jnp.zeros(cum.shape, F32)
    for load in loads[:5]:
        load.wait()
    cum[:, :head_count] = lax.dot_general(
        lower, decay_ref[...], (((1,), (1,)), ((), ())),
        precision=lax.Precision.HIGHEST, preferred_element_type=F32,
    )
    cum_rows[...] = lax.dot_general(
        decay_ref[...], lower, (((1,), (1,)), ((), ())),
        precision=lax.Precision.HIGHEST, preferred_element_type=F32,
    )
    skips[...] = jnp.zeros(skips.shape, F32)
    skips[0:1, :head_count] = skip_ref[...]
    product = lax.dot_general(
        read_ref[...], write_ref[...], (((1,), (1,)), ((), ())), preferred_element_type=F32
    )
    inter[...] = jnp.where(t >= s, product, 0.0)
    greeted(n * heads + groups - 2)

    share_rows = piece // groups

    def lend(k):
        return remote(
            weight_ref.at[pl.ds((keep + k) * piece + group * share_rows, share_rows)],
            borrowed.at[pl.ds(k * piece + group * share_rows, share_rows)],
            lend_send.at[k], lend_recv.at[k], {"ctx": beside_here},
        )

    def spread(k, i, back=False):
        owner = (group + groups - i) % groups if back else group
        part = borrowed.at[pl.ds(k * piece + owner * share_rows, share_rows)]
        return remote(
            part, part, spread_send.at[k, i], spread_recv.at[k, i],
            {"groups": (group + i) % groups},
        )

    @pl.when(me == n - 1)
    def _():
        loads[5].wait()
        for k in range(lent):
            lend(k).start()

    def lanes(p):
        return pl.ds(pl.multiple_of(p * span, span), span)

    def shifted(ref, p):
        lane_count = ref.shape[1]
        return pltpu.roll(ref[...], (lane_count - 2 * p) % lane_count, 1)

    band = rows // 2
    causal = lax.broadcasted_iota(jnp.int32, (band, band), 0) >= lax.broadcasted_iota(
        jnp.int32, (band, band), 1
    )

    def scan(p):
        x = x_ref[:, lanes(p)]
        cols = shifted(cum, p)
        skip = shifted(skips, p)
        outs, tails, lasts = [], [], []
        for j in range(2):
            col = cols[:, j : j + 1]
            row = cum_rows[pl.ds(2 * p + j, 1), :]
            last = col[rows - 1 : rows, :]
            lane = x[:, j * width : (j + 1) * width]
            bands = []
            for lo in range(0, rows, band):
                hi = lo + band
                spread = jnp.where(causal, col[lo:hi] - row[:, lo:hi], 0.0)
                if lo:
                    spread = jnp.concatenate([col[lo:hi] - row[:, :lo], spread], axis=1)
                mixing = (jnp.exp(-spread) * inter[lo:hi, :hi]).astype(BF)
                bands.append(jnp.dot(mixing, lane[:hi], preferred_element_type=F32))
            outs.append(jnp.concatenate(bands, axis=0))
            tails.append(jnp.exp(col - last))
            lasts.append(jnp.exp(-last))
        wide = x.astype(F32)
        direct = pair_wide(skip[0:1, 0:1], skip[0:1, 1:2], width) * wide
        mixed[p] = jnp.concatenate(outs, axis=1) + direct
        scaled = (wide * pair_wide(tails[0], tails[1], width)).astype(BF)
        state[p] = lax.dot_general(
            write_ref[...], scaled, (((0,), (0,)), ((), ())), preferred_element_type=F32
        )
        ends[p] = pair_wide(lasts[0], lasts[1], width)

    def chain_copy(q):
        return remote(
            outgoing.at[q], prior.at[q], chain_send.at[q], chain_recv.at[q], {"ctx": after}
        )

    def chain(q):
        @pl.when(me == 0)
        def _():
            prior[q] = jnp.zeros(prior.shape[1:], BF)
            outgoing[q] = state[q].astype(BF)

        @pl.when(has_prev)
        def _():
            chain_copy(q).wait_recv()
            outgoing[q] = (prior[q].astype(F32) * ends[q] + state[q]).astype(BF)

        pl.when(has_next)(lambda: chain_copy(q).start())

    def advance(i, carry):
        pl.when(i < pairs)(lambda: scan(i))
        q = i - lag * me
        pl.when(jnp.logical_and(q >= 0, q < pairs))(lambda: chain(q))
        return carry

    lax.fori_loop(0, pairs + lag * (n - 1), advance, 0)

    def upward(b, p):
        spot = blocks.at[b, p]
        return remote(spot, spot, up_send.at[b, p], up_recv.at[b, p], {"ctx": after})

    def downward(b, p):
        spot = blocks.at[b, p]
        return remote(spot, spot, down_send.at[b, p], down_recv.at[b, p], {"ctx": prev})

    pl.when(me < n - 1)(lambda: loads[5].wait())

    def goes_up(p):
        return jnp.logical_and(has_next, jnp.logical_or(p < keep, me + 1 < n - 1))

    def goes_down(p):
        return jnp.logical_and(has_prev, jnp.logical_or(p < keep, me > 1))

    def needed(p):
        return jnp.logical_or(p < keep, jnp.logical_not(at_end))

    group_pairs = GRP // span
    group_pieces = GRP // piece
    piece_pairs = piece // span
    loads[6].wait()
    loads[7].wait()

    def gate(g, carry):
        squares = jnp.zeros((rows, span), F32)
        for i in range(group_pairs):
            p = g * group_pairs + i
            cols = shifted(cum, p)
            reach = jnp.exp(-pair_wide(cols[:, 0:1], cols[:, 1:2], width))
            carried = jnp.dot(read_ref[...], prior[p], preferred_element_type=F32) * reach
            gating = gate_ref[:, lanes(p)].astype(F32)
            value = (mixed[p] + carried) * (gating / (1.0 + jnp.exp(-gating)))
            gated[i] = value
            squares = squares + value * value
        scale = lax.rsqrt(jnp.sum(squares, axis=1, keepdims=True) / GRP + epsilon)
        for i in range(group_pairs):
            p = g * group_pairs + i
            value = (gated[i] * scale * gain_ref[:, lanes(p)]).astype(BF)
            lo = (i % piece_pairs) * span
            blocks[me, g * group_pieces + i // piece_pairs, :, lo : lo + span] = value
        for k in range(group_pieces):
            p = g * group_pieces + k
            pl.when(goes_up(p))(lambda: upward(me, p).start())
            pl.when(goes_down(p))(lambda: downward(me, p).start())
        return carry

    for k in range(lent):
        pl.when(me == 0)(lambda: lend(k).start())
    lax.fori_loop(0, columns // GRP, gate, 0)

    def multiply(slot, b, p):
        step = min(out_width, 256)
        fed = blocks[b, p]
        for lo in range(0, out_width, step):
            held = acc[slot, :, lo : lo + step]
            part = weight_ref[pl.ds(pl.multiple_of(p * piece, piece), piece), lo : lo + step]
            acc[slot, :, lo : lo + step] = jnp.where(p == 0, 0.0, held) + jnp.dot(
                fed, part, preferred_element_type=F32
            )

    def core_copy(b, kind):
        return remote(
            parts.at[kind, b, 1 - core], core_in.at[kind, b], core_send.at[kind, b],
            core_recv.at[kind, b], {"heads": head + 1 - 2 * core},
        )

    def round_partial(b, slot, kind=0):
        for k in range(cores):
            parts[kind, b, k] = acc[slot, :, k * half : (k + 1) * half].astype(BF)
        core_copy(b, kind).start()

    def chip_copy(b, k, kind):
        to = (chip + k) % chips
        return remote(
            chip_out.at[kind, b, to], x_in.at[kind, b, k], x_send.at[kind, b, k],
            x_recv.at[kind, b, k], {"heads": to * cores + core},
        )

    def sum_cores(b, kind=0):
        core_copy(b, kind).wait_recv()
        for k in range(chips):
            part = slice(k * strip, (k + 1) * strip)
            both = parts[kind, b, core, part].astype(F32) + core_in[kind, b, part].astype(F32)
            chip_out[kind, b, k] = both.astype(BF)
        for k in range(1, chips):
            chip_copy(b, k, kind).start()

    def local_final(b, column):
        return jnp.logical_and(b == me, head == column // share)

    def final_copy(b, column, kind):
        return remote(
            fin_out.at[kind, b], final.at[column % share, head], fin_send.at[kind, b],
            fin_recv.at[column % share, head], {"ctx": b, "heads": column // share},
        )

    def strip_copy(b):
        return remote(
            fin_out.at[0, b], strips.at[b], fin_send.at[0, b], strip_recv.at[b],
            {"ctx": beside_here},
        )

    def to_beside(b):
        if not lent:
            return False
        return jnp.logical_and(at_end, b != me)

    def strip_total(b, kind):
        part = pl.ds(pl.multiple_of(chip * strip, strip), strip)
        total = parts[kind, b, core, part].astype(F32) + core_in[kind, b, part].astype(F32)
        for k in range(1, chips):
            chip_copy(b, k, kind).wait_recv()
            total = total + x_in[kind, b, k].astype(F32)
        return total

    def deliver(b, column, kind, total):
        @pl.when(local_final(b, column))
        def _():
            final[column % share, head] = total.astype(BF)

        pl.when(jnp.logical_not(local_final(b, column)))(
            lambda: final_copy(b, column, kind).start()
        )

    def sum_chips(b):
        total = strip_total(b, 0)
        fin_out[0, b] = total.astype(BF)
        if lent:
            pl.when(to_beside(b))(lambda: strip_copy(b).start())
            pl.when(jnp.logical_not(to_beside(b)))(lambda: deliver(b, me, 0, total))
        else:
            deliver(b, me, 0, total)

    def helps(b):
        return jnp.logical_and(beside, b != end_here)

    def helping(b):
        @pl.when(helps(b))
        def _():
            step = min(out_width, 256)
            for lo in range(0, out_width, step):
                total = jnp.zeros((rows, step), F32)
                for k in range(lent):
                    part = borrowed[k * piece : (k + 1) * piece, lo : lo + step]
                    total = total + jnp.dot(
                        blocks[b, keep + k], part, preferred_element_type=F32
                    )
                acc[2, :, lo : lo + step] = total
            round_partial(b, 2, 1)

    def combine(b):
        @pl.when(helps(b))
        def _():
            strip_copy(b).wait_recv()
            total = strip_total(b, 1) + strips[b].astype(F32)
            fin_out[1, b] = total.astype(BF)
            deliver(b, end_here, 1, total)

    def own(p, carry):
        multiply(0, me, p)
        return carry

    lax.fori_loop(0, count, own, 0)
    round_partial(me, 0)

    def around(s, act):
        low, high = me - s, me + s
        pl.when(low >= 0)(lambda: act(jnp.maximum(low, 0), 0))

        @pl.when(jnp.logical_and(high < n, s > 0))
        def _():
            act(jnp.minimum(high, n - 1), 1)

    def both_sides(s, act):
        around(s, lambda b, slot: act(b))

    def step(i, carry):
        s, p = 1 + i // count, i % count
        low, high = me - s, me + s
        low_spot, high_spot = jnp.maximum(low, 0), jnp.minimum(high, n - 1)
        wanted = needed(p)

        @pl.when(jnp.logical_and(low >= 0, wanted))
        def _():
            upward(low_spot, p).wait_recv()
            pl.when(goes_up(p))(lambda: upward(low_spot, p).start())

        @pl.when(jnp.logical_and(high < n, wanted))
        def _():
            downward(high_spot, p).wait_recv()
            pl.when(goes_down(p))(lambda: downward(high_spot, p).start())

        pl.when(wanted)(lambda: around(s, lambda b, slot: multiply(slot, b, p)))
        last = jnp.where(at_end, keep - 1, count - 1)
        pl.when(p == last)(lambda: around(s, round_partial))

        def at(spot, act):
            pl.when(p == min(spot, count - 1))(lambda: both_sides(s - 1, act))

        at(1, sum_cores)
        at(4, sum_chips)
        def reduce_help(b):
            pl.when(helps(b))(lambda: sum_cores(b, 1))

        if lent:
            @pl.when(jnp.logical_and(i == 1, beside))
            def _():
                for k in range(lent):
                    for g in range(1, groups):
                        spread(k, g, True).wait_recv()

            at(2, helping)
            at(4, reduce_help)
            pl.when(jnp.logical_and(p == min(7, count - 1), s > 1))(
                lambda: both_sides(s - 2, combine)
            )
        return carry

    for k in range(lent):
        @pl.when(beside)
        def _():
            lend(k).wait_recv()
            for g in range(1, groups):
                spread(k, g).start()

    lax.fori_loop(0, (n - 1) * count, step, 0)
    both_sides(n - 1, sum_cores)
    both_sides(n - 1, sum_chips)
    if lent:
        both_sides(n - 2, combine)
    loads[8].wait()

    for j in range(share):
        source = head * share + j
        if lent:
            outer = jnp.logical_and(source != me, jnp.logical_or(source == 0, source == n - 1))
            source = jnp.where(outer, jnp.where(source == 0, 1, n - 2), source)
        for k in range(heads):
            here = jnp.logical_and(source == me, k == head)

            @pl.when(jnp.logical_not(here))
            def _():
                remote(
                    fin_out.at[0, 0], final.at[j, k], fin_send.at[0, 0], fin_recv.at[j, k],
                    {"ctx": source, "heads": k},
                ).wait_recv()

            part = slice((k // cores) * strip, (k // cores + 1) * strip)
            lo = j * out_width + (k % cores) * half
            out_ref[part, lo : lo + half] = (
                resid_ref[part, lo : lo + half].astype(F32) + final[j, k].astype(F32)
            )

    for q in range(pairs):
        pl.when(has_next)(lambda: chain_copy(q).wait_send())
    for b in range(n):
        for p in range(count):
            pl.when(jnp.logical_and(goes_up(p), b <= me))(lambda: upward(b, p).wait_send())
            pl.when(jnp.logical_and(goes_down(p), b >= me))(lambda: downward(b, p).wait_send())
        core_copy(b, 0).wait_send()
        for k in range(1, chips):
            chip_copy(b, k, 0).wait_send()
        sent = jnp.logical_or(to_beside(b), jnp.logical_not(local_final(b, me)))
        pl.when(sent)(lambda: final_copy(b, me, 0).wait_send())

        if lent:
            @pl.when(helps(b))
            def _():
                core_copy(b, 1).wait_send()
                for k in range(1, chips):
                    chip_copy(b, k, 1).wait_send()
                pl.when(jnp.logical_not(local_final(b, end_here)))(
                    lambda: final_copy(b, end_here, 1).wait_send()
                )

    for k in range(lent):
        pl.when(at_end)(lambda: lend(k).wait_send())
        for g in range(1, groups):
            pl.when(beside)(lambda: spread(k, g).wait_send())


def slots_kernel(
    n, heads, width, features, src_ref, out_ref,
    first, middle, second, third,
    first_send, first_recv, second_send, second_recv, third_send, third_recv,
):
    me, head = lax.axis_index("ctx"), lax.axis_index("heads")

    for k in range(1, heads):
        greet({"heads": (head + k) % heads})
    for k in range(1, n):
        greet({"ctx": (me + k) % n})
    greeted(heads + n - 2)

    def first_copy(k):
        to = (head + k) % heads
        return remote(
            src_ref.at[to], first.at[k], first_send.at[k], first_recv.at[k], {"heads": to}
        )

    def second_copy(k):
        to = (me + k) % n
        return remote(
            middle.at[to], second.at[me], second_send.at[k], second_recv.at[k], {"ctx": to}
        )

    def third_copy(k):
        to = (head + k) % heads
        return remote(second, third.at[k], third_send.at[k], third_recv.at[k], {"heads": to})

    for k in range(1, heads):
        first_copy(k).start()
    total = src_ref[head].astype(F32)
    for k in range(1, heads):
        first_copy(k).wait_recv()
        total = total + first[k].astype(F32)
    if src_ref.shape[-1] > width:
        power = total[:, :, width : width + 1]
        total = total[:, :, :width] * lax.rsqrt(power / features + epsilon)
    middle[...] = total.astype(BF)
    for k in range(1, n):
        second_copy(k).start()
    second[me] = middle[me]
    for k in range(1, n):
        second_copy(k).wait_recv()
    for k in range(1, heads):
        third_copy(k).start()
    out_ref[head] = second[...]
    for k in range(1, heads):
        third_copy(k).wait_recv()
        out_ref[(head + heads - k) % heads] = third[k]
    for k in range(1, heads):
        first_copy(k).wait_send()
        third_copy(k).wait_send()
    for k in range(1, n):
        second_copy(k).wait_send()


def reaching(collective_id, grant=48 * 1024 * 1024):
    return pltpu.CompilerParams(
        collective_id=collective_id, has_side_effects=True, vmem_limit_bytes=grant
    )


def dma(*shape):
    return pltpu.SemaphoreType.DMA(shape)


def through_slots(pieces, width, features, collective_id):
    heads, n, rows, wide = pieces.shape
    return pl.pallas_call(
        functools.partial(slots_kernel, n, heads, width, features),
        out_shape=jax.ShapeDtypeStruct((heads, n, rows, width), BF),
        in_specs=vmem(),
        out_specs=vmem()[0],
        scratch_shapes=[
            pltpu.VMEM((heads, n, rows, wide), BF),
            pltpu.VMEM((n, rows, width), BF),
            pltpu.VMEM((n, rows, width), BF),
            pltpu.VMEM((heads, n, rows, width), BF),
            dma(heads), dma(heads), dma(n), dma(n), dma(heads), dma(heads),
        ],
        compiler_params=reaching(collective_id),
    )(pieces)


def mixer(
    ssm_input, decay_log, state_write, state_read, skip_scale, gate_input, ssm_gain, weight, residual_in
):
    n, heads, groups = lax.axis_size("ctx"), lax.axis_size("heads"), lax.axis_size("groups")
    rows, columns = ssm_input.shape
    head_count = decay_log.shape[1]
    width = columns // head_count
    states = state_write.shape[1]
    span = 2 * width
    pairs = columns // span
    piece = GRP // 4
    count = columns // piece
    lent = LENT_NUM * count // LENT_DEN if n > 3 else 0
    out_width = weight.shape[1]
    share = n // heads
    chips = heads // 2
    half, strip = out_width // 2, rows // chips
    lane_count = -(-head_count // 128) * 128
    block = (rows, out_width)
    anywhere = pl.BlockSpec(memory_space=pltpu.HBM)
    return pl.pallas_call(
        functools.partial(mixer_kernel, n, heads, groups, width, piece, 3, lent),
        out_shape=jax.ShapeDtypeStruct((rows, share * out_width), F32),
        in_specs=[anywhere] * 9,
        out_specs=vmem()[0],
        scratch_shapes=[
            pltpu.VMEM((rows, columns), BF),
            pltpu.VMEM((rows, states), BF),
            pltpu.VMEM((rows, states), BF),
            pltpu.VMEM((head_count, rows), F32),
            pltpu.VMEM((1, head_count), F32),
            pltpu.VMEM(weight.shape, BF),
            pltpu.VMEM((rows, columns), BF),
            pltpu.VMEM((1, columns), F32),
            pltpu.VMEM(residual_in.shape, BF),
            pltpu.VMEM((rows, lane_count), F32),
            pltpu.VMEM((head_count, rows), F32),
            pltpu.VMEM((8, lane_count), F32),
            pltpu.VMEM((rows, rows), F32),
            pltpu.VMEM((pairs, rows, span), F32),
            pltpu.VMEM((pairs, states, span), F32),
            pltpu.VMEM((pairs, 1, span), F32),
            pltpu.VMEM((pairs, states, span), BF),
            pltpu.VMEM((pairs, states, span), BF),
            pltpu.VMEM((GRP // span, rows, span), F32),
            pltpu.VMEM((n, count, rows, piece), BF),
            pltpu.VMEM((3,) + block, F32),
            pltpu.VMEM((2, n, 2, rows, half), BF),
            pltpu.VMEM((2, n, rows, half), BF),
            pltpu.VMEM((2, n, chips, strip, half), BF),
            pltpu.VMEM((2, n, chips, strip, half), BF),
            pltpu.VMEM((2, n, strip, half), BF),
            pltpu.VMEM((share, heads, strip, half), BF),
            pltpu.VMEM((max(lent, 1) * piece, out_width), BF),
            pltpu.VMEM((n, strip, half), BF),
            dma(9), dma(pairs), dma(pairs),
            dma(n, count), dma(n, count), dma(n, count), dma(n, count),
            dma(2, n), dma(2, n), dma(2, n, chips), dma(2, n, chips), dma(2, n), dma(share, heads),
            dma(max(lent, 1)), dma(max(lent, 1)), dma(max(lent, 1), groups), dma(max(lent, 1), groups), dma(n),
        ],
        compiler_params=reaching(1, 67043328),
    )(
        ssm_input, state_write, state_read, decay_log.T, skip_scale.reshape(1, head_count), weight,
        gate_input, ssm_gain.reshape(1, columns), residual_in,
    )


def local(
    ssm_input,
    decay_log,
    state_write,
    state_read,
    skip_scale,
    gate_input,
    ssm_gain,
    out_weight,
    residual_in,
    moe_gain,
    down_latent,
    expert_up,
    expert_down,
    up_latent,
    expert_ids,
    combine_fixed,
):
    row_count = ssm_input.shape[0]
    n, heads = lax.axis_size("ctx"), lax.axis_size("heads")
    features = residual_in.shape[1] * heads
    latent_width = down_latent.shape[1]
    piece = latent_width // heads
    experts_here = expert_up.shape[0]
    wave_size = experts_here * n
    slot_rows = experts_here * CAP

    matches = expert_ids[:, :, None] == jnp.arange(wave_size)[None, None, :]
    chosen = jnp.any(matches, axis=1).astype(jnp.int32)
    weight_fixed = jnp.sum(jnp.where(matches, combine_fixed[:, :, None], 0), axis=1)
    slot_index = jnp.cumsum(chosen, axis=0) - 1
    placed = (chosen[:, :, None] == 1) & (slot_index[:, :, None] == jnp.arange(CAP)[None, None, :])
    route_weight = (weight_fixed.astype(F32) / 65536.0).astype(BF)
    combine_table = jnp.where(placed, route_weight[:, :, None], jnp.zeros((), BF)).reshape(
        row_count, wave_size * CAP
    )
    placed = placed.astype(BF).reshape(row_count, wave_size * CAP)

    residual = mixer(
        ssm_input, decay_log, state_write, state_read, skip_scale, gate_input, ssm_gain,
        out_weight, residual_in,
    )
    scaled = (residual * moe_gain).astype(BF)
    latent_part = jnp.dot(scaled, down_latent, preferred_element_type=F32).astype(BF)
    squares = jnp.sum(residual * residual, axis=1).astype(BF)
    side = jnp.concatenate(
        [latent_part, jnp.broadcast_to(squares[:, None], (row_count, 128))], axis=1
    )
    slots = lax.dot_general(
        placed, side, (((0,), (0,)), ((), ())), preferred_element_type=F32
    ).astype(BF)
    slots = slots.reshape(n, slot_rows, latent_width + 128)
    pieces = jnp.stack(
        [
            jnp.concatenate(
                [slots[:, :, h * piece : (h + 1) * piece], slots[:, :, latent_width:]], axis=2
            )
            for h in range(heads)
        ]
    )
    incoming = through_slots(pieces, piece, features, 3)
    incoming = incoming.reshape(heads, n, experts_here, CAP, piece).transpose(2, 1, 3, 0, 4)
    incoming = incoming.reshape(experts_here, n * CAP, latent_width)
    hidden = jnp.einsum("esl,elf->esf", incoming, expert_up, preferred_element_type=F32)
    hidden = (jnp.maximum(hidden, 0.0) ** 2).astype(BF)
    expert_out = jnp.einsum("esf,efl->esl", hidden, expert_down, preferred_element_type=F32)
    expert_out = expert_out.astype(BF).reshape(experts_here, n, CAP, heads, piece)
    expert_out = expert_out.transpose(3, 1, 0, 2, 4).reshape(heads, n, slot_rows, piece)
    returned = through_slots(expert_out, piece, features, 4)
    returned = returned.transpose(1, 2, 0, 3).reshape(wave_size * CAP, latent_width)
    combined = jnp.dot(combine_table, returned, preferred_element_type=F32)
    moe_out = jnp.dot(combined.astype(BF), up_latent, preferred_element_type=F32)
    return (residual + moe_out).astype(BF)


def solution(mesh):
    placed = (
        P(("groups", "ctx"), "heads"),
        P(("groups", "ctx"), "heads"),
        P(("groups", "ctx"), None),
        P(("groups", "ctx"), None),
        P("heads"),
        P(("groups", "ctx"), "heads"),
        P("heads"),
        P("heads", "ctx"),
        P(("groups", "ctx"), "heads"),
        P("heads"),
        P("heads", None),
        P("ctx", None, "heads"),
        P("ctx", "heads", None),
        P(None, "heads"),
        P(("groups", "ctx"), None),
        P(("groups", "ctx"), None),
    )
    return jax.shard_map(
        local, mesh=mesh, in_specs=placed, out_specs=P(("groups", "ctx"), "heads"), check_vma=False
    )
```

```python
import functools

import jax
import jax.numpy as jnp
from jax import lax
from jax.experimental import pallas as pl
from jax.experimental.pallas import tpu as pltpu
from jax.sharding import PartitionSpec as P

GRP = 1024
CAP = 16
LENT_NUM, LENT_DEN = 3, 8


epsilon = 1e-05


MESH = pl.DeviceIdType.MESH
BF = jnp.bfloat16
F32 = jnp.float32


def vmem(count=1):
    return [pl.BlockSpec(memory_space=pltpu.VMEM)] * count


def greet(device):
    pl.semaphore_signal(
        pltpu.get_barrier_semaphore(), inc=1, device_id=device, device_id_type=MESH
    )


def greeted(count):
    pl.semaphore_wait(pltpu.get_barrier_semaphore(), count)


def remote(src, dst, send, recv, device):
    return pltpu.make_async_remote_copy(
        src_ref=src, dst_ref=dst, send_sem=send, recv_sem=recv, device_id=device, device_id_type=MESH
    )


def pair_wide(first, second, width):
    lane = lax.broadcasted_iota(jnp.int32, (first.shape[0], 2 * width), 1)
    return jnp.where(lane < width, first, second)


def layer_kernel(
    n, heads, groups, width, piece, lag, lent,
    x_hbm, write_hbm, read_hbm, decay_hbm, skip_hbm, weight_hbm, gate_hbm, gain_hbm, resid_hbm,
    ids_hbm, fixed_hbm, moe_hbm, latent_hbm, grow_hbm, shrink_hbm, lift_hbm,
    out_ref,
    x_ref, write_ref, read_ref, decay_ref, skip_ref, weight_ref, gate_ref, gain_ref, resid_ref,
    ids_ref, fixed_ref, moe_ref, latent_ref, grow_ref, shrink_ref, lift_ref,
    cum, cum_rows, skips, inter,
    mixed, state, ends, prior, outgoing, gated,
    blocks, acc, parts, core_in, chip_out, x_in, fin_out, final, borrowed, strips,
    residual, chosen, weights, placed, table, square_out, square_in,
    slots_out, slots_in, middle, gathered, back_out, back_in, back_middle, returned,
    load_sem, chain_send, chain_recv, up_send, up_recv, down_send, down_recv,
    core_send, core_recv, x_send, x_recv, fin_send, fin_recv, lend_send, lend_recv, spread_send, spread_recv, strip_recv,
    square_send, square_recv, first_send, first_recv, second_send, second_recv,
    third_send, third_recv, fourth_send, fourth_recv, fifth_send, fifth_recv, sixth_send, sixth_recv,
):
    me, head, group = lax.axis_index("ctx"), lax.axis_index("heads"), lax.axis_index("groups")
    rows, columns = x_ref.shape
    span = 2 * width
    pairs = columns // span
    head_count = decay_ref.shape[0]
    out_width = weight_ref.shape[1]
    count = columns // piece
    share = n // heads
    cores = 2
    chips = heads // cores
    core, chip = head % cores, head // cores
    half, strip = out_width // cores, rows // chips
    has_prev, has_next = me > 0, me < n - 1
    prev, after = jnp.maximum(me - 1, 0), jnp.minimum(me + 1, n - 1)
    keep = count - lent
    at_end = jnp.logical_or(me == 0, me == n - 1)
    beside = jnp.logical_or(me == 1, me == n - 2)
    end_here = jnp.where(me == 1, 0, n - 1)
    beside_here = jnp.where(me == 0, 1, n - 2)

    loads = [
        pltpu.make_async_copy(src, dst, load_sem.at[i])
        for i, (src, dst) in enumerate(
            [
                (x_hbm, x_ref), (write_hbm, write_ref), (read_hbm, read_ref), (decay_hbm, decay_ref),
                (skip_hbm, skip_ref), (weight_hbm, weight_ref), (gate_hbm, gate_ref),
                (gain_hbm, gain_ref), (resid_hbm, resid_ref),
                (ids_hbm, ids_ref), (fixed_hbm, fixed_ref), (moe_hbm, moe_ref),
                (latent_hbm, latent_ref), (grow_hbm, grow_ref), (shrink_hbm, shrink_ref),
                (lift_hbm, lift_ref),
            ]
        )
    ]
    for load in loads[:8]:
        load.start()
    for i in range(n):
        for j in range(heads):
            if i or j:
                greet({"ctx": (me + i) % n, "heads": (head + j) % heads})
    for i in range(1, groups):
        greet({"groups": (group + i) % groups})

    t = lax.broadcasted_iota(jnp.int32, (rows, rows), 0)
    s = lax.broadcasted_iota(jnp.int32, (rows, rows), 1)
    lower = jnp.where(t >= s, 1.0, 0.0)
    cum[...] = jnp.zeros(cum.shape, F32)
    for load in loads[:5]:
        load.wait()
    cum[:, :head_count] = lax.dot_general(
        lower, decay_ref[...], (((1,), (1,)), ((), ())),
        precision=lax.Precision.HIGHEST, preferred_element_type=F32,
    )
    cum_rows[...] = lax.dot_general(
        decay_ref[...], lower, (((1,), (1,)), ((), ())),
        precision=lax.Precision.HIGHEST, preferred_element_type=F32,
    )
    skips[...] = jnp.zeros(skips.shape, F32)
    skips[0:1, :head_count] = skip_ref[...]
    product = lax.dot_general(
        read_ref[...], write_ref[...], (((1,), (1,)), ((), ())), preferred_element_type=F32
    )
    inter[...] = jnp.where(t >= s, product, 0.0)
    greeted(n * heads + groups - 2)

    for load in loads[8:]:
        load.start()
    share_rows = piece // groups

    def lend(k):
        return remote(
            weight_ref.at[pl.ds((keep + k) * piece + group * share_rows, share_rows)],
            borrowed.at[pl.ds(k * piece + group * share_rows, share_rows)],
            lend_send.at[k], lend_recv.at[k], {"ctx": beside_here},
        )

    def spread(k, i, back=False):
        owner = (group + groups - i) % groups if back else group
        part = borrowed.at[pl.ds(k * piece + owner * share_rows, share_rows)]
        return remote(
            part, part, spread_send.at[k, i], spread_recv.at[k, i],
            {"groups": (group + i) % groups},
        )

    @pl.when(me == n - 1)
    def _():
        loads[5].wait()
        for k in range(lent):
            lend(k).start()

    def lanes(p):
        return pl.ds(pl.multiple_of(p * span, span), span)

    def shifted(ref, p):
        lane_count = ref.shape[1]
        return pltpu.roll(ref[...], (lane_count - 2 * p) % lane_count, 1)

    band = rows // 2
    causal = lax.broadcasted_iota(jnp.int32, (band, band), 0) >= lax.broadcasted_iota(
        jnp.int32, (band, band), 1
    )

    def scan(p):
        x = x_ref[:, lanes(p)]
        cols = shifted(cum, p)
        skip = shifted(skips, p)
        outs, tails, lasts = [], [], []
        for j in range(2):
            col = cols[:, j : j + 1]
            row = cum_rows[pl.ds(2 * p + j, 1), :]
            last = col[rows - 1 : rows, :]
            lane = x[:, j * width : (j + 1) * width]
            bands = []
            for lo in range(0, rows, band):
                hi = lo + band
                spread = jnp.where(causal, col[lo:hi] - row[:, lo:hi], 0.0)
                if lo:
                    spread = jnp.concatenate([col[lo:hi] - row[:, :lo], spread], axis=1)
                mixing = (jnp.exp(-spread) * inter[lo:hi, :hi]).astype(BF)
                bands.append(jnp.dot(mixing, lane[:hi], preferred_element_type=F32))
            outs.append(jnp.concatenate(bands, axis=0))
            tails.append(jnp.exp(col - last))
            lasts.append(jnp.exp(-last))
        wide = x.astype(F32)
        direct = pair_wide(skip[0:1, 0:1], skip[0:1, 1:2], width) * wide
        mixed[p] = jnp.concatenate(outs, axis=1) + direct
        scaled = (wide * pair_wide(tails[0], tails[1], width)).astype(BF)
        state[p] = lax.dot_general(
            write_ref[...], scaled, (((0,), (0,)), ((), ())), preferred_element_type=F32
        )
        ends[p] = pair_wide(lasts[0], lasts[1], width)

    def chain_copy(q):
        return remote(
            outgoing.at[q], prior.at[q], chain_send.at[q], chain_recv.at[q], {"ctx": after}
        )

    def chain(q):
        @pl.when(me == 0)
        def _():
            prior[q] = jnp.zeros(prior.shape[1:], BF)
            outgoing[q] = state[q].astype(BF)

        @pl.when(has_prev)
        def _():
            chain_copy(q).wait_recv()
            outgoing[q] = (prior[q].astype(F32) * ends[q] + state[q]).astype(BF)

        pl.when(has_next)(lambda: chain_copy(q).start())

    def advance(i, carry):
        pl.when(i < pairs)(lambda: scan(i))
        q = i - lag * me
        pl.when(jnp.logical_and(q >= 0, q < pairs))(lambda: chain(q))
        return carry

    lax.fori_loop(0, pairs + lag * (n - 1), advance, 0)

    def upward(b, p):
        spot = blocks.at[b, p]
        return remote(spot, spot, up_send.at[b, p], up_recv.at[b, p], {"ctx": after})

    def downward(b, p):
        spot = blocks.at[b, p]
        return remote(spot, spot, down_send.at[b, p], down_recv.at[b, p], {"ctx": prev})

    pl.when(me < n - 1)(lambda: loads[5].wait())

    def goes_up(p):
        return jnp.logical_and(has_next, jnp.logical_or(p < keep, me + 1 < n - 1))

    def goes_down(p):
        return jnp.logical_and(has_prev, jnp.logical_or(p < keep, me > 1))

    def needed(p):
        return jnp.logical_or(p < keep, jnp.logical_not(at_end))

    group_pairs = GRP // span
    group_pieces = GRP // piece
    piece_pairs = piece // span
    loads[6].wait()
    loads[7].wait()

    def gate(g, carry):
        squares = jnp.zeros((rows, span), F32)
        for i in range(group_pairs):
            p = g * group_pairs + i
            cols = shifted(cum, p)
            reach = jnp.exp(-pair_wide(cols[:, 0:1], cols[:, 1:2], width))
            carried = jnp.dot(read_ref[...], prior[p], preferred_element_type=F32) * reach
            gating = gate_ref[:, lanes(p)].astype(F32)
            value = (mixed[p] + carried) * (gating / (1.0 + jnp.exp(-gating)))
            gated[i] = value
            squares = squares + value * value
        scale = lax.rsqrt(jnp.sum(squares, axis=1, keepdims=True) / GRP + epsilon)
        for i in range(group_pairs):
            p = g * group_pairs + i
            value = (gated[i] * scale * gain_ref[:, lanes(p)]).astype(BF)
            lo = (i % piece_pairs) * span
            blocks[me, g * group_pieces + i // piece_pairs, :, lo : lo + span] = value
        for k in range(group_pieces):
            p = g * group_pieces + k
            pl.when(goes_up(p))(lambda: upward(me, p).start())
            pl.when(goes_down(p))(lambda: downward(me, p).start())
        return carry

    for k in range(lent):
        pl.when(me == 0)(lambda: lend(k).start())
    lax.fori_loop(0, columns // GRP, gate, 0)

    def multiply(slot, b, p):
        step = min(out_width, 256)
        fed = blocks[b, p]
        for lo in range(0, out_width, step):
            held = acc[slot, :, lo : lo + step]
            part = weight_ref[pl.ds(pl.multiple_of(p * piece, piece), piece), lo : lo + step]
            acc[slot, :, lo : lo + step] = jnp.where(p == 0, 0.0, held) + jnp.dot(
                fed, part, preferred_element_type=F32
            )

    def core_copy(b, kind):
        return remote(
            parts.at[kind, b, 1 - core], core_in.at[kind, b], core_send.at[kind, b],
            core_recv.at[kind, b], {"heads": head + 1 - 2 * core},
        )

    def round_partial(b, slot, kind=0):
        for k in range(cores):
            parts[kind, b, k] = acc[slot, :, k * half : (k + 1) * half].astype(BF)
        core_copy(b, kind).start()

    def chip_copy(b, k, kind):
        to = (chip + k) % chips
        return remote(
            chip_out.at[kind, b, to], x_in.at[kind, b, k], x_send.at[kind, b, k],
            x_recv.at[kind, b, k], {"heads": to * cores + core},
        )

    def sum_cores(b, kind=0):
        core_copy(b, kind).wait_recv()
        for k in range(chips):
            part = slice(k * strip, (k + 1) * strip)
            both = parts[kind, b, core, part].astype(F32) + core_in[kind, b, part].astype(F32)
            chip_out[kind, b, k] = both.astype(BF)
        for k in range(1, chips):
            chip_copy(b, k, kind).start()

    def local_final(b, column):
        return jnp.logical_and(b == me, head == column // share)

    def final_copy(b, column, kind):
        return remote(
            fin_out.at[kind, b], final.at[column % share, head], fin_send.at[kind, b],
            fin_recv.at[column % share, head], {"ctx": b, "heads": column // share},
        )

    def strip_copy(b):
        return remote(
            fin_out.at[0, b], strips.at[b], fin_send.at[0, b], strip_recv.at[b],
            {"ctx": beside_here},
        )

    def to_beside(b):
        if not lent:
            return False
        return jnp.logical_and(at_end, b != me)

    def strip_total(b, kind):
        part = pl.ds(pl.multiple_of(chip * strip, strip), strip)
        total = parts[kind, b, core, part].astype(F32) + core_in[kind, b, part].astype(F32)
        for k in range(1, chips):
            chip_copy(b, k, kind).wait_recv()
            total = total + x_in[kind, b, k].astype(F32)
        return total

    def deliver(b, column, kind, total):
        @pl.when(local_final(b, column))
        def _():
            final[column % share, head] = total.astype(BF)

        pl.when(jnp.logical_not(local_final(b, column)))(
            lambda: final_copy(b, column, kind).start()
        )

    def sum_chips(b):
        total = strip_total(b, 0)
        fin_out[0, b] = total.astype(BF)
        if lent:
            pl.when(to_beside(b))(lambda: strip_copy(b).start())
            pl.when(jnp.logical_not(to_beside(b)))(lambda: deliver(b, me, 0, total))
        else:
            deliver(b, me, 0, total)

    def helps(b):
        return jnp.logical_and(beside, b != end_here)

    def helping(b):
        @pl.when(helps(b))
        def _():
            step = min(out_width, 256)
            for lo in range(0, out_width, step):
                total = jnp.zeros((rows, step), F32)
                for k in range(lent):
                    part = borrowed[k * piece : (k + 1) * piece, lo : lo + step]
                    total = total + jnp.dot(
                        blocks[b, keep + k], part, preferred_element_type=F32
                    )
                acc[2, :, lo : lo + step] = total
            round_partial(b, 2, 1)

    def combine(b):
        @pl.when(helps(b))
        def _():
            strip_copy(b).wait_recv()
            total = strip_total(b, 1) + strips[b].astype(F32)
            fin_out[1, b] = total.astype(BF)
            deliver(b, end_here, 1, total)

    def own(p, carry):
        multiply(0, me, p)
        return carry

    lax.fori_loop(0, count, own, 0)
    round_partial(me, 0)

    loads[9].wait()
    loads[10].wait()
    wave = chosen.shape[0]
    for e in range(wave):
        named = ids_ref[...] == e
        chosen[e : e + 1, :] = jnp.sum(jnp.where(named, 1.0, 0.0), axis=0, keepdims=True)
        weights[e : e + 1, :] = jnp.sum(jnp.where(named, fixed_ref[...], 0), axis=0, keepdims=True)
    upto = jnp.where(t <= s, 1.0, 0.0).astype(BF)
    taken = jnp.dot(chosen[...].astype(BF), upto, preferred_element_type=F32)
    slot = lax.broadcasted_iota(jnp.int32, (CAP, rows), 0).astype(F32) + 1.0
    for e in range(wave):
        here = jnp.logical_and(chosen[e : e + 1, :] > 0.5, taken[e : e + 1, :] == slot)
        weight = weights[e : e + 1, :].astype(F32) / 65536.0
        part = slice(e * CAP, (e + 1) * CAP)
        placed[part] = jnp.where(here, 1.0, 0.0).astype(BF)
        table[part] = jnp.where(here, weight, 0.0).astype(BF)

    def around(s, act):
        low, high = me - s, me + s
        pl.when(low >= 0)(lambda: act(jnp.maximum(low, 0), 0))

        @pl.when(jnp.logical_and(high < n, s > 0))
        def _():
            act(jnp.minimum(high, n - 1), 1)

    def both_sides(s, act):
        around(s, lambda b, slot: act(b))

    def step(i, carry):
        s, p = 1 + i // count, i % count
        low, high = me - s, me + s
        low_spot, high_spot = jnp.maximum(low, 0), jnp.minimum(high, n - 1)
        wanted = needed(p)

        @pl.when(jnp.logical_and(low >= 0, wanted))
        def _():
            upward(low_spot, p).wait_recv()
            pl.when(goes_up(p))(lambda: upward(low_spot, p).start())

        @pl.when(jnp.logical_and(high < n, wanted))
        def _():
            downward(high_spot, p).wait_recv()
            pl.when(goes_down(p))(lambda: downward(high_spot, p).start())

        pl.when(wanted)(lambda: around(s, lambda b, slot: multiply(slot, b, p)))
        last = jnp.where(at_end, keep - 1, count - 1)
        pl.when(p == last)(lambda: around(s, round_partial))

        def at(spot, act):
            pl.when(p == min(spot, count - 1))(lambda: both_sides(s - 1, act))

        at(1, sum_cores)
        at(4, sum_chips)
        def reduce_help(b):
            pl.when(helps(b))(lambda: sum_cores(b, 1))

        if lent:
            @pl.when(jnp.logical_and(i == 1, beside))
            def _():
                for k in range(lent):
                    for g in range(1, groups):
                        spread(k, g, True).wait_recv()

            at(2, helping)
            at(4, reduce_help)
            pl.when(jnp.logical_and(p == min(7, count - 1), s > 1))(
                lambda: both_sides(s - 2, combine)
            )
        return carry

    for k in range(lent):
        @pl.when(beside)
        def _():
            lend(k).wait_recv()
            for g in range(1, groups):
                spread(k, g).start()

    lax.fori_loop(0, (n - 1) * count, step, 0)
    both_sides(n - 1, sum_cores)
    both_sides(n - 1, sum_chips)
    if lent:
        both_sides(n - 2, combine)
    loads[8].wait()

    for j in range(share):
        source = head * share + j
        if lent:
            outer = jnp.logical_and(source != me, jnp.logical_or(source == 0, source == n - 1))
            source = jnp.where(outer, jnp.where(source == 0, 1, n - 2), source)
        for k in range(heads):
            here = jnp.logical_and(source == me, k == head)

            @pl.when(jnp.logical_not(here))
            def _():
                remote(
                    fin_out.at[0, 0], final.at[j, k], fin_send.at[0, 0], fin_recv.at[j, k],
                    {"ctx": source, "heads": k},
                ).wait_recv()

            part = slice((k // cores) * strip, (k // cores + 1) * strip)
            lo = j * out_width + (k % cores) * half
            residual[part, lo : lo + half] = (
                resid_ref[part, lo : lo + half].astype(F32) + final[j, k].astype(F32)
            )

    for load in loads[11:]:
        load.wait()
    latent_width = latent_ref.shape[1]
    strand = latent_width // heads
    features = residual.shape[1] * heads
    experts_here = grow_ref.shape[0]
    slot_rows = experts_here * CAP
    held = residual[...]
    scaled = (held * moe_ref[...]).astype(BF)
    picked = jnp.dot(placed[...], scaled, preferred_element_type=F32).astype(BF)
    power = jnp.sum(held * held, axis=1, keepdims=True)
    power = jnp.transpose(jnp.broadcast_to(power, (rows, 128)))[:8, :]
    square_out[...] = lax.dot_general(
        power, placed[...].astype(F32), (((1,), (1,)), ((), ())),
        precision=lax.Precision.HIGHEST, preferred_element_type=F32,
    )

    def square_copy(k):
        return remote(
            square_out, square_in.at[k], square_send.at[k], square_recv.at[k],
            {"heads": (head + k) % heads},
        )

    def first_copy(k):
        to = (head + k) % heads
        return remote(
            slots_out.at[k], slots_in.at[k], first_send.at[k], first_recv.at[k], {"heads": to}
        )

    for k in range(1, heads):
        square_copy(k).start()
    for k in [*range(1, heads), 0]:
        to = (head + k) % heads
        lane = pl.ds(pl.multiple_of(to * strand, strand), strand)
        value = jnp.dot(picked, latent_ref[:, lane], preferred_element_type=F32).astype(BF)
        for z in range(n):
            slots_out[k, z] = value[z * slot_rows : (z + 1) * slot_rows]
        if k:
            first_copy(k).start()

    def second_copy(k):
        to = (me + k) % n
        return remote(
            middle.at[to], gathered.at[head, me], second_send.at[k], second_recv.at[k], {"ctx": to}
        )

    def third_copy(k, j):
        spot = gathered.at[head, (me + n - k) % n]
        return remote(
            spot, spot, third_send.at[k, j], third_recv.at[k, j], {"heads": (head + j) % heads}
        )

    power = square_out[...]
    for k in range(1, heads):
        square_copy(k).wait_recv()
        power = power + square_in[k]
    scale = lax.rsqrt(power / features + epsilon)
    scale = jnp.transpose(jnp.broadcast_to(scale[0:1, :], (128, scale.shape[1])))
    for k in range(1, heads):
        first_copy(k).wait_recv()
    for z in range(n):
        total = slots_out[0, z].astype(F32)
        for k in range(1, heads):
            total = total + slots_in[k, z].astype(F32)
        middle[z] = (total * scale[z * slot_rows : (z + 1) * slot_rows, 0:1]).astype(BF)
    for k in range(1, n):
        second_copy(k).start()
    gathered[head, me] = middle[me]
    for k in range(n):
        if k:
            second_copy(k).wait_recv()
        for j in range(1, heads):
            third_copy(k, j).start()
    for k in range(n):
        for j in range(1, heads):
            third_copy(k, j).wait_recv()

    def fourth_copy(e, k):
        return remote(
            back_out.at[e, (head + k) % heads], back_in.at[e, k], fourth_send.at[e, k],
            fourth_recv.at[e, k], {"heads": (head + k) % heads},
        )

    def fifth_copy(e, k):
        to = (me + k) % n
        return remote(
            back_middle.at[e, to], returned.at[head, me, e], fifth_send.at[e, k],
            fifth_recv.at[e, k], {"ctx": to},
        )

    def sixth_copy(k, j):
        spot = returned.at[head, (me + n - k) % n]
        return remote(
            spot, spot, sixth_send.at[k, j], sixth_recv.at[k, j], {"heads": (head + j) % heads}
        )

    for e in range(experts_here):
        part = slice(e * CAP, (e + 1) * CAP)
        fed = jnp.concatenate(
            [gathered[h, :, part].reshape(n * CAP, strand) for h in range(heads)], axis=1
        )
        hidden = lax.dot_general(
            fed, grow_ref[e], (((1,), (1,)), ((), ())), preferred_element_type=F32
        )
        hidden = (jnp.maximum(hidden, 0.0) ** 2).astype(BF)
        value = jnp.dot(hidden, shrink_ref[e], preferred_element_type=F32).astype(BF)
        for h in range(heads):
            for z in range(n):
                back_out[e, h, z] = value[z * CAP : (z + 1) * CAP, h * strand : (h + 1) * strand]
        for k in range(1, heads):
            fourth_copy(e, k).start()
    for e in range(experts_here):
        for k in range(1, heads):
            fourth_copy(e, k).wait_recv()
        total = back_out[e, head].astype(F32)
        for k in range(1, heads):
            total = total + back_in[e, k].astype(F32)
        back_middle[e] = total.astype(BF)
        for k in range(1, n):
            fifth_copy(e, k).start()
        returned[head, me, e] = back_middle[e, me]
    for k in range(n):
        if k:
            for e in range(experts_here):
                fifth_copy(e, k).wait_recv()
        for j in range(1, heads):
            sixth_copy(k, j).start()
    for k in range(n):
        for j in range(1, heads):
            sixth_copy(k, j).wait_recv()
    combined = jnp.concatenate(
        [
            lax.dot_general(
                table[...], returned[h].reshape(wave * CAP, strand), (((0,), (0,)), ((), ())),
                preferred_element_type=F32,
            ).astype(BF)
            for h in range(heads)
        ],
        axis=1,
    )
    lift_step = min(256, residual.shape[1])
    for lo in range(0, residual.shape[1], lift_step):
        part = slice(lo, lo + lift_step)
        value = jnp.dot(combined, lift_ref[:, part], preferred_element_type=F32)
        out_ref[:, part] = (residual[:, part] + value).astype(BF)

    for k in range(1, heads):
        square_copy(k).wait_send()
        first_copy(k).wait_send()
        for e in range(experts_here):
            fourth_copy(e, k).wait_send()
    for k in range(n):
        for j in range(1, heads):
            third_copy(k, j).wait_send()
            sixth_copy(k, j).wait_send()
        if k:
            second_copy(k).wait_send()
            for e in range(experts_here):
                fifth_copy(e, k).wait_send()
    for q in range(pairs):
        pl.when(has_next)(lambda: chain_copy(q).wait_send())
    for b in range(n):
        for p in range(count):
            pl.when(jnp.logical_and(goes_up(p), b <= me))(lambda: upward(b, p).wait_send())
            pl.when(jnp.logical_and(goes_down(p), b >= me))(lambda: downward(b, p).wait_send())
        core_copy(b, 0).wait_send()
        for k in range(1, chips):
            chip_copy(b, k, 0).wait_send()
        sent = jnp.logical_or(to_beside(b), jnp.logical_not(local_final(b, me)))
        pl.when(sent)(lambda: final_copy(b, me, 0).wait_send())

        if lent:
            @pl.when(helps(b))
            def _():
                core_copy(b, 1).wait_send()
                for k in range(1, chips):
                    chip_copy(b, k, 1).wait_send()
                pl.when(jnp.logical_not(local_final(b, end_here)))(
                    lambda: final_copy(b, end_here, 1).wait_send()
                )

    for k in range(lent):
        pl.when(at_end)(lambda: lend(k).wait_send())
        for g in range(1, groups):
            pl.when(beside)(lambda: spread(k, g).wait_send())


def reaching(collective_id, grant=48 * 1024 * 1024):
    return pltpu.CompilerParams(
        collective_id=collective_id, has_side_effects=True, vmem_limit_bytes=grant
    )


def dma(*shape):
    return pltpu.SemaphoreType.DMA(shape)


def local(
    ssm_input,
    decay_log,
    state_write,
    state_read,
    skip_scale,
    gate_input,
    ssm_gain,
    weight,
    residual_in,
    moe_gain,
    down_latent,
    expert_up,
    expert_down,
    up_latent,
    expert_ids,
    combine_fixed,
):
    n, heads, groups = lax.axis_size("ctx"), lax.axis_size("heads"), lax.axis_size("groups")
    rows, columns = ssm_input.shape
    head_count = decay_log.shape[1]
    width = columns // head_count
    states = state_write.shape[1]
    span = 2 * width
    pairs = columns // span
    piece = GRP // 4
    count = columns // piece
    lent = LENT_NUM * count // LENT_DEN if n > 3 else 0
    out_width = weight.shape[1]
    share = n // heads
    chips = heads // 2
    half, strip = out_width // 2, rows // chips
    lane_count = -(-head_count // 128) * 128
    block = (rows, out_width)
    features = residual_in.shape[1]
    experts_here = expert_up.shape[0]
    wave = experts_here * n
    slot_rows = experts_here * CAP
    strand = down_latent.shape[1] // heads
    grow = expert_up.transpose(0, 2, 1)
    ids, fixed = expert_ids.T, combine_fixed.T
    anywhere = pl.BlockSpec(memory_space=pltpu.HBM)
    return pl.pallas_call(
        functools.partial(layer_kernel, n, heads, groups, width, piece, 3, lent),
        out_shape=jax.ShapeDtypeStruct((rows, features), BF),
        in_specs=[anywhere] * 16,
        out_specs=vmem()[0],
        scratch_shapes=[
            pltpu.VMEM((rows, columns), BF),
            pltpu.VMEM((rows, states), BF),
            pltpu.VMEM((rows, states), BF),
            pltpu.VMEM((head_count, rows), F32),
            pltpu.VMEM((1, head_count), F32),
            pltpu.VMEM(weight.shape, BF),
            pltpu.VMEM((rows, columns), BF),
            pltpu.VMEM((1, columns), F32),
            pltpu.VMEM(residual_in.shape, BF),
            pltpu.VMEM(ids.shape, jnp.int32),
            pltpu.VMEM(fixed.shape, jnp.int32),
            pltpu.VMEM((1, features), F32),
            pltpu.VMEM(down_latent.shape, BF),
            pltpu.VMEM(grow.shape, BF),
            pltpu.VMEM(expert_down.shape, BF),
            pltpu.VMEM(up_latent.shape, BF),
            pltpu.VMEM((rows, lane_count), F32),
            pltpu.VMEM((head_count, rows), F32),
            pltpu.VMEM((8, lane_count), F32),
            pltpu.VMEM((rows, rows), F32),
            pltpu.VMEM((pairs, rows, span), F32),
            pltpu.VMEM((pairs, states, span), F32),
            pltpu.VMEM((pairs, 1, span), F32),
            pltpu.VMEM((pairs, states, span), BF),
            pltpu.VMEM((pairs, states, span), BF),
            pltpu.VMEM((GRP // span, rows, span), F32),
            pltpu.VMEM((n, count, rows, piece), BF),
            pltpu.VMEM((3,) + block, F32),
            pltpu.VMEM((2, n, 2, rows, half), BF),
            pltpu.VMEM((2, n, rows, half), BF),
            pltpu.VMEM((2, n, chips, strip, half), BF),
            pltpu.VMEM((2, n, chips, strip, half), BF),
            pltpu.VMEM((2, n, strip, half), BF),
            pltpu.VMEM((share, heads, strip, half), BF),
            pltpu.VMEM((max(lent, 1) * piece, out_width), BF),
            pltpu.VMEM((n, strip, half), BF),
            pltpu.VMEM((rows, features), F32),
            pltpu.VMEM((wave, rows), F32),
            pltpu.VMEM((wave, rows), jnp.int32),
            pltpu.VMEM((wave * CAP, rows), BF),
            pltpu.VMEM((wave * CAP, rows), BF),
            pltpu.VMEM((8, wave * CAP), F32),
            pltpu.VMEM((heads, 8, wave * CAP), F32),
            pltpu.VMEM((heads, n, slot_rows, strand), BF),
            pltpu.VMEM((heads, n, slot_rows, strand), BF),
            pltpu.VMEM((n, slot_rows, strand), BF),
            pltpu.VMEM((heads, n, slot_rows, strand), BF),
            pltpu.VMEM((experts_here, heads, n, CAP, strand), BF),
            pltpu.VMEM((experts_here, heads, n, CAP, strand), BF),
            pltpu.VMEM((experts_here, n, CAP, strand), BF),
            pltpu.VMEM((heads, n, experts_here, CAP, strand), BF),
            dma(16), dma(pairs), dma(pairs),
            dma(n, count), dma(n, count), dma(n, count), dma(n, count),
            dma(2, n), dma(2, n), dma(2, n, chips), dma(2, n, chips), dma(2, n), dma(share, heads),
            dma(max(lent, 1)), dma(max(lent, 1)), dma(max(lent, 1), groups), dma(max(lent, 1), groups), dma(n),
            dma(heads), dma(heads), dma(heads), dma(heads), dma(n), dma(n),
            dma(n, heads), dma(n, heads), dma(experts_here, heads), dma(experts_here, heads),
            dma(experts_here, n), dma(experts_here, n), dma(n, heads), dma(n, heads),
        ],
        compiler_params=reaching(1, 67043328),
    )(
        ssm_input, state_write, state_read, decay_log.T, skip_scale.reshape(1, head_count), weight,
        gate_input, ssm_gain.reshape(1, columns), residual_in,
        ids, fixed, moe_gain.reshape(1, features), down_latent, grow, expert_down, up_latent,
    )


def solution(mesh):
    placed = (
        P(("groups", "ctx"), "heads"),
        P(("groups", "ctx"), "heads"),
        P(("groups", "ctx"), None),
        P(("groups", "ctx"), None),
        P("heads"),
        P(("groups", "ctx"), "heads"),
        P("heads"),
        P("heads", "ctx"),
        P(("groups", "ctx"), "heads"),
        P("heads"),
        P("heads", None),
        P("ctx", None, "heads"),
        P("ctx", "heads", None),
        P(None, "heads"),
        P(("groups", "ctx"), None),
        P(("groups", "ctx"), None),
    )
    return jax.shard_map(
        local, mesh=mesh, in_specs=placed, out_specs=P(("groups", "ctx"), "heads"), check_vma=False
    )
```

```python
import functools

import jax
import jax.numpy as jnp
from jax import lax
from jax.experimental import pallas as pl
from jax.experimental.pallas import tpu as pltpu
from jax.sharding import PartitionSpec as P

GRP = 1024
CAP = 16
LENT_NUM, LENT_DEN = 1, 2
WAVES = 4


epsilon = 1e-05


MESH = pl.DeviceIdType.MESH
BF = jnp.bfloat16
F32 = jnp.float32


def vmem(count=1):
    return [pl.BlockSpec(memory_space=pltpu.VMEM)] * count


def greet(device):
    pl.semaphore_signal(
        pltpu.get_barrier_semaphore(), inc=1, device_id=device, device_id_type=MESH
    )


def greeted(count):
    pl.semaphore_wait(pltpu.get_barrier_semaphore(), count)


def remote(src, dst, send, recv, device):
    return pltpu.make_async_remote_copy(
        src_ref=src, dst_ref=dst, send_sem=send, recv_sem=recv, device_id=device, device_id_type=MESH
    )


def pair_wide(first, second, width):
    lane = lax.broadcasted_iota(jnp.int32, (first.shape[0], 2 * width), 1)
    return jnp.where(lane < width, first, second)


def layer_kernel(
    n, heads, groups, width, piece, lag, lent, waves,
    x_hbm, write_hbm, read_hbm, decay_hbm, skip_hbm, weight_hbm, gate_hbm, gain_hbm, resid_hbm,
    ids_hbm, fixed_hbm, moe_hbm, latent_hbm, grow_hbm, shrink_hbm, lift_hbm,
    out_ref,
    x_ref, write_ref, read_ref, decay_ref, skip_ref, weight_ref, gate_ref, gain_ref, resid_ref,
    ids_ref, fixed_ref, moe_ref, latent_ref, grow_ref, shrink_ref, lift_ref,
    cum, cum_rows, skips, inter,
    mixed, state, ends, prior, outgoing, gated,
    kept, rest, acc, parts, core_in, chip_out, x_in, fin_out, final, borrowed, strips,
    residual, chosen, weights, placed, table, square_out, square_in,
    slots_out, slots_in, middle, gathered, back_out, back_in, back_middle, returned,
    load_sem, chain_send, chain_recv, up_send, up_recv, down_send, down_recv,
    up_rest_send, up_rest_recv, down_rest_send, down_rest_recv,
    core_send, core_recv, x_send, x_recv, fin_send, fin_recv, lend_send, lend_recv, spread_send, spread_recv, strip_recv,
    square_send, square_recv, first_send, first_recv, second_send, second_recv,
    third_send, third_recv, fourth_send, fourth_recv, fifth_send, fifth_recv, sixth_send, sixth_recv,
):
    me, head, group = lax.axis_index("ctx"), lax.axis_index("heads"), lax.axis_index("groups")
    rows, columns = x_ref.shape
    span = 2 * width
    pairs = columns // span
    head_count = decay_ref.shape[0]
    out_width = weight_ref.shape[1]
    count = columns // piece
    share = n // heads
    cores = 2
    chips = heads // cores
    core, chip = head % cores, head // cores
    half, band_rows = out_width // cores, rows // waves
    strip = band_rows // chips
    has_prev, has_next = me > 0, me < n - 1
    prev, after = jnp.maximum(me - 1, 0), jnp.minimum(me + 1, n - 1)
    keep = count - lent
    keep_width = keep * piece
    at_end = jnp.logical_or(me == 0, me == n - 1)
    beside = jnp.logical_or(me == 1, me == n - 2)
    end_here = jnp.where(me == 1, 0, n - 1)
    beside_here = jnp.where(me == 0, 1, n - 2)

    loads = [
        pltpu.make_async_copy(src, dst, load_sem.at[i])
        for i, (src, dst) in enumerate(
            [
                (x_hbm, x_ref), (write_hbm, write_ref), (read_hbm, read_ref), (decay_hbm, decay_ref),
                (skip_hbm, skip_ref), (weight_hbm, weight_ref), (gate_hbm, gate_ref),
                (gain_hbm, gain_ref), (resid_hbm, resid_ref),
                (ids_hbm, ids_ref), (fixed_hbm, fixed_ref), (moe_hbm, moe_ref),
                (latent_hbm, latent_ref), (grow_hbm, grow_ref), (shrink_hbm, shrink_ref),
                (lift_hbm, lift_ref),
            ]
        )
    ]
    for load in loads[:8]:
        load.start()
    for i in range(n):
        for j in range(heads):
            if i or j:
                greet({"ctx": (me + i) % n, "heads": (head + j) % heads})
    for i in range(1, groups):
        greet({"groups": (group + i) % groups})

    t = lax.broadcasted_iota(jnp.int32, (rows, rows), 0)
    s = lax.broadcasted_iota(jnp.int32, (rows, rows), 1)
    lower = jnp.where(t >= s, 1.0, 0.0)
    cum[...] = jnp.zeros(cum.shape, F32)
    for load in loads[:5]:
        load.wait()
    cum[:, :head_count] = lax.dot_general(
        lower, decay_ref[...], (((1,), (1,)), ((), ())),
        precision=lax.Precision.HIGHEST, preferred_element_type=F32,
    )
    cum_rows[...] = lax.dot_general(
        decay_ref[...], lower, (((1,), (1,)), ((), ())),
        precision=lax.Precision.HIGHEST, preferred_element_type=F32,
    )
    skips[...] = jnp.zeros(skips.shape, F32)
    skips[0:1, :head_count] = skip_ref[...]
    product = lax.dot_general(
        read_ref[...], write_ref[...], (((1,), (1,)), ((), ())), preferred_element_type=F32
    )
    inter[...] = jnp.where(t >= s, product, 0.0)
    greeted(n * heads + groups - 2)

    for load in loads[8:]:
        load.start()
    share_rows = piece // groups

    def lend(k):
        return remote(
            weight_ref.at[pl.ds((keep + k) * piece + group * share_rows, share_rows)],
            borrowed.at[pl.ds(k * piece + group * share_rows, share_rows)],
            lend_send.at[k], lend_recv.at[k], {"ctx": beside_here},
        )

    def spread(k, i, back=False):
        owner = (group + groups - i) % groups if back else group
        part = borrowed.at[pl.ds(k * piece + owner * share_rows, share_rows)]
        return remote(
            part, part, spread_send.at[k, i], spread_recv.at[k, i],
            {"groups": (group + i) % groups},
        )

    @pl.when(me == n - 1)
    def _():
        loads[5].wait()
        for k in range(lent):
            lend(k).start()

    def lanes(p):
        return pl.ds(pl.multiple_of(p * span, span), span)

    def shifted(ref, p):
        lane_count = ref.shape[1]
        return pltpu.roll(ref[...], (lane_count - 2 * p) % lane_count, 1)

    band = rows // 2
    causal = lax.broadcasted_iota(jnp.int32, (band, band), 0) >= lax.broadcasted_iota(
        jnp.int32, (band, band), 1
    )

    def scan(p):
        x = x_ref[:, lanes(p)]
        cols = shifted(cum, p)
        skip = shifted(skips, p)
        outs, tails, lasts = [], [], []
        for j in range(2):
            col = cols[:, j : j + 1]
            row = cum_rows[pl.ds(2 * p + j, 1), :]
            last = col[rows - 1 : rows, :]
            lane = x[:, j * width : (j + 1) * width]
            bands = []
            for lo in range(0, rows, band):
                hi = lo + band
                spread = jnp.where(causal, col[lo:hi] - row[:, lo:hi], 0.0)
                if lo:
                    spread = jnp.concatenate([col[lo:hi] - row[:, :lo], spread], axis=1)
                mixing = (jnp.exp(-spread) * inter[lo:hi, :hi]).astype(BF)
                bands.append(jnp.dot(mixing, lane[:hi], preferred_element_type=F32))
            outs.append(jnp.concatenate(bands, axis=0))
            tails.append(jnp.exp(col - last))
            lasts.append(jnp.exp(-last))
        wide = x.astype(F32)
        direct = pair_wide(skip[0:1, 0:1], skip[0:1, 1:2], width) * wide
        mixed[p] = jnp.concatenate(outs, axis=1) + direct
        scaled = (wide * pair_wide(tails[0], tails[1], width)).astype(BF)
        state[p] = lax.dot_general(
            write_ref[...], scaled, (((0,), (0,)), ((), ())), preferred_element_type=F32
        )
        ends[p] = pair_wide(lasts[0], lasts[1], width)

    def chain_copy(q):
        return remote(
            outgoing.at[q], prior.at[q], chain_send.at[q], chain_recv.at[q], {"ctx": after}
        )

    def chain(q):
        @pl.when(me == 0)
        def _():
            prior[q] = jnp.zeros(prior.shape[1:], BF)
            outgoing[q] = state[q].astype(BF)

        @pl.when(has_prev)
        def _():
            chain_copy(q).wait_recv()
            outgoing[q] = (prior[q].astype(F32) * ends[q] + state[q]).astype(BF)

        pl.when(has_next)(lambda: chain_copy(q).start())

    def across(ref, sems, b, r, to):
        spot = ref.at[b, r]
        return remote(spot, spot, sems[0].at[b, r], sems[1].at[b, r], {"ctx": to})

    def upward(b, r):
        return across(kept, (up_send, up_recv), b, r, after)

    def downward(b, r):
        return across(kept, (down_send, down_recv), b, r, prev)

    def upward_rest(b, r):
        return across(rest, (up_rest_send, up_rest_recv), b, r, after)

    def downward_rest(b, r):
        return across(rest, (down_rest_send, down_rest_recv), b, r, prev)

    rest_up = jnp.logical_and(has_next, me + 1 < n - 1)
    rest_down = jnp.logical_and(has_prev, me > 1)
    inner = jnp.logical_not(at_end)

    group_pairs = GRP // span
    loads[6].wait()
    loads[7].wait()

    def gate(g):
        squares = jnp.zeros((rows, span), F32)
        for i in range(group_pairs):
            p = g * group_pairs + i
            cols = shifted(cum, p)
            reach = jnp.exp(-pair_wide(cols[:, 0:1], cols[:, 1:2], width))
            carried = jnp.dot(read_ref[...], prior[p], preferred_element_type=F32) * reach
            gating = gate_ref[:, lanes(p)].astype(F32)
            value = (mixed[p] + carried) * (gating / (1.0 + jnp.exp(-gating)))
            gated[i] = value
            squares = squares + value * value
        scale = lax.rsqrt(jnp.sum(squares, axis=1, keepdims=True) / GRP + epsilon)
        for i in range(group_pairs):
            p = g * group_pairs + i
            value = (gated[i] * scale * gain_ref[:, lanes(p)]).astype(BF)
            ref, lo = (kept, p * span) if p * span < keep_width else (rest, p * span - keep_width)
            for r in range(waves):
                ref[me, r, :, lo : lo + span] = value[r * band_rows : (r + 1) * band_rows]

    early = keep_width // GRP if lent and keep_width % GRP == 0 else 0

    def begin_down():
        for r in range(waves):
            pl.when(has_prev)(lambda: downward(me, r).start())

    def advance(i, carry):
        pl.when(i < pairs)(lambda: scan(i))
        q = i - lag * me
        pl.when(jnp.logical_and(q >= 0, q < pairs))(lambda: chain(q))
        if early:
            @pl.when(i == jnp.maximum(pairs - 1, early * group_pairs - 1 + lag * me))
            def _():
                for g in range(early):
                    gate(g)
                begin_down()

        return carry

    lax.fori_loop(0, pairs + lag * (n - 1), advance, 0)
    pl.when(me < n - 1)(lambda: loads[5].wait())
    for k in range(lent):
        pl.when(me == 0)(lambda: lend(k).start())
    for g in range(early, columns // GRP):
        gate(g)
    if not early:
        begin_down()
    for r in range(waves):
        pl.when(has_next)(lambda: upward(me, r).start())
    if lent:
        for r in range(waves):
            pl.when(rest_up)(lambda: upward_rest(me, r).start())
            pl.when(rest_down)(lambda: downward_rest(me, r).start())

    col_step = min(out_width, 256)

    def multiply(slot, b, r):
        for lo in range(0, out_width, col_step):
            acc[slot, r, :, lo : lo + col_step] = jnp.dot(
                kept[b, r], weight_ref[:keep_width, lo : lo + col_step], preferred_element_type=F32
            )

    def multiply_rest(slot, b, r):
        for lo in range(0, out_width, col_step):
            acc[slot, r, :, lo : lo + col_step] += jnp.dot(
                rest[b, r], weight_ref[keep_width:, lo : lo + col_step], preferred_element_type=F32
            )

    def core_copy(b, r, kind):
        return remote(
            parts.at[kind, b, r, 1 - core], core_in.at[kind, b, r], core_send.at[kind, b, r],
            core_recv.at[kind, b, r], {"heads": head + 1 - 2 * core},
        )

    def round_partial(b, r, slot, kind=0):
        for k in range(cores):
            parts[kind, b, r, k] = acc[slot, r, :, k * half : (k + 1) * half].astype(BF)
        core_copy(b, r, kind).start()

    def chip_copy(b, r, k, kind):
        to = (chip + k) % chips
        return remote(
            chip_out.at[kind, b, r, to], x_in.at[kind, b, r, k], x_send.at[kind, b, r, k],
            x_recv.at[kind, b, r, k], {"heads": to * cores + core},
        )

    def sum_cores(b, r, kind=0):
        core_copy(b, r, kind).wait_recv()
        for k in range(chips):
            part = slice(k * strip, (k + 1) * strip)
            both = parts[kind, b, r, core, part].astype(F32) + core_in[kind, b, r, part].astype(F32)
            chip_out[kind, b, r, k] = both.astype(BF)
        for k in range(1, chips):
            chip_copy(b, r, k, kind).start()

    def local_final(b, column):
        return jnp.logical_and(b == me, head == column // share)

    def final_copy(b, r, column, kind):
        return remote(
            fin_out.at[kind, b, r], final.at[column % share, head, r], fin_send.at[kind, b, r],
            fin_recv.at[column % share, head, r], {"ctx": b, "heads": column // share},
        )

    def strip_copy(b, r):
        return remote(
            fin_out.at[0, b, r], strips.at[b, r], fin_send.at[0, b, r], strip_recv.at[b, r],
            {"ctx": beside_here},
        )

    def to_beside(b):
        if not lent:
            return False
        return jnp.logical_and(at_end, b != me)

    def strip_total(b, r, kind):
        part = pl.ds(pl.multiple_of(chip * strip, strip), strip)
        total = parts[kind, b, r, core, part].astype(F32) + core_in[kind, b, r, part].astype(F32)
        for k in range(1, chips):
            chip_copy(b, r, k, kind).wait_recv()
            total = total + x_in[kind, b, r, k].astype(F32)
        return total

    def deliver(b, r, column, kind, total):
        @pl.when(local_final(b, column))
        def _():
            final[column % share, head, r] = total.astype(BF)

        pl.when(jnp.logical_not(local_final(b, column)))(
            lambda: final_copy(b, r, column, kind).start()
        )

    def sum_chips(b, r):
        total = strip_total(b, r, 0)
        fin_out[0, b, r] = total.astype(BF)
        if lent:
            pl.when(to_beside(b))(lambda: strip_copy(b, r).start())
            pl.when(jnp.logical_not(to_beside(b)))(lambda: deliver(b, r, me, 0, total))
        else:
            deliver(b, r, me, 0, total)

    def helps(b):
        return jnp.logical_and(beside, b != end_here)

    def helping(b, r):
        @pl.when(helps(b))
        def _():
            for lo in range(0, out_width, col_step):
                acc[2, r, :, lo : lo + col_step] = jnp.dot(
                    rest[b, r], borrowed[:, lo : lo + col_step], preferred_element_type=F32
                )
            round_partial(b, r, 2, 1)

    def reduce_help(b, r):
        pl.when(helps(b))(lambda: sum_cores(b, r, 1))

    def combine(b, r):
        @pl.when(helps(b))
        def _():
            strip_copy(b, r).wait_recv()
            total = strip_total(b, r, 1) + strips[b, r].astype(F32)
            fin_out[1, b, r] = total.astype(BF)
            deliver(b, r, end_here, 1, total)

    def own(r, carry):
        multiply(0, me, r)
        if lent:
            multiply_rest(0, me, r)
        round_partial(me, r, 0)
        return carry

    lax.fori_loop(0, waves, own, 0)

    loads[9].wait()
    loads[10].wait()
    wave = chosen.shape[0]
    for e in range(wave):
        named = ids_ref[...] == e
        chosen[e : e + 1, :] = jnp.sum(jnp.where(named, 1.0, 0.0), axis=0, keepdims=True)
        weights[e : e + 1, :] = jnp.sum(jnp.where(named, fixed_ref[...], 0), axis=0, keepdims=True)
    upto = jnp.where(t <= s, 1.0, 0.0).astype(BF)
    taken = jnp.dot(chosen[...].astype(BF), upto, preferred_element_type=F32)
    slot = lax.broadcasted_iota(jnp.int32, (CAP, rows), 0).astype(F32) + 1.0
    for e in range(wave):
        here = jnp.logical_and(chosen[e : e + 1, :] > 0.5, taken[e : e + 1, :] == slot)
        weight = weights[e : e + 1, :].astype(F32) / 65536.0
        part = slice(e * CAP, (e + 1) * CAP)
        placed[part] = jnp.where(here, 1.0, 0.0).astype(BF)
        table[part] = jnp.where(here, weight, 0.0).astype(BF)

    held_back = jnp.where(me == 1, 1, 0) if lent else 0

    def low_block(s):
        low = me - s + jnp.where(s > 0, held_back, 0)
        return jnp.where(jnp.logical_and(s > 0, low >= me), -1, low)

    def around(s, act):
        low, high = low_block(s), me + s
        pl.when(low >= 0)(lambda: act(jnp.maximum(low, 0), 0))

        @pl.when(jnp.logical_and(high < n, s > 0))
        def _():
            act(jnp.minimum(high, n - 1), 1)

    turns = 2 * waves
    ripe = jnp.where(at_end, 0, waves) if lent else 0

    def finished(i, act):
        s, r = i // turns, i % turns - ripe
        fits = jnp.logical_and(jnp.logical_and(r >= 0, r < waves), s > 0)
        spot = jnp.maximum(jnp.minimum(r, waves - 1), 0)
        pl.when(fits)(lambda: around(s, lambda b, slot: act(b, spot, slot)))

    def pass_on(k):
        lend(k).wait_recv()
        for g in range(1, groups):
            spread(k, g).start()

    for r in range(waves):
        sum_cores(me, r)
    for r in range(waves):
        sum_chips(me, r)
    for k in range(lent):
        pl.when(me == n - 2)(lambda: pass_on(k))
    first_help = 2 * turns + waves

    def step(i, carry):
        s, u = i // turns, i % turns
        low, high = low_block(s), me + s
        low_spot, high_spot = jnp.maximum(low, 0), jnp.minimum(high, n - 1)
        has_low, has_high = low >= 0, high < n

        @pl.when(u < waves)
        def _():
            r = jnp.minimum(u, waves - 1)

            @pl.when(has_low)
            def _():
                upward(low_spot, r).wait_recv()
                pl.when(has_next)(lambda: upward(low_spot, r).start())

            @pl.when(has_high)
            def _():
                downward(high_spot, r).wait_recv()
                pl.when(has_prev)(lambda: downward(high_spot, r).start())

            around(s, lambda b, slot: multiply(slot, b, r))

        if lent:
            @pl.when(jnp.logical_and(u >= waves, inner))
            def _():
                r = jnp.maximum(u - waves, 0)

                @pl.when(has_low)
                def _():
                    upward_rest(low_spot, r).wait_recv()
                    pl.when(rest_up)(lambda: upward_rest(low_spot, r).start())

                @pl.when(has_high)
                def _():
                    downward_rest(high_spot, r).wait_recv()
                    pl.when(rest_down)(lambda: downward_rest(high_spot, r).start())

                around(s, lambda b, slot: multiply_rest(slot, b, r))

        finished(i, lambda b, r, slot: round_partial(b, r, slot))
        finished(i - 1, lambda b, r, slot: sum_cores(b, r))
        finished(i - 3, lambda b, r, slot: sum_chips(b, r))
        for k in range(lent):
            when = min(turns + waves + (k + 1) * waves // lent, 2 * turns)
            pl.when(jnp.logical_and(i == when, me == 1))(lambda: pass_on(k))
        if lent:
            def early_help(spot, act):
                r = jnp.maximum(jnp.minimum(i - spot, waves - 1), 0)

                @pl.when(jnp.logical_and(i >= spot, i < spot + waves))
                def _():
                    for base in range(2):
                        around(base, lambda b, slot: act(b, r))

            @pl.when(jnp.logical_and(i == first_help, beside))
            def _():
                for k in range(lent):
                    for g in range(1, groups):
                        spread(k, g, True).wait_recv()

            early_help(first_help, helping)
            early_help(first_help + 1, reduce_help)
            early_help(first_help + 4, combine)

            def later(back, act):
                pl.when(i - back >= 2 * turns)(
                    lambda: finished(i - back, lambda b, r, slot: act(b, r))
                )

            later(1, helping)
            later(2, reduce_help)
            later(4, combine)
        return carry

    lax.fori_loop(turns, n * turns + 4, step, 0)
    loads[8].wait()

    for j in range(share):
        source = head * share + j
        if lent:
            outer = jnp.logical_and(source != me, jnp.logical_or(source == 0, source == n - 1))
            source = jnp.where(outer, jnp.where(source == 0, 1, n - 2), source)
        for k in range(heads):
            here = jnp.logical_and(source == me, k == head)

            for r in range(waves):
                @pl.when(jnp.logical_not(here))
                def _():
                    remote(
                        fin_out.at[0, 0, r], final.at[j, k, r], fin_send.at[0, 0, r],
                        fin_recv.at[j, k, r], {"ctx": source, "heads": k},
                    ).wait_recv()

                base = r * band_rows + (k // cores) * strip
                part = slice(base, base + strip)
                lo = j * out_width + (k % cores) * half
                residual[part, lo : lo + half] = (
                    resid_ref[part, lo : lo + half].astype(F32) + final[j, k, r].astype(F32)
                )

    for load in loads[11:]:
        load.wait()
    latent_width = latent_ref.shape[1]
    strand = latent_width // heads
    features = residual.shape[1] * heads
    experts_here = grow_ref.shape[0]
    slot_rows = experts_here * CAP
    held = residual[...]
    scaled = (held * moe_ref[...]).astype(BF)
    picked = jnp.dot(placed[...], scaled, preferred_element_type=F32).astype(BF)
    power = jnp.sum(held * held, axis=1, keepdims=True)
    power = jnp.transpose(jnp.broadcast_to(power, (rows, 128)))[:8, :]
    square_out[...] = lax.dot_general(
        power, placed[...].astype(F32), (((1,), (1,)), ((), ())),
        precision=lax.Precision.HIGHEST, preferred_element_type=F32,
    )

    def square_copy(k):
        return remote(
            square_out, square_in.at[k], square_send.at[k], square_recv.at[k],
            {"heads": (head + k) % heads},
        )

    def first_copy(k):
        to = (head + k) % heads
        return remote(
            slots_out.at[k], slots_in.at[k], first_send.at[k], first_recv.at[k], {"heads": to}
        )

    for k in range(1, heads):
        square_copy(k).start()
    for k in [*range(1, heads), 0]:
        to = (head + k) % heads
        lane = pl.ds(pl.multiple_of(to * strand, strand), strand)
        value = jnp.dot(picked, latent_ref[:, lane], preferred_element_type=F32).astype(BF)
        for z in range(n):
            slots_out[k, z] = value[z * slot_rows : (z + 1) * slot_rows]
        if k:
            first_copy(k).start()

    def second_copy(k):
        to = (me + k) % n
        return remote(
            middle.at[to], gathered.at[head, me], second_send.at[k], second_recv.at[k], {"ctx": to}
        )

    def third_copy(k, j):
        spot = gathered.at[head, (me + n - k) % n]
        return remote(
            spot, spot, third_send.at[k, j], third_recv.at[k, j], {"heads": (head + j) % heads}
        )

    power = square_out[...]
    for k in range(1, heads):
        square_copy(k).wait_recv()
        power = power + square_in[k]
    scale = lax.rsqrt(power / features + epsilon)
    scale = jnp.transpose(jnp.broadcast_to(scale[0:1, :], (128, scale.shape[1])))
    for k in range(1, heads):
        first_copy(k).wait_recv()
    for z in range(n):
        total = slots_out[0, z].astype(F32)
        for k in range(1, heads):
            total = total + slots_in[k, z].astype(F32)
        middle[z] = (total * scale[z * slot_rows : (z + 1) * slot_rows, 0:1]).astype(BF)
    for k in range(1, n):
        second_copy(k).start()
    gathered[head, me] = middle[me]
    for k in range(n):
        if k:
            second_copy(k).wait_recv()
        for j in range(1, heads):
            third_copy(k, j).start()
    for k in range(n):
        for j in range(1, heads):
            third_copy(k, j).wait_recv()

    def fourth_copy(e, k):
        return remote(
            back_out.at[e, (head + k) % heads], back_in.at[e, k], fourth_send.at[e, k],
            fourth_recv.at[e, k], {"heads": (head + k) % heads},
        )

    def fifth_copy(e, k):
        to = (me + k) % n
        return remote(
            back_middle.at[e, to], returned.at[head, me, e], fifth_send.at[e, k],
            fifth_recv.at[e, k], {"ctx": to},
        )

    def sixth_copy(k, j):
        spot = returned.at[head, (me + n - k) % n]
        return remote(
            spot, spot, sixth_send.at[k, j], sixth_recv.at[k, j], {"heads": (head + j) % heads}
        )

    for e in range(experts_here):
        part = slice(e * CAP, (e + 1) * CAP)
        fed = jnp.concatenate(
            [gathered[h, :, part].reshape(n * CAP, strand) for h in range(heads)], axis=1
        )
        hidden = lax.dot_general(
            fed, grow_ref[e], (((1,), (1,)), ((), ())), preferred_element_type=F32
        )
        hidden = (jnp.maximum(hidden, 0.0) ** 2).astype(BF)
        value = jnp.dot(hidden, shrink_ref[e], preferred_element_type=F32).astype(BF)
        for h in range(heads):
            for z in range(n):
                back_out[e, h, z] = value[z * CAP : (z + 1) * CAP, h * strand : (h + 1) * strand]
        for k in range(1, heads):
            fourth_copy(e, k).start()
    for e in range(experts_here):
        for k in range(1, heads):
            fourth_copy(e, k).wait_recv()
        total = back_out[e, head].astype(F32)
        for k in range(1, heads):
            total = total + back_in[e, k].astype(F32)
        back_middle[e] = total.astype(BF)
        for k in range(1, n):
            fifth_copy(e, k).start()
        returned[head, me, e] = back_middle[e, me]
    for k in range(n):
        if k:
            for e in range(experts_here):
                fifth_copy(e, k).wait_recv()
        for j in range(1, heads):
            sixth_copy(k, j).start()
    for k in range(n):
        for j in range(1, heads):
            sixth_copy(k, j).wait_recv()
    combined = jnp.concatenate(
        [
            lax.dot_general(
                table[...], returned[h].reshape(wave * CAP, strand), (((0,), (0,)), ((), ())),
                preferred_element_type=F32,
            ).astype(BF)
            for h in range(heads)
        ],
        axis=1,
    )
    lift_step = min(256, residual.shape[1])
    for lo in range(0, residual.shape[1], lift_step):
        part = slice(lo, lo + lift_step)
        value = jnp.dot(combined, lift_ref[:, part], preferred_element_type=F32)
        out_ref[:, part] = (residual[:, part] + value).astype(BF)

    for k in range(1, heads):
        square_copy(k).wait_send()
        first_copy(k).wait_send()
        for e in range(experts_here):
            fourth_copy(e, k).wait_send()
    for k in range(n):
        for j in range(1, heads):
            third_copy(k, j).wait_send()
            sixth_copy(k, j).wait_send()
        if k:
            second_copy(k).wait_send()
            for e in range(experts_here):
                fifth_copy(e, k).wait_send()
    for q in range(pairs):
        pl.when(has_next)(lambda: chain_copy(q).wait_send())
    for b in range(n):
        sent = jnp.logical_or(to_beside(b), jnp.logical_not(local_final(b, me)))
        for r in range(waves):
            pl.when(jnp.logical_and(has_next, b <= me))(lambda: upward(b, r).wait_send())
            pl.when(jnp.logical_and(has_prev, b >= me))(lambda: downward(b, r).wait_send())
            core_copy(b, r, 0).wait_send()
            for k in range(1, chips):
                chip_copy(b, r, k, 0).wait_send()
            pl.when(sent)(lambda: final_copy(b, r, me, 0).wait_send())
            if lent:
                pl.when(jnp.logical_and(rest_up, b <= me))(lambda: upward_rest(b, r).wait_send())
                pl.when(jnp.logical_and(rest_down, b >= me))(
                    lambda: downward_rest(b, r).wait_send()
                )

                @pl.when(helps(b))
                def _():
                    core_copy(b, r, 1).wait_send()
                    for k in range(1, chips):
                        chip_copy(b, r, k, 1).wait_send()
                    pl.when(jnp.logical_not(local_final(b, end_here)))(
                        lambda: final_copy(b, r, end_here, 1).wait_send()
                    )

    for k in range(lent):
        pl.when(at_end)(lambda: lend(k).wait_send())
        for g in range(1, groups):
            pl.when(beside)(lambda: spread(k, g).wait_send())


def reaching(collective_id, grant=48 * 1024 * 1024):
    return pltpu.CompilerParams(
        collective_id=collective_id, has_side_effects=True, vmem_limit_bytes=grant
    )


def dma(*shape):
    return pltpu.SemaphoreType.DMA(shape)


def local(
    ssm_input,
    decay_log,
    state_write,
    state_read,
    skip_scale,
    gate_input,
    ssm_gain,
    weight,
    residual_in,
    moe_gain,
    down_latent,
    expert_up,
    expert_down,
    up_latent,
    expert_ids,
    combine_fixed,
):
    n, heads, groups = lax.axis_size("ctx"), lax.axis_size("heads"), lax.axis_size("groups")
    rows, columns = ssm_input.shape
    head_count = decay_log.shape[1]
    width = columns // head_count
    states = state_write.shape[1]
    span = 2 * width
    pairs = columns // span
    piece = GRP // 4
    count = columns // piece
    lent = LENT_NUM * count // LENT_DEN if n > 3 else 0
    out_width = weight.shape[1]
    share = n // heads
    chips = heads // 2
    half, band_rows = out_width // 2, rows // WAVES
    strip = band_rows // chips
    keep_width, rest_width = (count - lent) * piece, max(lent, 1) * piece
    lane_count = -(-head_count // 128) * 128
    features = residual_in.shape[1]
    experts_here = expert_up.shape[0]
    wave = experts_here * n
    slot_rows = experts_here * CAP
    strand = down_latent.shape[1] // heads
    grow = expert_up.transpose(0, 2, 1)
    ids, fixed = expert_ids.T, combine_fixed.T
    anywhere = pl.BlockSpec(memory_space=pltpu.HBM)
    return pl.pallas_call(
        functools.partial(layer_kernel, n, heads, groups, width, piece, 3, lent, WAVES),
        out_shape=jax.ShapeDtypeStruct((rows, features), BF),
        in_specs=[anywhere] * 16,
        out_specs=vmem()[0],
        scratch_shapes=[
            pltpu.VMEM((rows, columns), BF),
            pltpu.VMEM((rows, states), BF),
            pltpu.VMEM((rows, states), BF),
            pltpu.VMEM((head_count, rows), F32),
            pltpu.VMEM((1, head_count), F32),
            pltpu.VMEM(weight.shape, BF),
            pltpu.VMEM((rows, columns), BF),
            pltpu.VMEM((1, columns), F32),
            pltpu.VMEM(residual_in.shape, BF),
            pltpu.VMEM(ids.shape, jnp.int32),
            pltpu.VMEM(fixed.shape, jnp.int32),
            pltpu.VMEM((1, features), F32),
            pltpu.VMEM(down_latent.shape, BF),
            pltpu.VMEM(grow.shape, BF),
            pltpu.VMEM(expert_down.shape, BF),
            pltpu.VMEM(up_latent.shape, BF),
            pltpu.VMEM((rows, lane_count), F32),
            pltpu.VMEM((head_count, rows), F32),
            pltpu.VMEM((8, lane_count), F32),
            pltpu.VMEM((rows, rows), F32),
            pltpu.VMEM((pairs, rows, span), F32),
            pltpu.VMEM((pairs, states, span), F32),
            pltpu.VMEM((pairs, 1, span), F32),
            pltpu.VMEM((pairs, states, span), BF),
            pltpu.VMEM((pairs, states, span), BF),
            pltpu.VMEM((GRP // span, rows, span), F32),
            pltpu.VMEM((n, WAVES, band_rows, keep_width), BF),
            pltpu.VMEM((n, WAVES, band_rows, rest_width), BF),
            pltpu.VMEM((3, WAVES, band_rows, out_width), F32),
            pltpu.VMEM((2, n, WAVES, 2, band_rows, half), BF),
            pltpu.VMEM((2, n, WAVES, band_rows, half), BF),
            pltpu.VMEM((2, n, WAVES, chips, strip, half), BF),
            pltpu.VMEM((2, n, WAVES, chips, strip, half), BF),
            pltpu.VMEM((2, n, WAVES, strip, half), BF),
            pltpu.VMEM((share, heads, WAVES, strip, half), BF),
            pltpu.VMEM((rest_width, out_width), BF),
            pltpu.VMEM((n, WAVES, strip, half), BF),
            pltpu.VMEM((rows, features), F32),
            pltpu.VMEM((wave, rows), F32),
            pltpu.VMEM((wave, rows), jnp.int32),
            pltpu.VMEM((wave * CAP, rows), BF),
            pltpu.VMEM((wave * CAP, rows), BF),
            pltpu.VMEM((8, wave * CAP), F32),
            pltpu.VMEM((heads, 8, wave * CAP), F32),
            pltpu.VMEM((heads, n, slot_rows, strand), BF),
            pltpu.VMEM((heads, n, slot_rows, strand), BF),
            pltpu.VMEM((n, slot_rows, strand), BF),
            pltpu.VMEM((heads, n, slot_rows, strand), BF),
            pltpu.VMEM((experts_here, heads, n, CAP, strand), BF),
            pltpu.VMEM((experts_here, heads, n, CAP, strand), BF),
            pltpu.VMEM((experts_here, n, CAP, strand), BF),
            pltpu.VMEM((heads, n, experts_here, CAP, strand), BF),
            dma(16), dma(pairs), dma(pairs),
            *[dma(n, WAVES)] * 8,
            dma(2, n, WAVES), dma(2, n, WAVES), dma(2, n, WAVES, chips), dma(2, n, WAVES, chips),
            dma(2, n, WAVES), dma(share, heads, WAVES),
            dma(max(lent, 1)), dma(max(lent, 1)), dma(max(lent, 1), groups), dma(max(lent, 1), groups), dma(n, WAVES),
            dma(heads), dma(heads), dma(heads), dma(heads), dma(n), dma(n),
            dma(n, heads), dma(n, heads), dma(experts_here, heads), dma(experts_here, heads),
            dma(experts_here, n), dma(experts_here, n), dma(n, heads), dma(n, heads),
        ],
        compiler_params=reaching(1, 67043328),
    )(
        ssm_input, state_write, state_read, decay_log.T, skip_scale.reshape(1, head_count), weight,
        gate_input, ssm_gain.reshape(1, columns), residual_in,
        ids, fixed, moe_gain.reshape(1, features), down_latent, grow, expert_down, up_latent,
    )


def solution(mesh):
    placed = (
        P(("groups", "ctx"), "heads"),
        P(("groups", "ctx"), "heads"),
        P(("groups", "ctx"), None),
        P(("groups", "ctx"), None),
        P("heads"),
        P(("groups", "ctx"), "heads"),
        P("heads"),
        P("heads", "ctx"),
        P(("groups", "ctx"), "heads"),
        P("heads"),
        P("heads", None),
        P("ctx", None, "heads"),
        P("ctx", "heads", None),
        P(None, "heads"),
        P(("groups", "ctx"), None),
        P(("groups", "ctx"), None),
    )
    return jax.shard_map(
        local, mesh=mesh, in_specs=placed, out_specs=P(("groups", "ctx"), "heads"), check_vma=False
    )
```

```python
import functools

import jax
import jax.numpy as jnp
from jax import lax
from jax.experimental import pallas as pl
from jax.experimental.pallas import tpu as pltpu
from jax.sharding import PartitionSpec as P

GRP = 1024
CAP = 16
LENT_NUM, LENT_DEN = 1, 2
WAVES = 4


epsilon = 1e-05


MESH = pl.DeviceIdType.MESH
BF = jnp.bfloat16
F32 = jnp.float32


def vmem(count=1):
    return [pl.BlockSpec(memory_space=pltpu.VMEM)] * count


def greet(device):
    pl.semaphore_signal(
        pltpu.get_barrier_semaphore(), inc=1, device_id=device, device_id_type=MESH
    )


def greeted(count):
    pl.semaphore_wait(pltpu.get_barrier_semaphore(), count)


def remote(src, dst, send, recv, device):
    return pltpu.make_async_remote_copy(
        src_ref=src, dst_ref=dst, send_sem=send, recv_sem=recv, device_id=device, device_id_type=MESH
    )


def pair_wide(first, second, width):
    lane = lax.broadcasted_iota(jnp.int32, (first.shape[0], 2 * width), 1)
    return jnp.where(lane < width, first, second)


def layer_kernel(
    n, heads, groups, width, piece, lag, lent, waves,
    x_hbm, write_hbm, read_hbm, decay_hbm, skip_hbm, weight_hbm, gate_hbm, gain_hbm, resid_hbm,
    ids_hbm, fixed_hbm, moe_hbm, latent_hbm, grow_hbm, shrink_hbm, lift_hbm,
    out_ref,
    x_ref, write_ref, read_ref, decay_ref, skip_ref, weight_ref, gate_ref, gain_ref, resid_ref,
    ids_ref, fixed_ref, moe_ref, latent_ref, grow_ref, shrink_ref, lift_ref,
    cum, cum_rows, skips, inter,
    mixed, state, ends, prior, outgoing, gated,
    kept, rest, acc, parts, core_in, chip_out, x_in, fin_out, final, borrowed, strips,
    residual, chosen, weights, placed, table, square_out, square_in,
    slots_out, slots_in, middle, gathered, back_out, back_in, back_middle, returned,
    load_sem, chain_send, chain_recv, up_send, up_recv, down_send, down_recv,
    up_rest_send, up_rest_recv, down_rest_send, down_rest_recv,
    core_send, core_recv, x_send, x_recv, fin_send, fin_recv, lend_send, lend_recv, spread_send, spread_recv, strip_recv,
    square_send, square_recv, first_send, first_recv, second_send, second_recv,
    third_send, third_recv, fourth_send, fourth_recv, fifth_send, fifth_recv, sixth_send, sixth_recv,
):
    me, head, group = lax.axis_index("ctx"), lax.axis_index("heads"), lax.axis_index("groups")
    rows, columns = x_ref.shape
    span = 2 * width
    pairs = columns // span
    head_count = decay_ref.shape[0]
    out_width = weight_ref.shape[1]
    count = columns // piece
    share = n // heads
    cores = 2
    chips = heads // cores
    core, chip = head % cores, head // cores
    half, band_rows = out_width // cores, rows // waves
    strip = band_rows // chips
    has_prev, has_next = me > 0, me < n - 1
    prev, after = jnp.maximum(me - 1, 0), jnp.minimum(me + 1, n - 1)
    keep = count - lent
    keep_width = keep * piece
    at_end = jnp.logical_or(me == 0, me == n - 1)
    beside = jnp.logical_or(me == 1, me == n - 2)
    end_here = jnp.where(me == 1, 0, n - 1)
    beside_here = jnp.where(me == 0, 1, n - 2)

    loads = [
        pltpu.make_async_copy(src, dst, load_sem.at[i])
        for i, (src, dst) in enumerate(
            [
                (x_hbm, x_ref), (write_hbm, write_ref), (read_hbm, read_ref), (decay_hbm, decay_ref),
                (skip_hbm, skip_ref), (weight_hbm, weight_ref), (gate_hbm, gate_ref),
                (gain_hbm, gain_ref), (resid_hbm, resid_ref),
                (ids_hbm, ids_ref), (fixed_hbm, fixed_ref), (moe_hbm, moe_ref),
                (latent_hbm, latent_ref), (grow_hbm, grow_ref), (shrink_hbm, shrink_ref),
                (lift_hbm, lift_ref),
            ]
        )
    ]
    for load in loads[:8]:
        load.start()
    for i in range(n):
        for j in range(heads):
            if i or j:
                greet({"ctx": (me + i) % n, "heads": (head + j) % heads})
    for i in range(1, groups):
        greet({"groups": (group + i) % groups})

    t = lax.broadcasted_iota(jnp.int32, (rows, rows), 0)
    s = lax.broadcasted_iota(jnp.int32, (rows, rows), 1)
    lower = jnp.where(t >= s, 1.0, 0.0)
    cum[...] = jnp.zeros(cum.shape, F32)
    for load in loads[:5]:
        load.wait()
    cum[:, :head_count] = lax.dot_general(
        lower, decay_ref[...], (((1,), (1,)), ((), ())),
        precision=lax.Precision.HIGHEST, preferred_element_type=F32,
    )
    cum_rows[...] = lax.dot_general(
        decay_ref[...], lower, (((1,), (1,)), ((), ())),
        precision=lax.Precision.HIGHEST, preferred_element_type=F32,
    )
    skips[...] = jnp.zeros(skips.shape, F32)
    skips[0:1, :head_count] = skip_ref[...]
    product = lax.dot_general(
        read_ref[...], write_ref[...], (((1,), (1,)), ((), ())), preferred_element_type=F32
    )
    inter[...] = jnp.where(t >= s, product, 0.0)
    greeted(n * heads + groups - 2)

    for load in loads[8:]:
        load.start()
    share_rows = piece // groups

    def lend(k):
        return remote(
            weight_ref.at[pl.ds((keep + k) * piece + group * share_rows, share_rows)],
            borrowed.at[pl.ds(k * piece + group * share_rows, share_rows)],
            lend_send.at[k], lend_recv.at[k], {"ctx": beside_here},
        )

    def spread(k, i, back=False):
        owner = (group + groups - i) % groups if back else group
        part = borrowed.at[pl.ds(k * piece + owner * share_rows, share_rows)]
        return remote(
            part, part, spread_send.at[k, i], spread_recv.at[k, i],
            {"groups": (group + i) % groups},
        )

    @pl.when(me == n - 1)
    def _():
        loads[5].wait()
        for k in range(lent):
            lend(k).start()

    def lanes(p):
        return pl.ds(pl.multiple_of(p * span, span), span)

    def shifted(ref, p):
        lane_count = ref.shape[1]
        return pltpu.roll(ref[...], (lane_count - 2 * p) % lane_count, 1)

    band = rows // 2
    causal = lax.broadcasted_iota(jnp.int32, (band, band), 0) >= lax.broadcasted_iota(
        jnp.int32, (band, band), 1
    )

    def scan(p):
        x = x_ref[:, lanes(p)]
        cols = shifted(cum, p)
        skip = shifted(skips, p)
        outs, tails, lasts = [], [], []
        for j in range(2):
            col = cols[:, j : j + 1]
            row = cum_rows[pl.ds(2 * p + j, 1), :]
            last = col[rows - 1 : rows, :]
            lane = x[:, j * width : (j + 1) * width]
            bands = []
            for lo in range(0, rows, band):
                hi = lo + band
                spread = jnp.where(causal, col[lo:hi] - row[:, lo:hi], 0.0)
                if lo:
                    spread = jnp.concatenate([col[lo:hi] - row[:, :lo], spread], axis=1)
                mixing = (jnp.exp(-spread) * inter[lo:hi, :hi]).astype(BF)
                bands.append(jnp.dot(mixing, lane[:hi], preferred_element_type=F32))
            outs.append(jnp.concatenate(bands, axis=0))
            tails.append(jnp.exp(col - last))
            lasts.append(jnp.exp(-last))
        wide = x.astype(F32)
        direct = pair_wide(skip[0:1, 0:1], skip[0:1, 1:2], width) * wide
        mixed[p] = jnp.concatenate(outs, axis=1) + direct
        scaled = (wide * pair_wide(tails[0], tails[1], width)).astype(BF)
        state[p] = lax.dot_general(
            write_ref[...], scaled, (((0,), (0,)), ((), ())), preferred_element_type=F32
        )
        ends[p] = pair_wide(lasts[0], lasts[1], width)

    def chain_copy(q):
        return remote(
            outgoing.at[q], prior.at[q], chain_send.at[q], chain_recv.at[q], {"ctx": after}
        )

    def chain(q):
        @pl.when(me == 0)
        def _():
            prior[q] = jnp.zeros(prior.shape[1:], BF)
            outgoing[q] = state[q].astype(BF)

        @pl.when(has_prev)
        def _():
            chain_copy(q).wait_recv()
            outgoing[q] = (prior[q].astype(F32) * ends[q] + state[q]).astype(BF)

        pl.when(has_next)(lambda: chain_copy(q).start())

    def across(ref, sems, b, r, to):
        spot = ref.at[b, r]
        return remote(spot, spot, sems[0].at[b, r], sems[1].at[b, r], {"ctx": to})

    def upward(b, r):
        return across(kept, (up_send, up_recv), b, r, after)

    def downward(b, r):
        return across(kept, (down_send, down_recv), b, r, prev)

    def upward_rest(b, r):
        return across(rest, (up_rest_send, up_rest_recv), b, r, after)

    def downward_rest(b, r):
        return across(rest, (down_rest_send, down_rest_recv), b, r, prev)

    rest_up = jnp.logical_and(has_next, me + 1 < n - 1)
    rest_down = jnp.logical_and(has_prev, me > 1)
    inner = jnp.logical_not(at_end)

    group_pairs = GRP // span
    loads[6].wait()
    loads[7].wait()

    def gate(g):
        squares = jnp.zeros((rows, span), F32)
        for i in range(group_pairs):
            p = g * group_pairs + i
            cols = shifted(cum, p)
            reach = jnp.exp(-pair_wide(cols[:, 0:1], cols[:, 1:2], width))
            carried = jnp.dot(read_ref[...], prior[p], preferred_element_type=F32) * reach
            gating = gate_ref[:, lanes(p)].astype(F32)
            value = (mixed[p] + carried) * (gating / (1.0 + jnp.exp(-gating)))
            gated[i] = value
            squares = squares + value * value
        scale = lax.rsqrt(jnp.sum(squares, axis=1, keepdims=True) / GRP + epsilon)
        for i in range(group_pairs):
            p = g * group_pairs + i
            value = (gated[i] * scale * gain_ref[:, lanes(p)]).astype(BF)
            ref, lo = (kept, p * span) if p * span < keep_width else (rest, p * span - keep_width)
            for r in range(waves):
                ref[me, r, :, lo : lo + span] = value[r * band_rows : (r + 1) * band_rows]

    early = keep_width // GRP if lent and keep_width % GRP == 0 else 0

    def begin_down():
        for r in range(waves):
            pl.when(has_prev)(lambda: downward(me, r).start())

    def advance(i, carry):
        pl.when(i < pairs)(lambda: scan(i))
        q = i - lag * me
        pl.when(jnp.logical_and(q >= 0, q < pairs))(lambda: chain(q))
        if early:
            @pl.when(i == jnp.maximum(pairs - 1, early * group_pairs - 1 + lag * me))
            def _():
                for g in range(early):
                    gate(g)
                begin_down()

        return carry

    lax.fori_loop(0, pairs + lag * (n - 1), advance, 0)
    pl.when(me < n - 1)(lambda: loads[5].wait())
    for k in range(lent):
        pl.when(me == 0)(lambda: lend(k).start())
    for g in range(early, columns // GRP):
        gate(g)
    if not early:
        begin_down()
    for r in range(waves):
        pl.when(has_next)(lambda: upward(me, r).start())
    if lent:
        for r in range(waves):
            pl.when(rest_up)(lambda: upward_rest(me, r).start())
            pl.when(rest_down)(lambda: downward_rest(me, r).start())

    col_step = min(out_width, 256)

    def multiply(slot, b, r):
        for lo in range(0, out_width, col_step):
            acc[slot, r, :, lo : lo + col_step] = jnp.dot(
                kept[b, r], weight_ref[:keep_width, lo : lo + col_step], preferred_element_type=F32
            )

    def multiply_rest(slot, b, r):
        for lo in range(0, out_width, col_step):
            acc[slot, r, :, lo : lo + col_step] += jnp.dot(
                rest[b, r], weight_ref[keep_width:, lo : lo + col_step], preferred_element_type=F32
            )

    def core_copy(b, r, kind):
        return remote(
            parts.at[kind, b, r, 1 - core], core_in.at[kind, b, r], core_send.at[kind, b, r],
            core_recv.at[kind, b, r], {"heads": head + 1 - 2 * core},
        )

    def round_partial(b, r, slot, kind=0):
        for k in range(cores):
            parts[kind, b, r, k] = acc[slot, r, :, k * half : (k + 1) * half].astype(BF)
        core_copy(b, r, kind).start()

    def chip_copy(b, r, k, kind):
        to = (chip + k) % chips
        return remote(
            chip_out.at[kind, b, r, to], x_in.at[kind, b, r, k], x_send.at[kind, b, r, k],
            x_recv.at[kind, b, r, k], {"heads": to * cores + core},
        )

    def sum_cores(b, r, kind=0):
        core_copy(b, r, kind).wait_recv()
        for k in range(chips):
            part = slice(k * strip, (k + 1) * strip)
            both = parts[kind, b, r, core, part].astype(F32) + core_in[kind, b, r, part].astype(F32)
            chip_out[kind, b, r, k] = both.astype(BF)
        for k in range(1, chips):
            chip_copy(b, r, k, kind).start()

    def local_final(b, column):
        return jnp.logical_and(b == me, head == column // share)

    def final_copy(b, r, column, kind):
        return remote(
            fin_out.at[kind, b, r], final.at[column % share, head, r], fin_send.at[kind, b, r],
            fin_recv.at[column % share, head, r], {"ctx": b, "heads": column // share},
        )

    def strip_copy(b, r):
        return remote(
            fin_out.at[0, b, r], strips.at[b, r], fin_send.at[0, b, r], strip_recv.at[b, r],
            {"ctx": beside_here},
        )

    def to_beside(b):
        if not lent:
            return False
        return jnp.logical_and(at_end, b != me)

    def strip_total(b, r, kind):
        part = pl.ds(pl.multiple_of(chip * strip, strip), strip)
        total = parts[kind, b, r, core, part].astype(F32) + core_in[kind, b, r, part].astype(F32)
        for k in range(1, chips):
            chip_copy(b, r, k, kind).wait_recv()
            total = total + x_in[kind, b, r, k].astype(F32)
        return total

    def deliver(b, r, column, kind, total):
        @pl.when(local_final(b, column))
        def _():
            final[column % share, head, r] = total.astype(BF)

        pl.when(jnp.logical_not(local_final(b, column)))(
            lambda: final_copy(b, r, column, kind).start()
        )

    def sum_chips(b, r):
        total = strip_total(b, r, 0)
        fin_out[0, b, r] = total.astype(BF)
        if lent:
            pl.when(to_beside(b))(lambda: strip_copy(b, r).start())
            pl.when(jnp.logical_not(to_beside(b)))(lambda: deliver(b, r, me, 0, total))
        else:
            deliver(b, r, me, 0, total)

    def helps(b):
        return jnp.logical_and(beside, b != end_here)

    def helping(b, r):
        @pl.when(helps(b))
        def _():
            for lo in range(0, out_width, col_step):
                acc[2, r, :, lo : lo + col_step] = jnp.dot(
                    rest[b, r], borrowed[:, lo : lo + col_step], preferred_element_type=F32
                )
            round_partial(b, r, 2, 1)

    def reduce_help(b, r):
        pl.when(helps(b))(lambda: sum_cores(b, r, 1))

    def combine(b, r):
        @pl.when(helps(b))
        def _():
            strip_copy(b, r).wait_recv()
            total = strip_total(b, r, 1) + strips[b, r].astype(F32)
            fin_out[1, b, r] = total.astype(BF)
            deliver(b, r, end_here, 1, total)

    def own(r, carry):
        multiply(0, me, r)
        if lent:
            multiply_rest(0, me, r)
        round_partial(me, r, 0)
        return carry

    lax.fori_loop(0, waves, own, 0)

    loads[9].wait()
    loads[10].wait()
    wave = chosen.shape[0]
    for e in range(wave):
        named = ids_ref[...] == e
        chosen[e : e + 1, :] = jnp.sum(jnp.where(named, 1.0, 0.0), axis=0, keepdims=True)
        weights[e : e + 1, :] = jnp.sum(jnp.where(named, fixed_ref[...], 0), axis=0, keepdims=True)
    upto = jnp.where(t <= s, 1.0, 0.0).astype(BF)
    taken = jnp.dot(chosen[...].astype(BF), upto, preferred_element_type=F32)
    slot = lax.broadcasted_iota(jnp.int32, (CAP, rows), 0).astype(F32) + 1.0
    for e in range(wave):
        here = jnp.logical_and(chosen[e : e + 1, :] > 0.5, taken[e : e + 1, :] == slot)
        weight = weights[e : e + 1, :].astype(F32) / 65536.0
        base = (e % grow_ref.shape[0] * n + e // grow_ref.shape[0]) * CAP
        part = slice(base, base + CAP)
        placed[part] = jnp.where(here, 1.0, 0.0).astype(BF)
        table[part] = jnp.where(here, weight, 0.0).astype(BF)

    held_back = jnp.where(me == 1, 1, 0) if lent else 0

    def low_block(s):
        low = me - s + jnp.where(s > 0, held_back, 0)
        return jnp.where(jnp.logical_and(s > 0, low >= me), -1, low)

    def around(s, act):
        low, high = low_block(s), me + s
        pl.when(low >= 0)(lambda: act(jnp.maximum(low, 0), 0))

        @pl.when(jnp.logical_and(high < n, s > 0))
        def _():
            act(jnp.minimum(high, n - 1), 1)

    turns = 2 * waves
    ripe = jnp.where(at_end, 0, waves) if lent else 0

    def finished(i, act):
        s, r = i // turns, i % turns - ripe
        fits = jnp.logical_and(jnp.logical_and(r >= 0, r < waves), s > 0)
        spot = jnp.maximum(jnp.minimum(r, waves - 1), 0)
        pl.when(fits)(lambda: around(s, lambda b, slot: act(b, spot, slot)))

    def pass_on(k):
        lend(k).wait_recv()
        for g in range(1, groups):
            spread(k, g).start()

    for r in range(waves):
        sum_cores(me, r)
    for r in range(waves):
        sum_chips(me, r)
    for k in range(lent):
        pl.when(me == n - 2)(lambda: pass_on(k))
    first_help = 2 * turns + waves

    def step(i, carry):
        s, u = i // turns, i % turns
        low, high = low_block(s), me + s
        low_spot, high_spot = jnp.maximum(low, 0), jnp.minimum(high, n - 1)
        has_low, has_high = low >= 0, high < n

        @pl.when(u < waves)
        def _():
            r = jnp.minimum(u, waves - 1)

            @pl.when(has_low)
            def _():
                upward(low_spot, r).wait_recv()
                pl.when(has_next)(lambda: upward(low_spot, r).start())

            @pl.when(has_high)
            def _():
                downward(high_spot, r).wait_recv()
                pl.when(has_prev)(lambda: downward(high_spot, r).start())

            around(s, lambda b, slot: multiply(slot, b, r))

        if lent:
            @pl.when(jnp.logical_and(u >= waves, inner))
            def _():
                r = jnp.maximum(u - waves, 0)

                @pl.when(has_low)
                def _():
                    upward_rest(low_spot, r).wait_recv()
                    pl.when(rest_up)(lambda: upward_rest(low_spot, r).start())

                @pl.when(has_high)
                def _():
                    downward_rest(high_spot, r).wait_recv()
                    pl.when(rest_down)(lambda: downward_rest(high_spot, r).start())

                around(s, lambda b, slot: multiply_rest(slot, b, r))

        finished(i, lambda b, r, slot: round_partial(b, r, slot))
        finished(i - 1, lambda b, r, slot: sum_cores(b, r))
        finished(i - 3, lambda b, r, slot: sum_chips(b, r))
        for k in range(lent):
            when = min(turns + waves + (k + 1) * waves // lent, 2 * turns)
            pl.when(jnp.logical_and(i == when, me == 1))(lambda: pass_on(k))
        if lent:
            def early_help(spot, act):
                r = jnp.maximum(jnp.minimum(i - spot, waves - 1), 0)

                @pl.when(jnp.logical_and(i >= spot, i < spot + waves))
                def _():
                    for base in range(2):
                        around(base, lambda b, slot: act(b, r))

            @pl.when(jnp.logical_and(i == first_help, beside))
            def _():
                for k in range(lent):
                    for g in range(1, groups):
                        spread(k, g, True).wait_recv()

            early_help(first_help, helping)
            early_help(first_help + 1, reduce_help)
            early_help(first_help + 4, combine)

            def later(back, act):
                pl.when(i - back >= 2 * turns)(
                    lambda: finished(i - back, lambda b, r, slot: act(b, r))
                )

            later(1, helping)
            later(2, reduce_help)
            later(4, combine)
        return carry

    lax.fori_loop(turns, n * turns + 4, step, 0)
    loads[8].wait()

    for j in range(share):
        source = head * share + j
        if lent:
            outer = jnp.logical_and(source != me, jnp.logical_or(source == 0, source == n - 1))
            source = jnp.where(outer, jnp.where(source == 0, 1, n - 2), source)
        for k in range(heads):
            here = jnp.logical_and(source == me, k == head)

            for r in range(waves):
                @pl.when(jnp.logical_not(here))
                def _():
                    remote(
                        fin_out.at[0, 0, r], final.at[j, k, r], fin_send.at[0, 0, r],
                        fin_recv.at[j, k, r], {"ctx": source, "heads": k},
                    ).wait_recv()

                base = r * band_rows + (k // cores) * strip
                part = slice(base, base + strip)
                lo = j * out_width + (k % cores) * half
                residual[part, lo : lo + half] = (
                    resid_ref[part, lo : lo + half].astype(F32) + final[j, k, r].astype(F32)
                )

    for load in loads[11:]:
        load.wait()
    latent_width = latent_ref.shape[1]
    strand = latent_width // heads
    features = residual.shape[1] * heads
    experts_here = grow_ref.shape[0]
    slot_rows = n * CAP
    held = residual[...]
    scaled = (held * moe_ref[...]).astype(BF)
    picked = jnp.dot(placed[...], scaled, preferred_element_type=F32).astype(BF)

    def square_copy(k):
        return remote(
            square_out, square_in.at[k], square_send.at[k], square_recv.at[k],
            {"heads": (head + k) % heads},
        )

    def first_copy(e, k):
        return remote(
            slots_out.at[e, k], slots_in.at[e, k], first_send.at[e, k], first_recv.at[e, k],
            {"heads": (head + k) % heads},
        )

    def second_copy(e, k):
        to = (me + k) % n
        return remote(
            middle.at[e, to], gathered.at[e, head, me], second_send.at[e, k],
            second_recv.at[e, k], {"ctx": to},
        )

    def third_copy(e, j):
        spot = gathered.at[e, head]
        return remote(
            spot, spot, third_send.at[e, j], third_recv.at[e, j], {"heads": (head + j) % heads}
        )

    def fourth_copy(e, k):
        return remote(
            back_out.at[e, (head + k) % heads], back_in.at[e, k], fourth_send.at[e, k],
            fourth_recv.at[e, k], {"heads": (head + k) % heads},
        )

    def fifth_copy(e, k):
        to = (me + k) % n
        return remote(
            back_middle.at[e, to], returned.at[head, e, me], fifth_send.at[e, k],
            fifth_recv.at[e, k], {"ctx": to},
        )

    def sixth_copy(e, j):
        spot = returned.at[head, e]
        return remote(
            spot, spot, sixth_send.at[e, j], sixth_recv.at[e, j], {"heads": (head + j) % heads}
        )

    far = heads // 2
    for e in range(experts_here):
        rows_here = picked[e * slot_rows : (e + 1) * slot_rows]
        for k in [far] + [k for k in range(1, heads) if k != far] + [0]:
            to = (head + k) % heads
            lane = pl.ds(pl.multiple_of(to * strand, strand), strand)
            value = jnp.dot(rows_here, latent_ref[:, lane], preferred_element_type=F32)
            slots_out[e, k] = value.astype(BF).reshape(n, CAP, strand)
            if k:
                first_copy(e, k).start()
        if e == 0:
            power = jnp.sum(held * held, axis=1, keepdims=True)
            power = jnp.transpose(jnp.broadcast_to(power, (rows, 128)))[:8, :]
            square_out[...] = lax.dot_general(
                power, placed[...].astype(F32), (((1,), (1,)), ((), ())),
                precision=lax.Precision.HIGHEST, preferred_element_type=F32,
            )
            for k in range(1, heads):
                square_copy(k).start()

    power = square_out[...]
    for k in range(1, heads):
        square_copy(k).wait_recv()
        power = power + square_in[k]
    scale = lax.rsqrt(power / features + epsilon)
    scale = jnp.transpose(jnp.broadcast_to(scale[0:1, :], (128, scale.shape[1])))
    for e in range(experts_here):
        for k in range(1, heads):
            first_copy(e, k).wait_recv()
        for z in range(n):
            total = slots_out[e, 0, z].astype(F32)
            for k in range(1, heads):
                total = total + slots_in[e, k, z].astype(F32)
            base = e * slot_rows + z * CAP
            middle[e, z] = (total * scale[base : base + CAP, 0:1]).astype(BF)
        for k in range(1, n):
            second_copy(e, k).start()
        gathered[e, head, me] = middle[e, me]
    for e in range(experts_here):
        for k in range(1, n):
            second_copy(e, k).wait_recv()
        for j in range(1, heads):
            third_copy(e, j).start()
    for e in range(experts_here):
        for j in range(1, heads):
            third_copy(e, j).wait_recv()
        fed = jnp.concatenate(
            [gathered[e, h].reshape(slot_rows, strand) for h in range(heads)], axis=1
        )
        hidden = lax.dot_general(
            fed, grow_ref[e], (((1,), (1,)), ((), ())), preferred_element_type=F32
        )
        hidden = (jnp.maximum(hidden, 0.0) ** 2).astype(BF)
        value = jnp.dot(hidden, shrink_ref[e], preferred_element_type=F32).astype(BF)
        for h in range(heads):
            back_out[e, h] = value[:, h * strand : (h + 1) * strand].reshape(n, CAP, strand)
        for k in range(1, heads):
            fourth_copy(e, k).start()
    for e in range(experts_here):
        for k in range(1, heads):
            fourth_copy(e, k).wait_recv()
        total = back_out[e, head].astype(F32)
        for k in range(1, heads):
            total = total + back_in[e, k].astype(F32)
        back_middle[e] = total.astype(BF)
        for k in range(1, n):
            fifth_copy(e, k).start()
        returned[head, e, me] = back_middle[e, me]
    for e in range(experts_here):
        for k in range(1, n):
            fifth_copy(e, k).wait_recv()
        for j in range(1, heads):
            sixth_copy(e, j).start()
    for e in range(experts_here):
        for j in range(1, heads):
            sixth_copy(e, j).wait_recv()
    combined = jnp.concatenate(
        [
            lax.dot_general(
                table[...], returned[h].reshape(wave * CAP, strand), (((0,), (0,)), ((), ())),
                preferred_element_type=F32,
            ).astype(BF)
            for h in range(heads)
        ],
        axis=1,
    )
    lift_step = min(256, residual.shape[1])
    for lo in range(0, residual.shape[1], lift_step):
        part = slice(lo, lo + lift_step)
        value = jnp.dot(combined, lift_ref[:, part], preferred_element_type=F32)
        out_ref[:, part] = (residual[:, part] + value).astype(BF)

    for k in range(1, heads):
        square_copy(k).wait_send()
    for e in range(experts_here):
        for k in range(1, heads):
            first_copy(e, k).wait_send()
            third_copy(e, k).wait_send()
            fourth_copy(e, k).wait_send()
            sixth_copy(e, k).wait_send()
        for k in range(1, n):
            second_copy(e, k).wait_send()
            fifth_copy(e, k).wait_send()
    for q in range(pairs):
        pl.when(has_next)(lambda: chain_copy(q).wait_send())
    for b in range(n):
        sent = jnp.logical_or(to_beside(b), jnp.logical_not(local_final(b, me)))
        for r in range(waves):
            pl.when(jnp.logical_and(has_next, b <= me))(lambda: upward(b, r).wait_send())
            pl.when(jnp.logical_and(has_prev, b >= me))(lambda: downward(b, r).wait_send())
            core_copy(b, r, 0).wait_send()
            for k in range(1, chips):
                chip_copy(b, r, k, 0).wait_send()
            pl.when(sent)(lambda: final_copy(b, r, me, 0).wait_send())
            if lent:
                pl.when(jnp.logical_and(rest_up, b <= me))(lambda: upward_rest(b, r).wait_send())
                pl.when(jnp.logical_and(rest_down, b >= me))(
                    lambda: downward_rest(b, r).wait_send()
                )

                @pl.when(helps(b))
                def _():
                    core_copy(b, r, 1).wait_send()
                    for k in range(1, chips):
                        chip_copy(b, r, k, 1).wait_send()
                    pl.when(jnp.logical_not(local_final(b, end_here)))(
                        lambda: final_copy(b, r, end_here, 1).wait_send()
                    )

    for k in range(lent):
        pl.when(at_end)(lambda: lend(k).wait_send())
        for g in range(1, groups):
            pl.when(beside)(lambda: spread(k, g).wait_send())


def reaching(collective_id, grant=48 * 1024 * 1024):
    return pltpu.CompilerParams(
        collective_id=collective_id, has_side_effects=True, vmem_limit_bytes=grant
    )


def dma(*shape):
    return pltpu.SemaphoreType.DMA(shape)


def local(
    ssm_input,
    decay_log,
    state_write,
    state_read,
    skip_scale,
    gate_input,
    ssm_gain,
    weight,
    residual_in,
    moe_gain,
    down_latent,
    expert_up,
    expert_down,
    up_latent,
    expert_ids,
    combine_fixed,
):
    n, heads, groups = lax.axis_size("ctx"), lax.axis_size("heads"), lax.axis_size("groups")
    rows, columns = ssm_input.shape
    head_count = decay_log.shape[1]
    width = columns // head_count
    states = state_write.shape[1]
    span = 2 * width
    pairs = columns // span
    piece = GRP // 4
    count = columns // piece
    lent = LENT_NUM * count // LENT_DEN if n > 3 else 0
    out_width = weight.shape[1]
    share = n // heads
    chips = heads // 2
    half, band_rows = out_width // 2, rows // WAVES
    strip = band_rows // chips
    keep_width, rest_width = (count - lent) * piece, max(lent, 1) * piece
    lane_count = -(-head_count // 128) * 128
    features = residual_in.shape[1]
    experts_here = expert_up.shape[0]
    wave = experts_here * n
    strand = down_latent.shape[1] // heads
    grow = expert_up.transpose(0, 2, 1)
    ids, fixed = expert_ids.T, combine_fixed.T
    anywhere = pl.BlockSpec(memory_space=pltpu.HBM)
    return pl.pallas_call(
        functools.partial(layer_kernel, n, heads, groups, width, piece, 4, lent, WAVES),
        out_shape=jax.ShapeDtypeStruct((rows, features), BF),
        in_specs=[anywhere] * 16,
        out_specs=vmem()[0],
        scratch_shapes=[
            pltpu.VMEM((rows, columns), BF),
            pltpu.VMEM((rows, states), BF),
            pltpu.VMEM((rows, states), BF),
            pltpu.VMEM((head_count, rows), F32),
            pltpu.VMEM((1, head_count), F32),
            pltpu.VMEM(weight.shape, BF),
            pltpu.VMEM((rows, columns), BF),
            pltpu.VMEM((1, columns), F32),
            pltpu.VMEM(residual_in.shape, BF),
            pltpu.VMEM(ids.shape, jnp.int32),
            pltpu.VMEM(fixed.shape, jnp.int32),
            pltpu.VMEM((1, features), F32),
            pltpu.VMEM(down_latent.shape, BF),
            pltpu.VMEM(grow.shape, BF),
            pltpu.VMEM(expert_down.shape, BF),
            pltpu.VMEM(up_latent.shape, BF),
            pltpu.VMEM((rows, lane_count), F32),
            pltpu.VMEM((head_count, rows), F32),
            pltpu.VMEM((8, lane_count), F32),
            pltpu.VMEM((rows, rows), F32),
            pltpu.VMEM((pairs, rows, span), F32),
            pltpu.VMEM((pairs, states, span), F32),
            pltpu.VMEM((pairs, 1, span), F32),
            pltpu.VMEM((pairs, states, span), BF),
            pltpu.VMEM((pairs, states, span), BF),
            pltpu.VMEM((GRP // span, rows, span), F32),
            pltpu.VMEM((n, WAVES, band_rows, keep_width), BF),
            pltpu.VMEM((n, WAVES, band_rows, rest_width), BF),
            pltpu.VMEM((3, WAVES, band_rows, out_width), F32),
            pltpu.VMEM((2, n, WAVES, 2, band_rows, half), BF),
            pltpu.VMEM((2, n, WAVES, band_rows, half), BF),
            pltpu.VMEM((2, n, WAVES, chips, strip, half), BF),
            pltpu.VMEM((2, n, WAVES, chips, strip, half), BF),
            pltpu.VMEM((2, n, WAVES, strip, half), BF),
            pltpu.VMEM((share, heads, WAVES, strip, half), BF),
            pltpu.VMEM((rest_width, out_width), BF),
            pltpu.VMEM((n, WAVES, strip, half), BF),
            pltpu.VMEM((rows, features), F32),
            pltpu.VMEM((wave, rows), F32),
            pltpu.VMEM((wave, rows), jnp.int32),
            pltpu.VMEM((wave * CAP, rows), BF),
            pltpu.VMEM((wave * CAP, rows), BF),
            pltpu.VMEM((8, wave * CAP), F32),
            pltpu.VMEM((heads, 8, wave * CAP), F32),
            pltpu.VMEM((experts_here, heads, n, CAP, strand), BF),
            pltpu.VMEM((experts_here, heads, n, CAP, strand), BF),
            pltpu.VMEM((experts_here, n, CAP, strand), BF),
            pltpu.VMEM((experts_here, heads, n, CAP, strand), BF),
            pltpu.VMEM((experts_here, heads, n, CAP, strand), BF),
            pltpu.VMEM((experts_here, heads, n, CAP, strand), BF),
            pltpu.VMEM((experts_here, n, CAP, strand), BF),
            pltpu.VMEM((heads, experts_here, n, CAP, strand), BF),
            dma(16), dma(pairs), dma(pairs),
            *[dma(n, WAVES)] * 8,
            dma(2, n, WAVES), dma(2, n, WAVES), dma(2, n, WAVES, chips), dma(2, n, WAVES, chips),
            dma(2, n, WAVES), dma(share, heads, WAVES),
            dma(max(lent, 1)), dma(max(lent, 1)), dma(max(lent, 1), groups), dma(max(lent, 1), groups), dma(n, WAVES),
            dma(heads), dma(heads),
            *[dma(experts_here, heads)] * 2, *[dma(experts_here, n)] * 2,
            *[dma(experts_here, heads)] * 4,
            *[dma(experts_here, n)] * 2, *[dma(experts_here, heads)] * 2,
        ],
        compiler_params=reaching(1, 67043328),
    )(
        ssm_input, state_write, state_read, decay_log.T, skip_scale.reshape(1, head_count), weight,
        gate_input, ssm_gain.reshape(1, columns), residual_in,
        ids, fixed, moe_gain.reshape(1, features), down_latent, grow, expert_down, up_latent,
    )


def solution(mesh):
    placed = (
        P(("groups", "ctx"), "heads"),
        P(("groups", "ctx"), "heads"),
        P(("groups", "ctx"), None),
        P(("groups", "ctx"), None),
        P("heads"),
        P(("groups", "ctx"), "heads"),
        P("heads"),
        P("heads", "ctx"),
        P(("groups", "ctx"), "heads"),
        P("heads"),
        P("heads", None),
        P("ctx", None, "heads"),
        P("ctx", "heads", None),
        P(None, "heads"),
        P(("groups", "ctx"), None),
        P(("groups", "ctx"), None),
    )
    return jax.shard_map(
        local, mesh=mesh, in_specs=placed, out_specs=P(("groups", "ctx"), "heads"), check_vma=False
    )
```

```python
import functools

import jax
import jax.numpy as jnp
from jax import lax
from jax.experimental import pallas as pl
from jax.experimental.pallas import tpu as pltpu
from jax.sharding import PartitionSpec as P

GRP = 1024
CAP = 16
LENT_NUM, LENT_DEN = 1, 2
WAVES = 4


epsilon = 1e-05


MESH = pl.DeviceIdType.MESH
BF = jnp.bfloat16
F32 = jnp.float32


def vmem(count=1):
    return [pl.BlockSpec(memory_space=pltpu.VMEM)] * count


def greet(device):
    pl.semaphore_signal(
        pltpu.get_barrier_semaphore(), inc=1, device_id=device, device_id_type=MESH
    )


def greeted(count):
    pl.semaphore_wait(pltpu.get_barrier_semaphore(), count)


def remote(src, dst, send, recv, device):
    return pltpu.make_async_remote_copy(
        src_ref=src, dst_ref=dst, send_sem=send, recv_sem=recv, device_id=device, device_id_type=MESH
    )


def pair_wide(first, second, width):
    lane = lax.broadcasted_iota(jnp.int32, (first.shape[0], 2 * width), 1)
    return jnp.where(lane < width, first, second)


def layer_kernel(
    n, heads, groups, width, piece, lag, lent, waves,
    x_hbm, write_hbm, read_hbm, decay_hbm, skip_hbm, weight_hbm, gate_hbm, gain_hbm, resid_hbm,
    ids_hbm, fixed_hbm, moe_hbm, latent_hbm, grow_hbm, shrink_hbm, lift_hbm,
    out_ref,
    x_ref, write_ref, read_ref, decay_ref, skip_ref, weight_ref, gate_ref, gain_ref, resid_ref,
    ids_ref, fixed_ref, moe_ref, latent_ref, grow_ref, shrink_ref, lift_ref,
    cum, cum_rows, skips, inter,
    mixed, state, ends, prior, outgoing, gated,
    kept, rest, acc, parts, core_in, chip_out, x_in, fin_out, final, borrowed, strips,
    residual, chosen, weights, placed, table, square_out, square_in,
    slots_out, slots_in, middle, gathered, back_out, back_in, back_middle, returned,
    load_sem, chain_send, chain_recv, up_send, up_recv, down_send, down_recv,
    up_rest_send, up_rest_recv, down_rest_send, down_rest_recv,
    core_send, core_recv, x_send, x_recv, fin_send, fin_recv, lend_send, lend_recv, spread_send, spread_recv, strip_recv,
    square_send, square_recv, first_send, first_recv, second_send, second_recv,
    third_send, third_recv, fourth_send, fourth_recv, fifth_send, fifth_recv, sixth_send, sixth_recv,
):
    me, head, group = lax.axis_index("ctx"), lax.axis_index("heads"), lax.axis_index("groups")
    rows, columns = x_ref.shape
    span = 2 * width
    pairs = columns // span
    head_count = decay_ref.shape[0]
    out_width = weight_ref.shape[1]
    count = columns // piece
    share = n // heads
    cores = 2
    chips = heads // cores
    core, chip = head % cores, head // cores
    half, band_rows = out_width // cores, rows // waves
    strip = band_rows // chips
    has_prev, has_next = me > 0, me < n - 1
    prev, after = jnp.maximum(me - 1, 0), jnp.minimum(me + 1, n - 1)
    keep = count - lent
    keep_width = keep * piece
    at_end = jnp.logical_or(me == 0, me == n - 1)
    beside = jnp.logical_or(me == 1, me == n - 2)
    end_here = jnp.where(me == 1, 0, n - 1)
    beside_here = jnp.where(me == 0, 1, n - 2)

    loads = [
        pltpu.make_async_copy(src, dst, load_sem.at[i])
        for i, (src, dst) in enumerate(
            [
                (x_hbm, x_ref), (write_hbm, write_ref), (read_hbm, read_ref), (decay_hbm, decay_ref),
                (skip_hbm, skip_ref), (weight_hbm, weight_ref), (gate_hbm, gate_ref),
                (gain_hbm, gain_ref), (resid_hbm, resid_ref),
                (ids_hbm, ids_ref), (fixed_hbm, fixed_ref), (moe_hbm, moe_ref),
                (latent_hbm, latent_ref), (grow_hbm, grow_ref), (shrink_hbm, shrink_ref),
                (lift_hbm, lift_ref),
            ]
        )
    ]
    for load in loads[:8]:
        load.start()
    for i in range(n):
        for j in range(heads):
            if i or j:
                greet({"ctx": (me + i) % n, "heads": (head + j) % heads})
    for i in range(1, groups):
        greet({"groups": (group + i) % groups})

    t = lax.broadcasted_iota(jnp.int32, (rows, rows), 0)
    s = lax.broadcasted_iota(jnp.int32, (rows, rows), 1)
    lower = jnp.where(t >= s, 1.0, 0.0)
    cum[...] = jnp.zeros(cum.shape, F32)
    for load in loads[:5]:
        load.wait()
    cum[:, :head_count] = lax.dot_general(
        lower, decay_ref[...], (((1,), (1,)), ((), ())),
        precision=lax.Precision.HIGHEST, preferred_element_type=F32,
    )
    cum_rows[...] = lax.dot_general(
        decay_ref[...], lower, (((1,), (1,)), ((), ())),
        precision=lax.Precision.HIGHEST, preferred_element_type=F32,
    )
    skips[...] = jnp.zeros(skips.shape, F32)
    skips[0:1, :head_count] = skip_ref[...]
    product = lax.dot_general(
        read_ref[...], write_ref[...], (((1,), (1,)), ((), ())), preferred_element_type=F32
    )
    inter[...] = jnp.where(t >= s, product, 0.0)
    greeted(n * heads + groups - 2)

    for load in loads[8:]:
        load.start()
    share_rows = piece // groups

    def lend(k):
        return remote(
            weight_ref.at[pl.ds((keep + k) * piece + group * share_rows, share_rows)],
            borrowed.at[pl.ds(k * piece + group * share_rows, share_rows)],
            lend_send.at[k], lend_recv.at[k], {"ctx": beside_here},
        )

    def spread(k, i, back=False):
        owner = (group + groups - i) % groups if back else group
        part = borrowed.at[pl.ds(k * piece + owner * share_rows, share_rows)]
        return remote(
            part, part, spread_send.at[k, i], spread_recv.at[k, i],
            {"groups": (group + i) % groups},
        )

    @pl.when(me == n - 1)
    def _():
        loads[5].wait()
        for k in range(lent):
            lend(k).start()

    def lanes(p):
        return pl.ds(pl.multiple_of(p * span, span), span)

    def shifted(ref, p):
        lane_count = ref.shape[1]
        return pltpu.roll(ref[...], (lane_count - 2 * p) % lane_count, 1)

    band = rows // 2
    causal = lax.broadcasted_iota(jnp.int32, (band, band), 0) >= lax.broadcasted_iota(
        jnp.int32, (band, band), 1
    )

    def scan(p):
        x = x_ref[:, lanes(p)]
        cols = shifted(cum, p)
        skip = shifted(skips, p)
        outs, tails, lasts = [], [], []
        for j in range(2):
            col = cols[:, j : j + 1]
            row = cum_rows[pl.ds(2 * p + j, 1), :]
            last = col[rows - 1 : rows, :]
            lane = x[:, j * width : (j + 1) * width]
            bands = []
            for lo in range(0, rows, band):
                hi = lo + band
                spread = jnp.where(causal, col[lo:hi] - row[:, lo:hi], 0.0)
                if lo:
                    spread = jnp.concatenate([col[lo:hi] - row[:, :lo], spread], axis=1)
                mixing = (jnp.exp(-spread) * inter[lo:hi, :hi]).astype(BF)
                bands.append(jnp.dot(mixing, lane[:hi], preferred_element_type=F32))
            outs.append(jnp.concatenate(bands, axis=0))
            tails.append(jnp.exp(col - last))
            lasts.append(jnp.exp(-last))
        wide = x.astype(F32)
        direct = pair_wide(skip[0:1, 0:1], skip[0:1, 1:2], width) * wide
        mixed[p] = jnp.concatenate(outs, axis=1) + direct
        scaled = (wide * pair_wide(tails[0], tails[1], width)).astype(BF)
        state[p] = lax.dot_general(
            write_ref[...], scaled, (((0,), (0,)), ((), ())), preferred_element_type=F32
        )
        ends[p] = pair_wide(lasts[0], lasts[1], width)

    def chain_copy(q):
        return remote(
            outgoing.at[q], prior.at[q], chain_send.at[q], chain_recv.at[q], {"ctx": after}
        )

    def chain(q):
        @pl.when(me == 0)
        def _():
            prior[q] = jnp.zeros(prior.shape[1:], BF)
            outgoing[q] = state[q].astype(BF)

        @pl.when(has_prev)
        def _():
            chain_copy(q).wait_recv()
            outgoing[q] = (prior[q].astype(F32) * ends[q] + state[q]).astype(BF)

        pl.when(has_next)(lambda: chain_copy(q).start())

    def across(ref, sems, b, r, to):
        spot = ref.at[b, r]
        return remote(spot, spot, sems[0].at[b, r], sems[1].at[b, r], {"ctx": to})

    def upward(b, r):
        return across(kept, (up_send, up_recv), b, r, after)

    def downward(b, r):
        return across(kept, (down_send, down_recv), b, r, prev)

    def upward_rest(b, r):
        return across(rest, (up_rest_send, up_rest_recv), b, r, after)

    def downward_rest(b, r):
        return across(rest, (down_rest_send, down_rest_recv), b, r, prev)

    rest_up = jnp.logical_and(has_next, me + 1 < n - 1)
    rest_down = jnp.logical_and(has_prev, me > 1)
    inner = jnp.logical_not(at_end)

    group_pairs = GRP // span
    loads[6].wait()
    loads[7].wait()

    def gate(g):
        squares = jnp.zeros((rows, span), F32)
        for i in range(group_pairs):
            p = g * group_pairs + i
            cols = shifted(cum, p)
            reach = jnp.exp(-pair_wide(cols[:, 0:1], cols[:, 1:2], width))
            carried = jnp.dot(read_ref[...], prior[p], preferred_element_type=F32) * reach
            gating = gate_ref[:, lanes(p)].astype(F32)
            value = (mixed[p] + carried) * (gating / (1.0 + jnp.exp(-gating)))
            gated[i] = value
            squares = squares + value * value
        scale = lax.rsqrt(jnp.sum(squares, axis=1, keepdims=True) / GRP + epsilon)
        for i in range(group_pairs):
            p = g * group_pairs + i
            value = (gated[i] * scale * gain_ref[:, lanes(p)]).astype(BF)
            ref, lo = (kept, p * span) if p * span < keep_width else (rest, p * span - keep_width)
            for r in range(waves):
                ref[me, r, :, lo : lo + span] = value[r * band_rows : (r + 1) * band_rows]

    early = keep_width // GRP if lent and keep_width % GRP == 0 else 0

    def begin_down():
        for r in range(waves):
            pl.when(has_prev)(lambda: downward(me, r).start())

    def advance(i, carry):
        pl.when(i < pairs)(lambda: scan(i))
        q = i - lag * me
        pl.when(jnp.logical_and(q >= 0, q < pairs))(lambda: chain(q))
        if early:
            @pl.when(i == jnp.maximum(pairs - 1, early * group_pairs - 1 + lag * me))
            def _():
                for g in range(early):
                    gate(g)
                begin_down()

        return carry

    lax.fori_loop(0, pairs + lag * (n - 1), advance, 0)
    pl.when(me < n - 1)(lambda: loads[5].wait())
    for k in range(lent):
        pl.when(me == 0)(lambda: lend(k).start())
    def begin_up():
        for r in range(waves):
            pl.when(has_next)(lambda: upward(me, r).start())

    if early:
        begin_up()
    for g in range(early, columns // GRP):
        gate(g)
    if not early:
        begin_down()
        begin_up()
    if lent:
        for r in range(waves):
            pl.when(rest_up)(lambda: upward_rest(me, r).start())
            pl.when(rest_down)(lambda: downward_rest(me, r).start())

    col_step = min(out_width, 256)

    def multiply(slot, b, r):
        for lo in range(0, out_width, col_step):
            acc[slot, r, :, lo : lo + col_step] = jnp.dot(
                kept[b, r], weight_ref[:keep_width, lo : lo + col_step], preferred_element_type=F32
            )

    def multiply_rest(slot, b, r):
        for lo in range(0, out_width, col_step):
            acc[slot, r, :, lo : lo + col_step] += jnp.dot(
                rest[b, r], weight_ref[keep_width:, lo : lo + col_step], preferred_element_type=F32
            )

    def core_copy(b, r, kind):
        return remote(
            parts.at[kind, b, r, 1 - core], core_in.at[kind, b, r], core_send.at[kind, b, r],
            core_recv.at[kind, b, r], {"heads": head + 1 - 2 * core},
        )

    def round_partial(b, r, slot, kind=0):
        for k in range(cores):
            parts[kind, b, r, k] = acc[slot, r, :, k * half : (k + 1) * half].astype(BF)
        core_copy(b, r, kind).start()

    def chip_copy(b, r, k, kind):
        to = (chip + k) % chips
        return remote(
            chip_out.at[kind, b, r, to], x_in.at[kind, b, r, k], x_send.at[kind, b, r, k],
            x_recv.at[kind, b, r, k], {"heads": to * cores + core},
        )

    def sum_cores(b, r, kind=0):
        core_copy(b, r, kind).wait_recv()
        for k in range(chips):
            part = slice(k * strip, (k + 1) * strip)
            both = parts[kind, b, r, core, part].astype(F32) + core_in[kind, b, r, part].astype(F32)
            chip_out[kind, b, r, k] = both.astype(BF)
        for k in range(1, chips):
            chip_copy(b, r, k, kind).start()

    def local_final(b, column):
        return jnp.logical_and(b == me, head == column // share)

    def final_copy(b, r, column, kind):
        return remote(
            fin_out.at[kind, b, r], final.at[column % share, head, r], fin_send.at[kind, b, r],
            fin_recv.at[column % share, head, r], {"ctx": b, "heads": column // share},
        )

    def strip_copy(b, r):
        return remote(
            fin_out.at[0, b, r], strips.at[b, r], fin_send.at[0, b, r], strip_recv.at[b, r],
            {"ctx": beside_here},
        )

    def to_beside(b):
        if not lent:
            return False
        return jnp.logical_and(at_end, b != me)

    def strip_total(b, r, kind):
        part = pl.ds(pl.multiple_of(chip * strip, strip), strip)
        total = parts[kind, b, r, core, part].astype(F32) + core_in[kind, b, r, part].astype(F32)
        for k in range(1, chips):
            chip_copy(b, r, k, kind).wait_recv()
            total = total + x_in[kind, b, r, k].astype(F32)
        return total

    def deliver(b, r, column, kind, total):
        @pl.when(local_final(b, column))
        def _():
            final[column % share, head, r] = total.astype(BF)

        pl.when(jnp.logical_not(local_final(b, column)))(
            lambda: final_copy(b, r, column, kind).start()
        )

    def sum_chips(b, r):
        total = strip_total(b, r, 0)
        fin_out[0, b, r] = total.astype(BF)
        if lent:
            pl.when(to_beside(b))(lambda: strip_copy(b, r).start())
            pl.when(jnp.logical_not(to_beside(b)))(lambda: deliver(b, r, me, 0, total))
        else:
            deliver(b, r, me, 0, total)

    def helps(b):
        return jnp.logical_and(beside, b != end_here)

    def helping(b, r):
        @pl.when(helps(b))
        def _():
            for lo in range(0, out_width, col_step):
                acc[2, r, :, lo : lo + col_step] = jnp.dot(
                    rest[b, r], borrowed[:, lo : lo + col_step], preferred_element_type=F32
                )
            round_partial(b, r, 2, 1)

    def reduce_help(b, r):
        pl.when(helps(b))(lambda: sum_cores(b, r, 1))

    def combine(b, r):
        @pl.when(helps(b))
        def _():
            strip_copy(b, r).wait_recv()
            total = strip_total(b, r, 1) + strips[b, r].astype(F32)
            fin_out[1, b, r] = total.astype(BF)
            deliver(b, r, end_here, 1, total)

    def own(r, carry):
        multiply(0, me, r)
        if lent:
            multiply_rest(0, me, r)
        round_partial(me, r, 0)
        return carry

    lax.fori_loop(0, waves, own, 0)

    loads[9].wait()
    loads[10].wait()
    wave = chosen.shape[0]
    for e in range(wave):
        named = ids_ref[...] == e
        chosen[e : e + 1, :] = jnp.sum(jnp.where(named, 1.0, 0.0), axis=0, keepdims=True)
        weights[e : e + 1, :] = jnp.sum(jnp.where(named, fixed_ref[...], 0), axis=0, keepdims=True)
    upto = jnp.where(t <= s, 1.0, 0.0).astype(BF)
    taken = jnp.dot(chosen[...].astype(BF), upto, preferred_element_type=F32)
    slot = lax.broadcasted_iota(jnp.int32, (CAP, rows), 0).astype(F32) + 1.0
    for e in range(wave):
        here = jnp.logical_and(chosen[e : e + 1, :] > 0.5, taken[e : e + 1, :] == slot)
        weight = weights[e : e + 1, :].astype(F32) / 65536.0
        base = (e % grow_ref.shape[0] * n + e // grow_ref.shape[0]) * CAP
        part = slice(base, base + CAP)
        placed[part] = jnp.where(here, 1.0, 0.0).astype(BF)
        table[part] = jnp.where(here, weight, 0.0).astype(BF)

    held_back = jnp.where(me == 1, 1, 0) if lent else 0

    def low_block(s):
        low = me - s + jnp.where(s > 0, held_back, 0)
        return jnp.where(jnp.logical_and(s > 0, low >= me), -1, low)

    def around(s, act):
        low, high = low_block(s), me + s
        pl.when(low >= 0)(lambda: act(jnp.maximum(low, 0), 0))

        @pl.when(jnp.logical_and(high < n, s > 0))
        def _():
            act(jnp.minimum(high, n - 1), 1)

    turns = 2 * waves
    ripe = jnp.where(at_end, 0, waves) if lent else 0

    def finished(i, act):
        s, r = i // turns, i % turns - ripe
        fits = jnp.logical_and(jnp.logical_and(r >= 0, r < waves), s > 0)
        spot = jnp.maximum(jnp.minimum(r, waves - 1), 0)
        pl.when(fits)(lambda: around(s, lambda b, slot: act(b, spot, slot)))

    def pass_on(k):
        lend(k).wait_recv()
        for g in range(1, groups):
            spread(k, g).start()

    for r in range(waves):
        sum_cores(me, r)
    for r in range(waves):
        sum_chips(me, r)
    for k in range(lent):
        pl.when(me == n - 2)(lambda: pass_on(k))
    first_help = 2 * turns + waves

    def step(i, carry):
        s, u = i // turns, i % turns
        low, high = low_block(s), me + s
        low_spot, high_spot = jnp.maximum(low, 0), jnp.minimum(high, n - 1)
        has_low, has_high = low >= 0, high < n

        @pl.when(u < waves)
        def _():
            r = jnp.minimum(u, waves - 1)

            @pl.when(has_low)
            def _():
                upward(low_spot, r).wait_recv()
                pl.when(has_next)(lambda: upward(low_spot, r).start())

            @pl.when(has_high)
            def _():
                downward(high_spot, r).wait_recv()
                pl.when(has_prev)(lambda: downward(high_spot, r).start())

            around(s, lambda b, slot: multiply(slot, b, r))

        if lent:
            @pl.when(jnp.logical_and(u >= waves, inner))
            def _():
                r = jnp.maximum(u - waves, 0)

                @pl.when(has_low)
                def _():
                    upward_rest(low_spot, r).wait_recv()
                    pl.when(rest_up)(lambda: upward_rest(low_spot, r).start())

                @pl.when(has_high)
                def _():
                    downward_rest(high_spot, r).wait_recv()
                    pl.when(rest_down)(lambda: downward_rest(high_spot, r).start())

                around(s, lambda b, slot: multiply_rest(slot, b, r))

        finished(i, lambda b, r, slot: round_partial(b, r, slot))
        finished(i - 1, lambda b, r, slot: sum_cores(b, r))
        finished(i - 3, lambda b, r, slot: sum_chips(b, r))
        for k in range(lent):
            when = min(turns + waves + (k + 1) * waves // lent, 2 * turns)
            pl.when(jnp.logical_and(i == when, me == 1))(lambda: pass_on(k))
        if lent:
            def early_help(spot, act):
                r = jnp.maximum(jnp.minimum(i - spot, waves - 1), 0)

                @pl.when(jnp.logical_and(i >= spot, i < spot + waves))
                def _():
                    for base in range(2):
                        around(base, lambda b, slot: act(b, r))

            @pl.when(jnp.logical_and(i == first_help, beside))
            def _():
                for k in range(lent):
                    for g in range(1, groups):
                        spread(k, g, True).wait_recv()

            early_help(first_help, helping)
            early_help(first_help + 1, reduce_help)
            early_help(first_help + 4, combine)

            def later(back, act):
                pl.when(i - back >= 2 * turns)(
                    lambda: finished(i - back, lambda b, r, slot: act(b, r))
                )

            later(1, helping)
            later(2, reduce_help)
            later(4, combine)
        return carry

    lax.fori_loop(turns, n * turns + 4, step, 0)
    loads[8].wait()

    for j in range(share):
        source = head * share + j
        if lent:
            outer = jnp.logical_and(source != me, jnp.logical_or(source == 0, source == n - 1))
            source = jnp.where(outer, jnp.where(source == 0, 1, n - 2), source)
        for k in range(heads):
            here = jnp.logical_and(source == me, k == head)

            for r in range(waves):
                @pl.when(jnp.logical_not(here))
                def _():
                    remote(
                        fin_out.at[0, 0, r], final.at[j, k, r], fin_send.at[0, 0, r],
                        fin_recv.at[j, k, r], {"ctx": source, "heads": k},
                    ).wait_recv()

                base = r * band_rows + (k // cores) * strip
                part = slice(base, base + strip)
                lo = j * out_width + (k % cores) * half
                residual[part, lo : lo + half] = (
                    resid_ref[part, lo : lo + half].astype(F32) + final[j, k, r].astype(F32)
                )

    for load in loads[11:]:
        load.wait()
    latent_width = latent_ref.shape[1]
    strand = latent_width // heads
    features = residual.shape[1] * heads
    experts_here = grow_ref.shape[0]
    slot_rows = n * CAP
    held = residual[...]
    scaled = (held * moe_ref[...]).astype(BF)
    picked = jnp.dot(placed[...], scaled, preferred_element_type=F32).astype(BF)

    def square_copy(k):
        return remote(
            square_out, square_in.at[k], square_send.at[k], square_recv.at[k],
            {"heads": (head + k) % heads},
        )

    def first_copy(e, k):
        return remote(
            slots_out.at[e, k], slots_in.at[e, k], first_send.at[e, k], first_recv.at[e, k],
            {"heads": (head + k) % heads},
        )

    def second_copy(e, k):
        to = (me + k) % n
        return remote(
            middle.at[e, to], gathered.at[e, head, me], second_send.at[e, k],
            second_recv.at[e, k], {"ctx": to},
        )

    def third_copy(e, j):
        spot = gathered.at[e, head]
        return remote(
            spot, spot, third_send.at[e, j], third_recv.at[e, j], {"heads": (head + j) % heads}
        )

    def fourth_copy(e, k):
        return remote(
            back_out.at[e, (head + k) % heads], back_in.at[e, k], fourth_send.at[e, k],
            fourth_recv.at[e, k], {"heads": (head + k) % heads},
        )

    def fifth_copy(e, k):
        to = (me + k) % n
        return remote(
            back_middle.at[e, to], returned.at[head, e, me], fifth_send.at[e, k],
            fifth_recv.at[e, k], {"ctx": to},
        )

    def sixth_copy(e, j):
        spot = returned.at[head, e]
        return remote(
            spot, spot, sixth_send.at[e, j], sixth_recv.at[e, j], {"heads": (head + j) % heads}
        )

    far = heads // 2
    for e in range(experts_here):
        rows_here = picked[e * slot_rows : (e + 1) * slot_rows]
        for k in [far] + [k for k in range(1, heads) if k != far] + [0]:
            to = (head + k) % heads
            lane = pl.ds(pl.multiple_of(to * strand, strand), strand)
            value = jnp.dot(rows_here, latent_ref[:, lane], preferred_element_type=F32)
            slots_out[e, k] = value.astype(BF).reshape(n, CAP, strand)
            if k:
                first_copy(e, k).start()
        if e == 0:
            power = jnp.sum(held * held, axis=1, keepdims=True)
            power = jnp.transpose(jnp.broadcast_to(power, (rows, 128)))[:8, :]
            square_out[...] = lax.dot_general(
                power, placed[...].astype(F32), (((1,), (1,)), ((), ())),
                precision=lax.Precision.HIGHEST, preferred_element_type=F32,
            )
            for k in range(1, heads):
                square_copy(k).start()

    power = square_out[...]
    for k in range(1, heads):
        square_copy(k).wait_recv()
        power = power + square_in[k]
    scale = lax.rsqrt(power / features + epsilon)
    scale = jnp.transpose(jnp.broadcast_to(scale[0:1, :], (128, scale.shape[1])))
    for e in range(experts_here):
        for k in range(1, heads):
            first_copy(e, k).wait_recv()
        for z in range(n):
            total = slots_out[e, 0, z].astype(F32)
            for k in range(1, heads):
                total = total + slots_in[e, k, z].astype(F32)
            base = e * slot_rows + z * CAP
            middle[e, z] = (total * scale[base : base + CAP, 0:1]).astype(BF)
        for k in range(1, n):
            second_copy(e, k).start()
        gathered[e, head, me] = middle[e, me]
    for e in range(experts_here):
        for k in range(1, n):
            second_copy(e, k).wait_recv()
        for j in range(1, heads):
            third_copy(e, j).start()
    for e in range(experts_here):
        for j in range(1, heads):
            third_copy(e, j).wait_recv()
        fed = jnp.concatenate(
            [gathered[e, h].reshape(slot_rows, strand) for h in range(heads)], axis=1
        )
        hidden = lax.dot_general(
            fed, grow_ref[e], (((1,), (1,)), ((), ())), preferred_element_type=F32
        )
        hidden = (jnp.maximum(hidden, 0.0) ** 2).astype(BF)
        value = jnp.dot(hidden, shrink_ref[e], preferred_element_type=F32).astype(BF)
        for h in range(heads):
            back_out[e, h] = value[:, h * strand : (h + 1) * strand].reshape(n, CAP, strand)
        for k in range(1, heads):
            fourth_copy(e, k).start()
    for e in range(experts_here):
        for k in range(1, heads):
            fourth_copy(e, k).wait_recv()
        total = back_out[e, head].astype(F32)
        for k in range(1, heads):
            total = total + back_in[e, k].astype(F32)
        back_middle[e] = total.astype(BF)
        for k in range(1, n):
            fifth_copy(e, k).start()
        returned[head, e, me] = back_middle[e, me]
    for e in range(experts_here):
        for k in range(1, n):
            fifth_copy(e, k).wait_recv()
        for j in range(1, heads):
            sixth_copy(e, j).start()
    for e in range(experts_here):
        for j in range(1, heads):
            sixth_copy(e, j).wait_recv()
    combined = jnp.concatenate(
        [
            lax.dot_general(
                table[...], returned[h].reshape(wave * CAP, strand), (((0,), (0,)), ((), ())),
                preferred_element_type=F32,
            ).astype(BF)
            for h in range(heads)
        ],
        axis=1,
    )
    lift_step = min(256, residual.shape[1])
    for lo in range(0, residual.shape[1], lift_step):
        part = slice(lo, lo + lift_step)
        value = jnp.dot(combined, lift_ref[:, part], preferred_element_type=F32)
        out_ref[:, part] = (residual[:, part] + value).astype(BF)

    for k in range(1, heads):
        square_copy(k).wait_send()
    for e in range(experts_here):
        for k in range(1, heads):
            first_copy(e, k).wait_send()
            third_copy(e, k).wait_send()
            fourth_copy(e, k).wait_send()
            sixth_copy(e, k).wait_send()
        for k in range(1, n):
            second_copy(e, k).wait_send()
            fifth_copy(e, k).wait_send()
    for q in range(pairs):
        pl.when(has_next)(lambda: chain_copy(q).wait_send())
    for b in range(n):
        sent = jnp.logical_or(to_beside(b), jnp.logical_not(local_final(b, me)))
        for r in range(waves):
            pl.when(jnp.logical_and(has_next, b <= me))(lambda: upward(b, r).wait_send())
            pl.when(jnp.logical_and(has_prev, b >= me))(lambda: downward(b, r).wait_send())
            core_copy(b, r, 0).wait_send()
            for k in range(1, chips):
                chip_copy(b, r, k, 0).wait_send()
            pl.when(sent)(lambda: final_copy(b, r, me, 0).wait_send())
            if lent:
                pl.when(jnp.logical_and(rest_up, b <= me))(lambda: upward_rest(b, r).wait_send())
                pl.when(jnp.logical_and(rest_down, b >= me))(
                    lambda: downward_rest(b, r).wait_send()
                )

                @pl.when(helps(b))
                def _():
                    core_copy(b, r, 1).wait_send()
                    for k in range(1, chips):
                        chip_copy(b, r, k, 1).wait_send()
                    pl.when(jnp.logical_not(local_final(b, end_here)))(
                        lambda: final_copy(b, r, end_here, 1).wait_send()
                    )

    for k in range(lent):
        pl.when(at_end)(lambda: lend(k).wait_send())
        for g in range(1, groups):
            pl.when(beside)(lambda: spread(k, g).wait_send())


def reaching(collective_id, grant=48 * 1024 * 1024):
    return pltpu.CompilerParams(
        collective_id=collective_id, has_side_effects=True, vmem_limit_bytes=grant
    )


def dma(*shape):
    return pltpu.SemaphoreType.DMA(shape)


def local(
    ssm_input,
    decay_log,
    state_write,
    state_read,
    skip_scale,
    gate_input,
    ssm_gain,
    weight,
    residual_in,
    moe_gain,
    down_latent,
    expert_up,
    expert_down,
    up_latent,
    expert_ids,
    combine_fixed,
):
    n, heads, groups = lax.axis_size("ctx"), lax.axis_size("heads"), lax.axis_size("groups")
    rows, columns = ssm_input.shape
    head_count = decay_log.shape[1]
    width = columns // head_count
    states = state_write.shape[1]
    span = 2 * width
    pairs = columns // span
    piece = GRP // 4
    count = columns // piece
    lent = LENT_NUM * count // LENT_DEN if n > 3 else 0
    out_width = weight.shape[1]
    share = n // heads
    chips = heads // 2
    half, band_rows = out_width // 2, rows // WAVES
    strip = band_rows // chips
    keep_width, rest_width = (count - lent) * piece, max(lent, 1) * piece
    lane_count = -(-head_count // 128) * 128
    features = residual_in.shape[1]
    experts_here = expert_up.shape[0]
    wave = experts_here * n
    strand = down_latent.shape[1] // heads
    grow = expert_up.transpose(0, 2, 1)
    ids, fixed = expert_ids.T, combine_fixed.T
    anywhere = pl.BlockSpec(memory_space=pltpu.HBM)
    return pl.pallas_call(
        functools.partial(layer_kernel, n, heads, groups, width, piece, 4, lent, WAVES),
        out_shape=jax.ShapeDtypeStruct((rows, features), BF),
        in_specs=[anywhere] * 16,
        out_specs=vmem()[0],
        scratch_shapes=[
            pltpu.VMEM((rows, columns), BF),
            pltpu.VMEM((rows, states), BF),
            pltpu.VMEM((rows, states), BF),
            pltpu.VMEM((head_count, rows), F32),
            pltpu.VMEM((1, head_count), F32),
            pltpu.VMEM(weight.shape, BF),
            pltpu.VMEM((rows, columns), BF),
            pltpu.VMEM((1, columns), F32),
            pltpu.VMEM(residual_in.shape, BF),
            pltpu.VMEM(ids.shape, jnp.int32),
            pltpu.VMEM(fixed.shape, jnp.int32),
            pltpu.VMEM((1, features), F32),
            pltpu.VMEM(down_latent.shape, BF),
            pltpu.VMEM(grow.shape, BF),
            pltpu.VMEM(expert_down.shape, BF),
            pltpu.VMEM(up_latent.shape, BF),
            pltpu.VMEM((rows, lane_count), F32),
            pltpu.VMEM((head_count, rows), F32),
            pltpu.VMEM((8, lane_count), F32),
            pltpu.VMEM((rows, rows), F32),
            pltpu.VMEM((pairs, rows, span), F32),
            pltpu.VMEM((pairs, states, span), F32),
            pltpu.VMEM((pairs, 1, span), F32),
            pltpu.VMEM((pairs, states, span), BF),
            pltpu.VMEM((pairs, states, span), BF),
            pltpu.VMEM((GRP // span, rows, span), F32),
            pltpu.VMEM((n, WAVES, band_rows, keep_width), BF),
            pltpu.VMEM((n, WAVES, band_rows, rest_width), BF),
            pltpu.VMEM((3, WAVES, band_rows, out_width), F32),
            pltpu.VMEM((2, n, WAVES, 2, band_rows, half), BF),
            pltpu.VMEM((2, n, WAVES, band_rows, half), BF),
            pltpu.VMEM((2, n, WAVES, chips, strip, half), BF),
            pltpu.VMEM((2, n, WAVES, chips, strip, half), BF),
            pltpu.VMEM((2, n, WAVES, strip, half), BF),
            pltpu.VMEM((share, heads, WAVES, strip, half), BF),
            pltpu.VMEM((rest_width, out_width), BF),
            pltpu.VMEM((n, WAVES, strip, half), BF),
            pltpu.VMEM((rows, features), F32),
            pltpu.VMEM((wave, rows), F32),
            pltpu.VMEM((wave, rows), jnp.int32),
            pltpu.VMEM((wave * CAP, rows), BF),
            pltpu.VMEM((wave * CAP, rows), BF),
            pltpu.VMEM((8, wave * CAP), F32),
            pltpu.VMEM((heads, 8, wave * CAP), F32),
            pltpu.VMEM((experts_here, heads, n, CAP, strand), BF),
            pltpu.VMEM((experts_here, heads, n, CAP, strand), BF),
            pltpu.VMEM((experts_here, n, CAP, strand), BF),
            pltpu.VMEM((experts_here, heads, n, CAP, strand), BF),
            pltpu.VMEM((experts_here, heads, n, CAP, strand), BF),
            pltpu.VMEM((experts_here, heads, n, CAP, strand), BF),
            pltpu.VMEM((experts_here, n, CAP, strand), BF),
            pltpu.VMEM((heads, experts_here, n, CAP, strand), BF),
            dma(16), dma(pairs), dma(pairs),
            *[dma(n, WAVES)] * 8,
            dma(2, n, WAVES), dma(2, n, WAVES), dma(2, n, WAVES, chips), dma(2, n, WAVES, chips),
            dma(2, n, WAVES), dma(share, heads, WAVES),
            dma(max(lent, 1)), dma(max(lent, 1)), dma(max(lent, 1), groups), dma(max(lent, 1), groups), dma(n, WAVES),
            dma(heads), dma(heads),
            *[dma(experts_here, heads)] * 2, *[dma(experts_here, n)] * 2,
            *[dma(experts_here, heads)] * 4,
            *[dma(experts_here, n)] * 2, *[dma(experts_here, heads)] * 2,
        ],
        compiler_params=reaching(1, 67043328),
    )(
        ssm_input, state_write, state_read, decay_log.T, skip_scale.reshape(1, head_count), weight,
        gate_input, ssm_gain.reshape(1, columns), residual_in,
        ids, fixed, moe_gain.reshape(1, features), down_latent, grow, expert_down, up_latent,
    )


def solution(mesh):
    placed = (
        P(("groups", "ctx"), "heads"),
        P(("groups", "ctx"), "heads"),
        P(("groups", "ctx"), None),
        P(("groups", "ctx"), None),
        P("heads"),
        P(("groups", "ctx"), "heads"),
        P("heads"),
        P("heads", "ctx"),
        P(("groups", "ctx"), "heads"),
        P("heads"),
        P("heads", None),
        P("ctx", None, "heads"),
        P("ctx", "heads", None),
        P(None, "heads"),
        P(("groups", "ctx"), None),
        P(("groups", "ctx"), None),
    )
    return jax.shard_map(
        local, mesh=mesh, in_specs=placed, out_specs=P(("groups", "ctx"), "heads"), check_vma=False
    )
```
